128 devices in a mesh: client: 128 (over x, z, y, core).
Axes of the slice: x: 4, y: 4, z: 4, core: 2. Of those that a mesh axis runs over, the one named last changes fastest.
Arguments:
- patches: bfloat16 [16384, 192], P('client'), may hold values from -6 to 6
- labels: int32 [1024], replicated, may hold values from 0 to 9
- assign: int32 [128, 1], replicated, may hold values from 0 to 15; in each aligned block of 128 rows (0 to 127, 128 to 255, ...) at most 16 rows name the same one
- patch_embed: bfloat16 [192, 384], replicated, may hold values from -0.4375 to 0.4375
- positions: bfloat16 [16, 384], replicated, may hold values from -3 to 3
- client_in: bfloat16 [384, 3072], replicated, may hold values from -3 to 3
- client_down: bfloat16 [1536, 384], replicated, may hold values from -0.15625 to 0.15625
- server_in: bfloat16 [2, 6144, 3072], P(None, 'client'), may hold values from -3 to 3
- server_down: bfloat16 [2, 24576, 384], P(None, 'client'), may hold values from -0.15625 to 0.15625
- classifier: bfloat16 [16, 384, 10], replicated, may hold values from -15 to 15
Outputs:
- losses: float32 [128, 16], P('client')
- grad_patch_embed: float32 [192, 384], P(None, 'client')
- grad_positions: float32 [16, 384], P(None, 'client')
- grad_client_in: float32 [384, 3072], P(None, 'client')
- grad_client_down: float32 [1536, 384], P(None, 'client')
- grad_server_in: float32 [2, 6144, 3072], P(None, 'client')
- grad_server_down: float32 [2, 24576, 384], P(None, 'client')
- grad_classifier: float32 [6144, 10], P('client')
The draws below stay inside these ranges and needn't reach their ends.
Inputs may be any that keep to these rules, and one draw needn't show every extreme that they name: `assign`: no server shard is named by more than 16 clients, a bound that some block reaches.
All inputs are finite; a program needn't handle non-finite values.
Results may differ from the reference program's by a relative error of at most 0.025.
Values may be sent and summed in bfloat16 or wider, within the bound.
A program may use at most 128 MiB of HBM per device.

```python
import math
import jax
import jax.numpy as jnp
import numpy as np
from jax import lax

D = 384
HEADS = 6
FF = 1536
PATCH = 192
TOK = 16
CLASSES = 10
IMG = 8
SHARDS = 16
SLOTS = 2
SERVER_LAYERS = 2
CAPACITY = 16
N_CLIENT = 128


def scaled_normal(key, shape, fan_in):
    return jax.random.truncated_normal(key, -4.0, 4.0, shape, jnp.float32) / math.sqrt(fan_in)


def draw_client_in(key, part):
    values = scaled_normal(jax.random.fold_in(key, 11), (D, 4 * D + FF), D)
    return values.astype(jnp.bfloat16)


def draw_server_in(key, part):
    values = scaled_normal(jax.random.fold_in(key, 23), (SERVER_LAYERS, SHARDS * D, 4 * D + FF), D)
    return values.astype(jnp.bfloat16)


def draw_classifier(key, part):
    values = scaled_normal(jax.random.fold_in(key, 37), (SHARDS, D, CLASSES), D)
    return values.astype(jnp.bfloat16)


def place_ends(result, key, least, high):
    dims = result.shape
    place = [jax.random.randint(jax.random.fold_in(key, axis), (), 0, dims[axis]) for axis in range(len(dims))]
    result = result.at[tuple(place)].set(least)
    longest = dims.index(max(dims))
    place[longest] = (place[longest] + 1) % dims[longest]
    return result.at[tuple(place)].set(high)


def levels(key, extent, split, least, top_value):
    level, own = 1.0, jax.random.fold_in(key, 6)
    for dim, blocks in split:
        steps = jnp.exp(jax.random.uniform(jax.random.fold_in(own, dim), (blocks,), jnp.float32, least / len(split), top_value / len(split)))
        level = level * jnp.repeat(steps, extent[dim] // blocks).reshape([-1 if axis == dim else 1 for axis in range(len(extent))])
    return level


def assign_block(stream_key, own, number, rows, amount, top, reach, lean):
    sequence = jax.random.permutation(stream_key, amount)
    heavy_load, common = shares(amount, rows * top, reach, lean, True), shares(amount, rows * top, reach, lean, False)
    places = jnp.arange(amount)

    def named(sizes, rotation):
        used = int((sizes > 0).sum())
        fixed = max(1, used // 4)
        shifted = fixed + (places - fixed + rotation * (used - fixed)) % max(1, amount - fixed)
        return jnp.zeros((amount,), jnp.int32).at[sequence[jnp.where(places < fixed, places, shifted)]].set(jnp.asarray(sizes, jnp.int32))

    sizes = jnp.where(number % 4 == 0, named(heavy_load, number // 4), named(common, number - number // 4 - 1))
    mixed = jax.random.permutation(jax.random.fold_in(own, 3), amount)
    donor, sink = mixed[0:amount // 2 * 2:2], mixed[1:amount // 2 * 2:2]
    margin = jnp.minimum(sizes[donor] - 1, reach - sizes[sink]) // 2
    margin = jnp.where((donor == sequence[0]) | (sink == sequence[0]) | (sizes[sink] == 0), 0, jnp.maximum(margin, 0))
    shifted = jax.random.randint(jax.random.fold_in(own, 4), (amount // 2,), 0, 1 << 20) % (margin + 1)
    sizes = sizes.at[donor].add(-shifted).at[sink].add(shifted)
    items = jnp.searchsorted(jnp.cumsum(sizes), jnp.arange(rows * top), side="right").astype(jnp.int32)
    grid = items.reshape(top, rows).T
    grid = grid[jax.random.permutation(jax.random.fold_in(own, 1), rows)]
    rotation = jax.random.randint(jax.random.fold_in(own, 2), (rows, 1), 0, top)
    return jnp.take_along_axis(grid, (jnp.arange(top)[None, :] + rotation) % top, axis=1)


def shares(count, total, reach, slope, full):
    weights = [(1 << 20) // math.isqrt(rank ** slope) + 1 for rank in range(1, count + 1)]
    largest = reach if full else min(reach, max(-(-total // count), total * weights[0] // sum(weights)))
    least = 1 if total - largest >= count - 1 else 0
    given, spare = [largest] + [least] * (count - 1), total - largest - least * (count - 1)
    while spare > 0:
        candidates = [i for i in range(1, count) if given[i] < largest] or [i for i in range(1, count) if given[i] < reach]
        mass, remaining = sum([weights[i] for i in candidates]), spare
        for i in candidates:
            addition = min(reach - given[i], max(1, remaining * weights[i] // mass), spare)
            given[i] = given[i] + addition
            spare = spare - addition
    return np.array(given)


def normal_values(rng, extent, scale, bound, cuts=(), kind=jnp.bfloat16):
    entries = jax.random.normal(rng, extent, jnp.float32) * scale
    if len(cuts) > 0:
        entries = levels(rng, extent, cuts, -0.22, 0.18) * entries
    return jnp.clip(entries, min=-bound, max=bound).astype(kind)


def setup_inputs(seed: int = 0) -> dict:
    splits = jax.random.split(jax.random.key(seed), 11)
    patches = normal_values(splits[0], (N_CLIENT * IMG * TOK, PATCH), 1.0, 6.0, ((0, 128),))
    labels = place_ends(jax.random.randint(splits[1], (N_CLIENT * IMG,), 0, CLASSES), jax.random.fold_in(splits[1], 1), 0, CLASSES - 1).astype(jnp.int32)
    assign_keys = jax.random.split(jax.random.fold_in(splits[2], 1), N_CLIENT // N_CLIENT)
    assign_turns = jax.random.permutation(jax.random.fold_in(splits[2], 3), N_CLIENT // N_CLIENT)
    assign = jax.vmap(lambda own, number: assign_block(jax.random.fold_in(splits[2], 2), own, number, N_CLIENT, SHARDS, 1, CAPACITY, 2))(assign_keys, assign_turns).reshape((N_CLIENT, 1))
    patch_embed = normal_values(splits[3], (PATCH, D), PATCH ** -0.5, 0.4375)
    positions = normal_values(splits[4], (TOK, D), 0.5, 3.0)
    client_in = draw_client_in(jax.random.fold_in(splits[10], 71), 0)
    client_down = normal_values(splits[6], (FF, D), FF ** -0.5, 0.15625)
    server_in = draw_server_in(jax.random.fold_in(splits[10], 71), 0)
    server_down = normal_values(splits[8], (SERVER_LAYERS, SHARDS * FF, D), FF ** -0.5, 0.15625, ((1, 128),))
    classifier = draw_classifier(jax.random.fold_in(splits[10], 71), 0)
    return dict(patches=patches, labels=labels, assign=assign, patch_embed=patch_embed, positions=positions, client_in=client_in, client_down=client_down, server_in=server_in, server_down=server_down, classifier=classifier)


EPSILON = 1e-06

def layer_norm(inputs):
    centre = inputs - lax.optimization_barrier(jnp.mean(inputs, axis=-1, keepdims=True))
    spread = lax.optimization_barrier(jnp.mean(centre * centre, axis=-1, keepdims=True))
    return centre * lax.rsqrt(spread + EPSILON)

def encoder_block(stream, weight_in, weight_down):
    images, tokens, model_width = stream.shape
    head_dim = model_width // HEADS
    normed = layer_norm(stream).astype(jnp.bfloat16).reshape(images * tokens, model_width)
    projected = jnp.dot(normed, weight_in[:, :3 * model_width], preferred_element_type=jnp.float32)
    projected = projected.reshape(images, tokens, 3, HEADS, head_dim)
    queries = projected[:, :, 0]
    key_rows = projected[:, :, 1]
    values = projected[:, :, 2]
    scores = jnp.einsum('bqhe,bkhe->bhqk', queries, key_rows, precision=lax.Precision.HIGHEST) / math.sqrt(head_dim)
    weights_attn = jax.nn.softmax(scores, axis=-1)
    attended = jnp.einsum('bhqk,bkhe->bqhe', weights_attn, values, precision=lax.Precision.HIGHEST)
    attended = attended.reshape(images * tokens, model_width).astype(jnp.bfloat16)
    stream = stream + jnp.dot(attended, weight_in[:, 3 * model_width:4 * model_width], preferred_element_type=jnp.float32).reshape(images, tokens, model_width)
    normed = layer_norm(stream).astype(jnp.bfloat16).reshape(images * tokens, model_width)
    hidden = jax.nn.gelu(jnp.dot(normed, weight_in[:, 4 * model_width:], preferred_element_type=jnp.float32)).astype(jnp.bfloat16)
    return stream + jnp.dot(hidden, weight_down, preferred_element_type=jnp.float32).reshape(images, tokens, model_width)

def client_forward(patch_rows, patch_embed, positions, client_in, client_down):
    stream = jnp.dot(patch_rows, patch_embed, preferred_element_type=jnp.float32).reshape(-1, TOK, D)
    stream = stream + positions.astype(jnp.float32)
    stream = encoder_block(stream, client_in, client_down)
    return stream.reshape(-1, D).astype(jnp.bfloat16)

def server_loss(cut_rows, slot_hot, weights_in, weights_down, class_shard):
    stream = cut_rows.astype(jnp.float32).reshape(-1, TOK, D)
    for layer in range(len(weights_in)):
        stream = encoder_block(stream, weights_in[layer], weights_down[layer])
    pooled = layer_norm(lax.optimization_barrier(jnp.mean(stream, axis=1))).astype(jnp.bfloat16)
    logits = jnp.dot(pooled, class_shard, preferred_element_type=jnp.float32)
    per_loss = (jax.nn.logsumexp(logits, axis=-1) - lax.optimization_barrier(jnp.sum(slot_hot * logits, axis=-1))) * lax.optimization_barrier(jnp.sum(slot_hot, axis=-1))
    return (jnp.sum(per_loss), per_loss)

def arrival_rank(routes):
    places = jnp.arange(routes.shape[0], dtype=jnp.int32)
    earlier = (routes[:, None] == routes[None, :]) & (places[:, None] < places[None, :])
    return lax.optimization_barrier(jnp.sum(earlier.astype(jnp.int32), axis=0))

def select_matrix(routes, arrival, shard, capacity):
    slots_here = jnp.arange(capacity, dtype=jnp.int32)[:, None]
    return ((routes[None, :] == shard) & (arrival[None, :] == slots_here)).astype(jnp.bfloat16)

def slot_labels(labels, selector, rank_in_group, per_image, members):
    label_table = labels.reshape(members, IMG)
    label_part = lax.dynamic_slice_in_dim(label_table, (rank_in_group * per_image).astype(jnp.int32), per_image, 1)
    onehot = (label_part[:, :, None] == jnp.arange(CLASSES, dtype=jnp.int32)[None, None, :]).astype(jnp.float32)
    onehot = onehot.reshape(members, per_image * CLASSES)
    chosen = jnp.dot(selector.astype(jnp.float32), onehot, precision=lax.Precision.HIGHEST)
    return chosen.reshape(-1, CLASSES)

def reference(patches, labels, assign, patch_embed, positions, client_in, client_down, server_in, server_down, classifier):
    members = N_CLIENT
    group_size = members // SHARDS
    per_image = IMG // group_size
    piece_rows = IMG * TOK // group_size
    capacity = SLOTS * group_size
    width_all = 4 * D + FF
    routes = assign[:, 0]
    arrival = arrival_rank(routes)
    patch_sets = patches.reshape(members, IMG * TOK, PATCH)

    def client_cut(patch_rows):
        return client_forward(patch_rows, patch_embed, positions, client_in, client_down)
    cuts = lax.map(client_cut, patch_sets)
    cut_pieces = cuts.reshape(members, group_size, piece_rows * D)
    shard_in = server_in.reshape(SERVER_LAYERS, SHARDS, D, width_all)
    shard_down = server_down.reshape(SERVER_LAYERS, SHARDS, FF, D)

    def device_step(carry, device):
        acc_in, acc_down, acc_class = carry
        shard = device // group_size
        rank_in_group = device % group_size
        selector = select_matrix(routes, arrival, shard, capacity)
        own_piece = lax.dynamic_index_in_dim(cut_pieces, rank_in_group, 1, keepdims=False)
        compact = jnp.dot(selector, own_piece, preferred_element_type=jnp.float32).astype(jnp.bfloat16)
        compact = compact.reshape(capacity * piece_rows, D)
        slot_hot = slot_labels(labels, selector, rank_in_group, per_image, members)
        layer_in = lax.dynamic_index_in_dim(shard_in, shard, 1, keepdims=False)
        layer_down = lax.dynamic_index_in_dim(shard_down, shard, 1, keepdims=False)
        class_shard = lax.dynamic_index_in_dim(classifier, shard, 0, keepdims=False)

        def loss_of(cut_rows, weights_in, weights_down, class_weights):
            return server_loss(cut_rows, slot_hot, weights_in, weights_down, class_weights)
        list_in = tuple((layer_in[layer] for layer in range(SERVER_LAYERS)))
        list_down = tuple((layer_down[layer] for layer in range(SERVER_LAYERS)))
        total_loss, server_back, per_loss = jax.vjp(loss_of, compact, list_in, list_down, class_shard, has_aux=True)
        grad_cut, grad_in, grad_down, grad_class = server_back(jnp.ones((), jnp.float32))
        acc_in = acc_in.at[:, shard].add(jnp.stack(grad_in).astype(jnp.float32))
        acc_down = acc_down.at[:, shard].add(jnp.stack(grad_down).astype(jnp.float32))
        acc_class = acc_class.at[shard].add(grad_class.astype(jnp.float32))
        return ((acc_in, acc_down, acc_class), (grad_cut, per_loss))
    start = (jnp.zeros((SERVER_LAYERS, SHARDS, D, width_all), jnp.float32), jnp.zeros((SERVER_LAYERS, SHARDS, FF, D), jnp.float32), jnp.zeros((SHARDS, D, CLASSES), jnp.float32))
    sums, outputs = lax.scan(device_step, start, jnp.arange(members, dtype=jnp.int32))
    acc_in, acc_down, acc_class = sums
    cut_grads, loss_rows = outputs
    cut_grads = cut_grads.reshape(SHARDS, group_size, capacity, piece_rows * D)

    def client_step(carry, client):
        shard = routes[client]
        slot = arrival[client]
        by_shard = lax.dynamic_index_in_dim(cut_grads, shard, 0, keepdims=False)
        own_grads = lax.dynamic_index_in_dim(by_shard, slot, 1, keepdims=False).reshape(IMG * TOK, D)
        patch_rows = lax.dynamic_index_in_dim(patch_sets, client, 0, keepdims=False)

        def client_of(embed_weights, position_weights, in_weights, down_weights):
            return client_forward(patch_rows, embed_weights, position_weights, in_weights, down_weights)
        cut_again, client_back = jax.vjp(client_of, patch_embed, positions, client_in, client_down)
        grads = client_back(own_grads)
        return (tuple((total + part_grad.astype(jnp.float32) for total, part_grad in zip(carry, grads))), None)
    client_start = (jnp.zeros((PATCH, D), jnp.float32), jnp.zeros((TOK, D), jnp.float32), jnp.zeros((D, width_all), jnp.float32), jnp.zeros((FF, D), jnp.float32))
    client_sums, unused = lax.scan(client_step, client_start, jnp.arange(members, dtype=jnp.int32))
    return (loss_rows, client_sums[0], client_sums[1], client_sums[2], client_sums[3], acc_in.reshape(SERVER_LAYERS, SHARDS * D, width_all), acc_down.reshape(SERVER_LAYERS, SHARDS * FF, D), acc_class.reshape(SHARDS * D, CLASSES))
```

```python
import math

import jax
import jax.numpy as jnp
from jax import lax
from jax.experimental import pallas as pl
from jax.experimental.pallas import tpu as pltpu
from jax.sharding import PartitionSpec as P

D = 384
FF = 1536
TOK = 16
IMG = 8
CLASSES = 10
LAYERS = 2
CAP = 16
EPSILON = 1e-06
SCALE = 0.125
GELU_A = math.sqrt(2.0 / math.pi)
GELU_B = 0.044715
PACK = LAYERS * (D + FF // 8) + D // 8
CUT_A = 576

bf16 = jnp.bfloat16
f32 = jnp.float32
MESH = pl.DeviceIdType.MESH
VMEM = pl.BlockSpec(memory_space=pltpu.VMEM)
SMEM = pl.BlockSpec(memory_space=pltpu.SMEM)
ANY = pl.BlockSpec(memory_space=pl.ANY)


def mm(a, b, ca=1, cb=0):
    return lax.dot_general(a, b, (((ca,), (cb,)), ((), ())), preferred_element_type=f32)


def iota(shape, dim):
    return lax.broadcasted_iota(jnp.int32, shape, dim)


def norm(v):
    centre = v - jnp.mean(v, axis=-1, keepdims=True)
    rstd = lax.rsqrt(jnp.mean(centre * centre, axis=-1, keepdims=True) + EPSILON)
    return centre * rstd, rstd


def norm_back(v, grad):
    hat, rstd = norm(v)
    along = jnp.mean(grad * hat, axis=-1, keepdims=True)
    return rstd * (grad - jnp.mean(grad, axis=-1, keepdims=True) - hat * along)


def rounded(v):
    return v.astype(bf16).astype(f32)


def head_masks(rows):
    low = (iota((rows, 128), 1) < 64).astype(f32)
    return low.astype(bf16), (1.0 - low).astype(bf16)


def two_heads(v):
    low, high = head_masks(v.shape[0])
    return jnp.concatenate([v * low, v * high], axis=0)


def merge_heads(v):
    rows = v.shape[0] // 2
    return jnp.where(iota((rows, 128), 1) < 64, v[:rows], v[rows:])


def block_forward(l, rows, S, win, wdn):
    x = S["x"][l]
    hat, _ = norm(x)
    u1 = hat.astype(bf16)
    S["u1"][l] = u1
    for n in range(3):
        cols = slice(D * n, D * n + D)
        S["qkv"][l, :, cols] = mm(u1, win[l, :, cols]).astype(bf16)
    same = ((iota((256, 128), 0) & 127) >> 4) == (iota((256, 128), 1) >> 4)
    for g in range(rows // 128):
        part = slice(128 * g, 128 * g + 128)
        for p in range(3):
            q2 = S["qkv"][l, part, 128 * p : 128 * p + 128]
            k2 = S["qkv"][l, part, D + 128 * p : D + 128 * p + 128]
            v2 = S["qkv"][l, part, 2 * D + 128 * p : 2 * D + 128 * p + 128]
            scores = mm(two_heads(q2), k2, 1, 1) * SCALE
            scores = jnp.where(same, scores, -1e30)
            grown = jnp.exp(scores - jnp.max(scores, axis=-1, keepdims=True))
            prob = grown / jnp.sum(grown, axis=-1, keepdims=True)
            S["prob"][l, 3 * g + p] = prob
            S["att"][l, part, 128 * p : 128 * p + 128] = merge_heads(mm(prob.astype(bf16), v2)).astype(bf16)
    x1 = S["x"][l] + mm(S["att"][l], win[l, :, 3 * D : 4 * D])
    S["x1"][l] = x1
    hat, _ = norm(x1)
    u2 = hat.astype(bf16)
    S["u2"][l] = u2
    for n in range(4):
        pre = mm(u2, win[l, :, 4 * D + D * n : 5 * D + D * n])
        S["pre"][l, :, D * n : D * n + D] = pre
        bent = jnp.tanh(GELU_A * (pre + GELU_B * pre * pre * pre))
        S["h"][l, :, D * n : D * n + D] = (0.5 * pre * (1.0 + bent)).astype(bf16)
    return S["x1"][l] + mm(S["h"][l], wdn[l])


def block_backward(l, rows, S, win, wdn, dy_ref, emit_in, emit_down):
    dyb = dy_ref[...].astype(bf16)
    for n in range(4):
        cols = slice(D * n, D * n + D)
        dh = rounded(mm(dyb, wdn[l, cols, :], 1, 1))
        pre = S["pre"][l, :, cols]
        bent = jnp.tanh(GELU_A * (pre + GELU_B * pre * pre * pre))
        slope = 0.5 * (1.0 + bent) + 0.5 * pre * (1.0 - bent * bent) * GELU_A * (1.0 + 3.0 * GELU_B * pre * pre)
        S["dpre"][:, cols] = (dh * slope).astype(bf16)
        emit_down(n, S["h"][l, :, cols], dyb)
        emit_in(4 + n, S["u2"][l], S["dpre"][:, cols])
    du2 = rounded(mm(S["dpre"][...], win[l, :, 4 * D :], 1, 1))
    dx1 = dy_ref[...] + norm_back(S["x1"][l], du2)
    dy_ref[...] = dx1
    dx1b = dx1.astype(bf16)
    emit_in(3, S["att"][l], dx1b)
    datt = mm(dx1b, win[l, :, 3 * D : 4 * D], 1, 1).astype(bf16)
    S["datt"][...] = datt
    for g in range(rows // 128):
        part = slice(128 * g, 128 * g + 128)
        for p in range(3):
            cq = slice(128 * p, 128 * p + 128)
            ck = slice(D + 128 * p, D + 128 * p + 128)
            cv = slice(2 * D + 128 * p, 2 * D + 128 * p + 128)
            qs = two_heads(S["qkv"][l, part, cq])
            dos = two_heads(S["datt"][part, cq])
            prob = S["prob"][l, 3 * g + p]
            dprob = mm(dos, S["qkv"][l, part, cv], 1, 1)
            dscore = prob * (dprob - jnp.sum(prob * dprob, axis=-1, keepdims=True)) * SCALE
            dsb = dscore.astype(bf16)
            S["dqkv"][part, cq] = merge_heads(mm(dsb, S["qkv"][l, part, ck])).astype(bf16)
            S["dqkv"][part, ck] = mm(dsb, qs, 0, 0).astype(bf16)
            S["dqkv"][part, cv] = mm(prob.astype(bf16), dos, 0, 0).astype(bf16)
    for n in range(3):
        emit_in(n, S["u1"][l], S["dqkv"][:, D * n : D * n + D])
    du1 = rounded(mm(S["dqkv"][...], win[l, :, : 3 * D], 1, 1))
    dy_ref[...] = dy_ref[...] + norm_back(S["x"][l], du1)


def saved_shapes(layers, rows):
    return dict(
        x1=((layers, rows, D), f32),
        u1=((layers, rows, D), bf16),
        u2=((layers, rows, D), bf16),
        qkv=((layers, rows, 3 * D), bf16),
        prob=((layers, 3 * rows // 128, 256, 128), f32),
        att=((layers, rows, D), bf16),
        pre=((layers, rows, FF), f32),
        h=((layers, rows, FF), bf16),
    )


SAVED = tuple(saved_shapes(1, 128))


def client_forward_kernel(patches, embed, positions, win, wdn, *refs):
    S = dict(zip(("cut", "x") + SAVED, refs))
    tiled = jnp.concatenate([positions[...].astype(f32)] * IMG, axis=0)
    S["x"][0] = mm(patches[...], embed[...]) + tiled
    y = block_forward(0, 128, S, win, wdn)
    S["cut"][...] = y.astype(bf16)


def client_forward(patches, embed, positions, win, wdn):
    shapes = saved_shapes(1, 128)
    out = [jax.ShapeDtypeStruct((128, D), bf16), jax.ShapeDtypeStruct((1, 128, D), f32)]
    out += [jax.ShapeDtypeStruct(*shapes[k]) for k in SAVED]
    return pl.pallas_call(
        client_forward_kernel,
        out_shape=out,
        in_specs=[VMEM] * 5,
        out_specs=[VMEM] * len(out),
        compiler_params=pltpu.CompilerParams(vmem_limit_bytes=56 << 20),
        name="client_forward",
    )(patches, embed, positions, win, wdn)


def client_backward_kernel(grads, patches, win, wdn, *refs):
    n_in = 1 + len(SAVED)
    S = dict(zip(("x",) + SAVED, refs[:n_in]))
    packed, dy, dpre, datt, dqkv, tail, pp = refs[n_in:]
    S.update(dpre=dpre, datt=datt, dqkv=dqkv)
    dy[...] = grads[...].astype(f32)
    tail[...] = jnp.zeros_like(tail)

    def emit_in(b, u, dout):
        val = mm(dout, u, 0, 0).astype(bf16)
        for i in range(2):
            packed[2 * b + i, 0] = val[192 * i : 192 * i + 160]
            packed[2 * b + i, 1, 0:32] = val[192 * i + 160 : 192 * i + 192]

    def emit_tail(q, dout, right):
        val = mm(dout, right, 0, 0)
        for i in range(16):
            tail[i, 24 * q : 24 * q + 24] = val[24 * i : 24 * i + 24]

    block_backward(0, 128, S, win, wdn, dy, emit_in, lambda n, h, dyb: emit_tail(n, dyb, h))
    pp[...] = (iota((128, D), 1) - 192 == (iota((128, D), 0) & 15)).astype(f32).astype(bf16)
    pp[:, 0:192] = patches[...]
    emit_tail(4, dy[...].astype(bf16), pp[...])
    for i in range(16):
        packed[i, 1, 32:160] = tail[i].astype(bf16)


def client_backward(grads, patches, win, wdn, saved):
    return pl.pallas_call(
        client_backward_kernel,
        out_shape=jax.ShapeDtypeStruct((16, 2, 160, D), bf16),
        in_specs=[VMEM] * (4 + len(saved)),
        out_specs=VMEM,
        scratch_shapes=[
            pltpu.VMEM((128, D), f32),
            pltpu.VMEM((128, FF), bf16),
            pltpu.VMEM((128, D), bf16),
            pltpu.VMEM((128, 3 * D), bf16),
            pltpu.VMEM((16, 128, D), f32),
            pltpu.VMEM((128, D), bf16),
        ],
        compiler_params=pltpu.CompilerParams(vmem_limit_bytes=56 << 20),
        name="client_backward",
    )(grads, patches, win, wdn, *saved)


def server_kernel(arrived, acol, arow, labels, win, wdn, classes, losses, packed, gcut, source, *refs):
    names = ("x",) + SAVED + ("dpre", "datt", "dqkv", "dy", "cls", "sem")
    S = dict(zip(names, refs))
    me = lax.axis_index("client")
    shard, rank_in = me // 8, me % 8
    copy = pltpu.make_async_copy(classes.at[shard], S["cls"], S["sem"])
    copy.start()
    earlier = (acol[...] == arow[...]) & (iota((128, 128), 0) < iota((128, 128), 1))
    rank = jnp.sum(earlier.astype(f32), axis=0, keepdims=True)
    rank_i = rank.astype(jnp.int32)
    source[...] = arow[...] * CAP + rank_i
    chosen = (jnp.broadcast_to(arow[...], (CAP, 128)) == shard) & (
        jnp.broadcast_to(rank_i, (CAP, 128)) == iota((CAP, 128), 0)
    )
    selector = chosen.astype(f32).astype(bf16)
    label = jnp.sum(jnp.where(iota((128, IMG), 1) == rank_in, labels[...], 0), axis=1, keepdims=True)
    onehot = (label == iota((128, CLASSES), 1)).astype(f32).astype(bf16)
    hot = mm(selector, onehot)
    filled = jnp.sum(hot, axis=1, keepdims=True)
    spread = (iota((128, 2048), 0) == (iota((128, 2048), 1) >> 4)).astype(f32).astype(bf16)
    wide = mm(selector, spread).astype(bf16)
    repeat = ((iota((256, CAP), 0) >> 4) == iota((256, CAP), 1)).astype(f32).astype(bf16)
    tall = mm(repeat, wide)
    same = (iota((256, 2048), 0) & 15) == (iota((256, 2048), 1) & 15)
    S["x"][0] = mm(jnp.where(same, tall, 0.0).astype(bf16), arrived[...])

    def forward(l, carry):
        S["x"][l + 1] = block_forward(l, 256, S, win, wdn)
        return carry

    lax.fori_loop(0, LAYERS, forward, 0)
    copy.wait()
    mean = jnp.mean(S["x"][LAYERS].reshape(CAP, TOK, D), axis=1)
    hat, _ = norm(mean)
    pooled = hat.astype(bf16)
    logits = mm(pooled, S["cls"][...])
    top = jnp.max(logits, axis=1, keepdims=True)
    grown = jnp.exp(logits - top)
    total = jnp.sum(grown, axis=1, keepdims=True)
    per = (jnp.log(total) + top - jnp.sum(hot * logits, axis=1, keepdims=True)) * filled
    eye = iota((CAP, CAP), 0) == iota((CAP, CAP), 1)
    losses[...] = jnp.sum(jnp.where(eye, per, 0.0), axis=0, keepdims=True)
    dlogits = ((grown / total) * filled - hot).astype(bf16)
    gcls = mm(pooled, dlogits, 0, 0).astype(bf16)
    for r in range(8):
        packed[r, PACK - 48 :, :] = jnp.zeros((48, D), bf16)
        packed[r, PACK - 48 :, 0:CLASSES] = gcls[48 * r : 48 * r + 48]
    dpooled = rounded(mm(dlogits, S["cls"][...], 1, 1))
    dmean = norm_back(mean, dpooled) * (1.0 / TOK)
    S["dy"][...] = jnp.broadcast_to(dmean[:, None, :], (CAP, TOK, D)).reshape(CAP * TOK, D)

    def backward(i, carry):
        l = LAYERS - 1 - i
        base = 576 * l

        def emit_in(b, u, dout):
            val = mm(u, dout, 0, 0).astype(bf16)
            for r in range(8):
                packed[r, pl.ds(pl.multiple_of(base + 48 * b, 16), 48), :] = val[48 * r : 48 * r + 48]

        def emit_down(n, h, dyb):
            val = mm(h, dyb, 0, 0).astype(bf16)
            for j in range(2):
                packed[2 * n + j, pl.ds(pl.multiple_of(base + D, 16), 192), :] = val[192 * j : 192 * j + 192]

        block_backward(l, 256, S, win, wdn, S["dy"], emit_in, emit_down)
        return carry

    lax.fori_loop(0, LAYERS, backward, 0)
    gcut[...] = S["dy"][...].astype(bf16)


def server(arrived, acol, arow, labels, win, wdn, classes):
    shapes = saved_shapes(LAYERS, 256)
    return pl.pallas_call(
        server_kernel,
        out_shape=[
            jax.ShapeDtypeStruct((1, CAP), f32),
            jax.ShapeDtypeStruct((8, PACK, D), bf16),
            jax.ShapeDtypeStruct((256, D), bf16),
            jax.ShapeDtypeStruct((1, 128), jnp.int32),
        ],
        in_specs=[VMEM] * 6 + [ANY],
        out_specs=[VMEM] * 4,
        scratch_shapes=[pltpu.VMEM((LAYERS + 1, 256, D), f32)]
        + [pltpu.VMEM(*shapes[k]) for k in SAVED]
        + [
            pltpu.VMEM((256, FF), bf16),
            pltpu.VMEM((256, D), bf16),
            pltpu.VMEM((256, 3 * D), bf16),
            pltpu.VMEM((256, D), f32),
            pltpu.VMEM((D, CLASSES), bf16),
            pltpu.SemaphoreType.DMA,
        ],
        compiler_params=pltpu.CompilerParams(vmem_limit_bytes=60 << 20),
        name="server",
    )(arrived, acol, arow, labels, win, wdn, classes)


class Place:
    def __init__(self):
        me = lax.axis_index("client")
        self.me = me
        self.c, self.y, self.z, self.x = me % 2, me // 2 % 4, me // 8 % 4, me // 32
        self.r, self.group = me % 8, me // 8 * 8
        self.partner = me + 1 - 2 * self.c
        self.yp, self.ym = self.at(0, 0, 1), self.at(0, 0, 3)
        self.xp, self.xm = self.at(1, 0, 0), self.at(3, 0, 0)
        self.zp, self.zm = self.at(0, 1, 0), self.at(0, 3, 0)

    def at(self, dx, dz, dy):
        x, z, y = (self.x + dx) % 4, (self.z + dz) % 4, (self.y + dy) % 4
        return ((x * 4 + z) * 4 + y) * 2 + self.c

    def greet(self, group, plane):
        peers = []
        if group:
            peers += [self.group + (self.r + i) % 8 for i in range(1, 8)]
        if plane:
            peers += [self.xp, self.xm, self.zp, self.zm]
        barrier = pltpu.get_barrier_semaphore()
        for peer in peers:
            pl.semaphore_signal(barrier, inc=1, device_id=(peer,), device_id_type=MESH)
        pl.semaphore_wait(barrier, len(peers))


class Wire:
    def __init__(self, send_sem, recv_sem):
        self.send_sem, self.recv_sem, self.sent = send_sem, recv_sem, []

    def make(self, src, dst, k, device):
        return pltpu.make_async_remote_copy(
            src_ref=src,
            dst_ref=dst,
            send_sem=self.send_sem.at[k],
            recv_sem=self.recv_sem.at[k],
            device_id=(device,),
            device_id_type=MESH,
        )

    def send(self, src, dst, k, device):
        copy = self.make(src, dst, k, device)
        copy.start()
        self.sent.append(copy)

    def wait(self, landed, k, device):
        self.make(landed, landed, k, device).wait_recv()

    def finish(self):
        for copy in self.sent:
            copy.wait_send()


def plane_gather(wire, place, buf, count, k0):
    half, quarter = count // 2, count // 4
    x, z = place.x, place.z
    xm, xp, zm, zp = (x + 3) % 4, (x + 1) % 4, (z + 3) % 4, (z + 1) % 4
    xo, zo = (x + 2) % 4, (z + 2) % 4
    X, XA, XB = pl.ds(0, half), pl.ds(0, quarter), pl.ds(quarter, quarter)
    Z, ZA, ZB = pl.ds(half, half), pl.ds(half, quarter), pl.ds(half + quarter, quarter)

    def both(ref, k, device):
        wire.send(ref, ref, k0 + k, device)

    def first():
        both(buf.at[x, z, X], 0, place.xp)
        both(buf.at[x, z, X], 1, place.xm)
        both(buf.at[x, z, Z], 2, place.zp)
        both(buf.at[x, z, Z], 3, place.zm)

    def second():
        wire.wait(buf.at[xm, z, X], k0 + 0, place.xm)
        both(buf.at[xm, z, XA], 4, place.xp)
        wire.wait(buf.at[xp, z, X], k0 + 1, place.xp)
        both(buf.at[xp, z, XB], 5, place.xm)
        wire.wait(buf.at[x, zm, Z], k0 + 2, place.zm)
        both(buf.at[x, zm, ZA], 6, place.zp)
        wire.wait(buf.at[x, zp, Z], k0 + 3, place.zp)
        both(buf.at[x, zp, ZB], 7, place.zm)

    def third():
        wire.wait(buf.at[xo, z, XA], k0 + 4, place.xm)
        wire.wait(buf.at[xo, z, XB], k0 + 5, place.xp)
        both(buf.at[:, z, X], 8, place.zp)
        both(buf.at[:, z, X], 9, place.zm)
        wire.wait(buf.at[x, zo, ZA], k0 + 6, place.zm)
        wire.wait(buf.at[x, zo, ZB], k0 + 7, place.zp)
        both(buf.at[x, :, Z], 10, place.xp)
        both(buf.at[x, :, Z], 11, place.xm)

    def fourth():
        wire.wait(buf.at[:, zm, X], k0 + 8, place.zm)
        both(buf.at[0:2, zm, X], 12, place.zp)
        wire.wait(buf.at[:, zp, X], k0 + 9, place.zp)
        both(buf.at[2:4, zp, X], 13, place.zm)
        wire.wait(buf.at[xm, :, Z], k0 + 10, place.xm)
        both(buf.at[xm, 0:2, Z], 14, place.xp)
        wire.wait(buf.at[xp, :, Z], k0 + 11, place.xp)
        both(buf.at[xp, 2:4, Z], 15, place.xm)

    def fifth():
        wire.wait(buf.at[0:2, zo, X], k0 + 12, place.zm)
        wire.wait(buf.at[2:4, zo, X], k0 + 13, place.zp)
        wire.wait(buf.at[xo, 0:2, Z], k0 + 14, place.xm)
        wire.wait(buf.at[xo, 2:4, Z], k0 + 15, place.xp)

    return first, second, third, fourth, fifth


def gather_kernel(cut, win_s, wdn_s, arrived, win, wdn, send_sem, recv_sem, local_sem):
    place = Place()
    x, z, y, r = place.x, place.z, place.y, place.r
    place.greet(True, True)
    wire = Wire(send_sem, recv_sem)
    for i in range(1, 8):
        j = (r + i) % 8
        wire.send(cut.at[j], arrived.at[x, z, r], i, place.group + j)
    arrived[x, z, r] = cut[r]

    def owner(dy, other=False):
        c = 1 - place.c if other else place.c
        return (y + dy) % 4 * 2 + c

    def window(l, down, rank, part):
        if down:
            low, size = {None: (0, 192), 0: (0, 96), 1: (96, 96)}[part]
            return wdn.at[l, pl.ds(pl.multiple_of(rank * 192 + low, 16), size), :]
        cols = {None: pl.ds(0, 3072), 0: pl.ds(0, 1536), 1: pl.ds(1536, 1536)}[part]
        return win.at[l, pl.ds(pl.multiple_of(rank * 48, 16), 48), cols]

    local = []
    pieces = [(l, down) for l in range(LAYERS) for down in (False, True)]
    base = {piece: 8 + 9 * n for n, piece in enumerate(pieces)}
    for n, piece in enumerate(pieces):
        l, down = piece
        shard = (wdn_s if down else win_s).at[l]
        here = window(l, down, r, None)
        wire.send(shard, here, base[piece] + 0, place.yp)
        wire.send(shard, here, base[piece] + 1, place.ym)
        wire.send(shard, here, base[piece] + 4, place.partner)
        copy = pltpu.make_async_copy(shard, here, local_sem.at[n])
        copy.start()
        local.append(copy)

    def forward(piece):
        l, down = piece
        b = base[piece]
        left, right = owner(3), owner(1)
        wire.wait(window(l, down, left, None), b + 0, place.ym)
        half = window(l, down, left, 0)
        wire.send(half, half, b + 2, place.yp)
        whole = window(l, down, left, None)
        wire.send(whole, whole, b + 5, place.partner)
        wire.wait(window(l, down, right, None), b + 1, place.yp)
        half = window(l, down, right, 1)
        wire.send(half, half, b + 3, place.ym)
        whole = window(l, down, right, None)
        wire.send(whole, whole, b + 6, place.partner)

    def across(piece):
        l, down = piece
        b = base[piece]
        far = owner(2)
        for part, device in ((0, place.ym), (1, place.yp)):
            half = window(l, down, far, part)
            wire.wait(half, b + 2 + part, device)
            wire.send(half, half, b + 7 + part, place.partner)

    def settle(piece):
        l, down = piece
        b = base[piece]
        wire.wait(window(l, down, owner(0, True), None), b + 4, place.partner)
        wire.wait(window(l, down, owner(3, True), None), b + 5, place.partner)
        wire.wait(window(l, down, owner(1, True), None), b + 6, place.partner)
        for part in range(2):
            wire.wait(window(l, down, owner(2, True), part), b + 7 + part, place.partner)

    first, second, third, fourth, fifth = plane_gather(wire, place, arrived, IMG, 44)
    for i in range(1, 8):
        j = (r - i + 8) % 8
        wire.wait(arrived.at[x, z, j], i, place.group + j)
    first()
    second()
    forward(pieces[0])
    third()
    forward(pieces[1])
    fourth()
    across(pieces[0])
    forward(pieces[2])
    fifth()
    across(pieces[1])
    forward(pieces[3])
    across(pieces[2])
    across(pieces[3])
    for piece in pieces:
        settle(piece)
    for copy in local:
        copy.wait()
    wire.finish()


def gather(cut, win_s, wdn_s):
    return pl.pallas_call(
        gather_kernel,
        out_shape=[
            jax.ShapeDtypeStruct((4, 4, IMG, TOK, D), bf16),
            jax.ShapeDtypeStruct((LAYERS, D, 4 * D + FF), bf16),
            jax.ShapeDtypeStruct((LAYERS, FF, D), bf16),
        ],
        in_specs=[VMEM] * 3,
        out_specs=[VMEM, ANY, ANY],
        scratch_shapes=[
            pltpu.SemaphoreType.DMA((60,)),
            pltpu.SemaphoreType.DMA((60,)),
            pltpu.SemaphoreType.DMA((4,)),
        ],
        compiler_params=pltpu.CompilerParams(collective_id=0, has_side_effects=True, vmem_limit_bytes=16 << 20),
        name="gather",
    )(cut, win_s, wdn_s)


def add_rows(start, stop, step, body):
    def run(i, carry):
        body(pl.ds(pl.multiple_of(start + i * step, 16), step))
        return carry

    lax.fori_loop(0, (stop - start) // step, run, 0)


def reduce_kernel(packed, gcut, source, gin, gdn, gcls, own, swapped, mine, from_m, from_p, fin_p, fin_m, plane, picked, acc, send_sem, recv_sem):
    place = Place()
    x, z, y, c, r = place.x, place.z, place.y, place.c, place.r
    place.greet(True, True)
    wire = Wire(send_sem, recv_sem)
    A, B = pl.ds(0, CUT_A), pl.ds(CUT_A, PACK - CUT_A)

    def row(k, core):
        return (y + k) % 4 * 2 + core

    for k in (2, 1, 3, 0):
        wire.send(packed.at[row(k, 1 - c)], swapped.at[k], k, place.partner)
    plane[x, z] = gcut[...]
    first, second, third, fourth, fifth = plane_gather(wire, place, plane, CAP, 16)
    first()

    def combine(k):
        wire.wait(swapped.at[k], k, place.partner)

        def body(rows):
            total = packed[row(k, c), rows, :].astype(f32) + swapped[k, rows, :].astype(f32)
            mine[k, rows, :] = total.astype(bf16)

        add_rows(0, PACK, 48, body)

    combine(2)
    wire.send(mine.at[2, A], from_m, 4, place.yp)
    wire.send(mine.at[2, B], from_p, 5, place.ym)
    combine(1)
    wire.send(mine.at[1, B], fin_p.at[B], 6, place.yp)
    combine(3)
    wire.send(mine.at[3, A], fin_m.at[A], 7, place.ym)
    second()
    wire.wait(swapped.at[0], 0, place.partner)

    def start_own(rows):
        acc[rows, :] = packed[row(0, c), rows, :].astype(f32) + swapped[0, rows, :].astype(f32)

    add_rows(0, PACK, 48, start_own)
    third()
    wire.wait(from_m, 4, place.ym)

    def add_a(rows):
        mine[1, rows, :] = (mine[1, rows, :].astype(f32) + from_m[rows, :].astype(f32)).astype(bf16)

    add_rows(0, CUT_A, 48, add_a)
    wire.send(mine.at[1, A], fin_p.at[A], 8, place.yp)
    wire.wait(from_p, 5, place.yp)

    def add_b(i, carry):
        here = pl.ds(pl.multiple_of(i * 48, 16), 48)
        rows = pl.ds(pl.multiple_of(CUT_A + i * 48, 16), 48)
        mine[3, rows, :] = (mine[3, rows, :].astype(f32) + from_p[here, :].astype(f32)).astype(bf16)
        return carry

    lax.fori_loop(0, (PACK - CUT_A) // 48, add_b, 0)
    wire.send(mine.at[3, B], fin_m.at[B], 9, place.ym)
    fourth()
    fifth()
    for m in range(8):
        at = source[0, place.group + m]
        piece = plane[at // 64, at // 16 % 4, at % 16]
        picked[m] = piece
    own[r] = picked[r]
    for i in range(1, 8):
        m = (r + i) % 8
        wire.send(picked.at[m], own.at[r], 32 + i, place.group + m)
    wire.wait(fin_p.at[B], 6, place.ym)
    wire.wait(fin_m.at[A], 7, place.yp)
    wire.wait(fin_p.at[A], 8, place.ym)
    wire.wait(fin_m.at[B], 9, place.yp)

    def total(first_row, rows):
        at = pl.ds(first_row, rows)
        return acc[at, :] + fin_p[at, :].astype(f32) + fin_m[at, :].astype(f32)

    for l in range(LAYERS):
        for b in range(8):
            gin[l, :, D * b : D * b + D] = total(576 * l + 48 * b, 48)
        for b in range(4):
            gdn[l, 48 * b : 48 * b + 48, :] = total(576 * l + D + 48 * b, 48)
    gcls[...] = total(PACK - 48, 48)[:, 0:CLASSES]
    for i in range(1, 8):
        j = (r - i + 8) % 8
        wire.wait(own.at[j], 32 + i, place.group + j)
    wire.finish()


def reduce(packed, gcut, source):
    return pl.pallas_call(
        reduce_kernel,
        out_shape=[
            jax.ShapeDtypeStruct((LAYERS, 48, 4 * D + FF), f32),
            jax.ShapeDtypeStruct((LAYERS, 192, D), f32),
            jax.ShapeDtypeStruct((48, CLASSES), f32),
            jax.ShapeDtypeStruct((IMG, TOK, D), bf16),
        ],
        in_specs=[VMEM, VMEM, SMEM],
        out_specs=[VMEM] * 4,
        scratch_shapes=[
            pltpu.VMEM((4, PACK, D), bf16),
            pltpu.VMEM((4, PACK, D), bf16),
            pltpu.VMEM((CUT_A, D), bf16),
            pltpu.VMEM((PACK - CUT_A, D), bf16),
            pltpu.VMEM((PACK, D), bf16),
            pltpu.VMEM((PACK, D), bf16),
            pltpu.VMEM((4, 4, CAP, TOK, D), bf16),
            pltpu.VMEM((IMG, TOK, D), bf16),
            pltpu.VMEM((PACK, D), f32),
            pltpu.SemaphoreType.DMA((40,)),
            pltpu.SemaphoreType.DMA((40,)),
        ],
        compiler_params=pltpu.CompilerParams(collective_id=1, has_side_effects=True, vmem_limit_bytes=56 << 20),
        name="reduce",
    )(packed, gcut, source)


def client_reduce_kernel(packed, out, swapped, mine, hop_x, hop_z, fin_x, fin_z, half_x, half_z, hop2_x, hop2_z, fin2_x, fin2_z, last, ring, send_sem, recv_sem):
    place = Place()
    x, z, y, c, r = place.x, place.z, place.y, place.c, place.r
    place.greet(True, True)
    wire = Wire(send_sem, recv_sem)
    for q in range(4):
        wire.send(packed.at[pl.ds(4 * q, 4), 1 - c], swapped.at[pl.ds(4 * q, 4)], q, place.partner)
    for q in range(4):
        wire.wait(swapped.at[pl.ds(4 * q, 4)], q, place.partner)
        for i in range(4):
            at = 4 * q + i
            mine[q, i] = (packed[at, c].astype(f32) + swapped[at].astype(f32)).astype(bf16)

    X, Z = pl.ds(0, 80), pl.ds(80, 80)

    def src_x(k, part=None):
        to = (x + k) % 4
        if part is None:
            return mine.at[to, :, X]
        return mine.at[to, pl.ds(2 * part, 2), X]

    def src_z(k, part=None):
        to = (z + k) % 4
        if part is None:
            return mine.at[:, to, Z]
        return mine.at[pl.ds(2 * part, 2), to, Z]

    def ring_one(src, hop, fin, up, down, k0):
        wire.send(src(2, 0), hop.at[0], k0, up)
        wire.send(src(2, 1), hop.at[1], k0 + 1, down)
        wire.send(src(1, 1), fin.at[0, pl.ds(2, 2)], k0 + 2, up)
        wire.send(src(3, 0), fin.at[1, pl.ds(0, 2)], k0 + 3, down)

    def ring_two(src, load, hop, fin, up, down, k0):
        wire.wait(hop.at[0], k0, down)
        load(1, 0, hop)
        wire.send(src(1, 0), fin.at[0, pl.ds(0, 2)], k0 + 4, up)
        wire.wait(hop.at[1], k0 + 1, up)
        load(3, 1, hop)
        wire.send(src(3, 1), fin.at[1, pl.ds(2, 2)], k0 + 5, down)

    def ring_three(fin, up, down, k0):
        wire.wait(fin.at[0, pl.ds(2, 2)], k0 + 2, down)
        wire.wait(fin.at[1, pl.ds(0, 2)], k0 + 3, up)
        wire.wait(fin.at[0, pl.ds(0, 2)], k0 + 4, down)
        wire.wait(fin.at[1, pl.ds(2, 2)], k0 + 5, up)

    def load_x(k, part, hop):
        to = (x + k) % 4
        for i in range(2):
            at = 2 * part + i
            mine[to, at, 0:80] = (mine[to, at, 0:80].astype(f32) + hop[part, i].astype(f32)).astype(bf16)

    def load_z(k, part, hop):
        to = (z + k) % 4
        for i in range(2):
            at = 2 * part + i
            mine[at, to, 80:160] = (mine[at, to, 80:160].astype(f32) + hop[part, i].astype(f32)).astype(bf16)

    ring_one(src_x, hop_x, fin_x, place.xp, place.xm, 4)
    ring_one(src_z, hop_z, fin_z, place.zp, place.zm, 10)
    ring_two(src_x, load_x, hop_x, fin_x, place.xp, place.xm, 4)
    ring_two(src_z, load_z, hop_z, fin_z, place.zp, place.zm, 10)
    ring_three(fin_x, place.xp, place.xm, 4)
    for i in range(4):
        half_x[i] = (mine[x, i, 0:80].astype(f32) + fin_x[0, i].astype(f32) + fin_x[1, i].astype(f32)).astype(bf16)
    ring_three(fin_z, place.zp, place.zm, 10)
    for i in range(4):
        half_z[i] = (mine[i, z, 80:160].astype(f32) + fin_z[0, i].astype(f32) + fin_z[1, i].astype(f32)).astype(bf16)

    for k in range(1, 4):
        wire.send(half_x.at[(z + k) % 4], fin2_x.at[k - 1], 15 + k, place.at(0, k, 0))
        wire.send(half_z.at[(x + k) % 4], fin2_z.at[k - 1], 18 + k, place.at(k, 0, 0))
    for k in range(1, 4):
        wire.wait(fin2_x.at[k - 1], 15 + k, place.at(0, 4 - k, 0))
        wire.wait(fin2_z.at[k - 1], 18 + k, place.at(4 - k, 0, 0))
    top = half_x[z].astype(f32)
    low = half_z[x].astype(f32)
    for k in range(3):
        top = top + fin2_x[k].astype(f32)
        low = low + fin2_z[k].astype(f32)
    last[y, c, 0:80] = top.astype(bf16)
    last[y, c, 80:160] = low.astype(bf16)

    wire.send(last.at[y, c], last.at[y, c], 22, place.yp)
    wire.send(last.at[y, c], last.at[y, c], 23, place.ym)
    wire.send(last.at[y, c], last.at[y, c], 24, place.partner)
    left, right, far = (y + 3) % 4, (y + 1) % 4, (y + 2) % 4
    lo, hi = pl.ds(0, 80), pl.ds(80, 80)
    wire.wait(last.at[left, c], 22, place.ym)
    wire.send(last.at[left, c, lo], last.at[left, c, lo], 25, place.yp)
    wire.send(last.at[left, c], last.at[left, c], 27, place.partner)
    wire.wait(last.at[right, c], 23, place.yp)
    wire.send(last.at[right, c, hi], last.at[right, c, hi], 26, place.ym)
    wire.send(last.at[right, c], last.at[right, c], 28, place.partner)
    wire.wait(last.at[far, c, lo], 25, place.ym)
    wire.send(last.at[far, c, lo], last.at[far, c, lo], 29, place.partner)
    wire.wait(last.at[far, c, hi], 26, place.yp)
    wire.send(last.at[far, c, hi], last.at[far, c, hi], 30, place.partner)
    o = 1 - c
    wire.wait(last.at[y, o], 24, place.partner)
    wire.wait(last.at[left, o], 27, place.partner)
    wire.wait(last.at[right, o], 28, place.partner)
    wire.wait(last.at[far, o, lo], 29, place.partner)
    wire.wait(last.at[far, o, hi], 30, place.partner)
    for core in range(2):
        total = last[0, core].astype(f32)
        for k in range(1, 4):
            total = total + last[k, core].astype(f32)
        ring[160 * core : 160 * core + 160, :] = total
    col, line = iota((320, 128), 1), iota((320, 128), 0)
    wanted = jnp.where(
        col < 24,
        24 * r + col,
        jnp.where(col < 36, 192 + 24 * ((col - 24) // 3) + 3 * r + (col - 24) % 3, 288 + 3 * r + col - 36),
    )
    pick = ((line == wanted) & (col < 39)).astype(f32)
    out[...] = lax.dot_general(
        ring[...], pick, (((0,), (0,)), ((), ())), precision=lax.Precision.HIGHEST, preferred_element_type=f32
    )
    wire.finish()


def client_reduce(packed):
    return pl.pallas_call(
        client_reduce_kernel,
        out_shape=jax.ShapeDtypeStruct((D, 128), f32),
        in_specs=[VMEM],
        out_specs=VMEM,
        scratch_shapes=[
            pltpu.VMEM((16, 160, D), bf16),
            pltpu.VMEM((4, 4, 160, D), bf16),
            pltpu.VMEM((2, 2, 80, D), bf16),
            pltpu.VMEM((2, 2, 80, D), bf16),
            pltpu.VMEM((2, 4, 80, D), bf16),
            pltpu.VMEM((2, 4, 80, D), bf16),
            pltpu.VMEM((4, 80, D), bf16),
            pltpu.VMEM((4, 80, D), bf16),
            pltpu.VMEM((8, 128), f32),
            pltpu.VMEM((8, 128), f32),
            pltpu.VMEM((3, 80, D), bf16),
            pltpu.VMEM((3, 80, D), bf16),
            pltpu.VMEM((4, 2, 160, D), bf16),
            pltpu.VMEM((320, D), f32),
            pltpu.SemaphoreType.DMA((32,)),
            pltpu.SemaphoreType.DMA((32,)),
        ],
        compiler_params=pltpu.CompilerParams(collective_id=2, has_side_effects=True, vmem_limit_bytes=56 << 20),
        name="client_reduce",
    )(packed)


def per_device(patches, labels, assign, patch_embed, positions, client_in, client_down, server_in, server_down, classifier):
    win_c, wdn_c = client_in[None], client_down[None]
    cut, *saved = client_forward(patches, patch_embed, positions, win_c, wdn_c)
    arrived, win, wdn = gather(cut.reshape(IMG, TOK, D), server_in, server_down)
    losses, packed, gcut, source = server(
        arrived.reshape(2048, D), assign, assign.reshape(1, 128), labels.reshape(128, IMG), win, wdn, classifier
    )
    gin, gdn, gcls, own = reduce(packed, gcut.reshape(CAP, TOK, D), source)
    packed_c = client_backward(own.reshape(128, D), patches, win_c, wdn_c, saved)
    cols = client_reduce(packed_c)
    grad_down = jnp.concatenate([cols[:, 24 + 3 * q : 27 + 3 * q] for q in range(4)], axis=0)
    return (
        losses,
        cols[:192, 36:39],
        cols[192:208, 36:39],
        cols[:, :24],
        grad_down,
        gin,
        gdn,
        gcls,
    )


def solution(mesh):
    in_specs = (
        P("client", None),
        P(),
        P(),
        P(),
        P(),
        P(),
        P(),
        P(None, "client", None),
        P(None, "client", None),
        P(),
    )
    out_specs = (
        P("client", None),
        P(None, "client"),
        P(None, "client"),
        P(None, "client"),
        P(None, "client"),
        P(None, "client", None),
        P(None, "client", None),
        P("client", None),
    )
    return jax.shard_map(per_device, mesh=mesh, in_specs=in_specs, out_specs=out_specs, check_vma=False)
```

```python
import math

import jax
import jax.numpy as jnp
from jax import lax
from jax.experimental import pallas as pl
from jax.experimental.pallas import tpu as pltpu
from jax.sharding import PartitionSpec as P

D = 384
FF = 1536
TOK = 16
IMG = 8
CLASSES = 10
LAYERS = 2
CAP = 16
EPSILON = 1e-06
SCALE = 0.125
GELU_A = math.sqrt(2.0 / math.pi)
GELU_B = 0.044715
PACK = LAYERS * (D + FF // 8) + D // 8
CUT_A = 576
MAIN = 96
TAIL = 80
BLOCK = MAIN + TAIL

bf16 = jnp.bfloat16
f32 = jnp.float32
MESH = pl.DeviceIdType.MESH
VMEM = pl.BlockSpec(memory_space=pltpu.VMEM)
SMEM = pl.BlockSpec(memory_space=pltpu.SMEM)
ANY = pl.BlockSpec(memory_space=pl.ANY)


def mm(a, b, ca=1, cb=0):
    return lax.dot_general(a, b, (((ca,), (cb,)), ((), ())), preferred_element_type=f32)


def iota(shape, dim):
    return lax.broadcasted_iota(jnp.int32, shape, dim)


def norm(v):
    centre = v - jnp.mean(v, axis=-1, keepdims=True)
    rstd = lax.rsqrt(jnp.mean(centre * centre, axis=-1, keepdims=True) + EPSILON)
    return centre * rstd, rstd


def norm_back(v, grad):
    hat, rstd = norm(v)
    along = jnp.mean(grad * hat, axis=-1, keepdims=True)
    return rstd * (grad - jnp.mean(grad, axis=-1, keepdims=True) - hat * along)


def rounded(v):
    return v.astype(bf16).astype(f32)


def head_masks(rows):
    low = (iota((rows, 128), 1) < 64).astype(f32)
    return low.astype(bf16), (1.0 - low).astype(bf16)


def two_heads(v):
    low, high = head_masks(v.shape[0])
    return jnp.concatenate([v * low, v * high], axis=0)


def merge_heads(v):
    rows = v.shape[0] // 2
    return jnp.where(iota((rows, 128), 1) < 64, v[:rows], v[rows:])


def block_forward(l, rows, S, win, wdn):
    x = S["x"][l]
    hat, _ = norm(x)
    u1 = hat.astype(bf16)
    S["u1"][l] = u1
    for n in range(3):
        cols = slice(D * n, D * n + D)
        S["qkv"][l, :, cols] = mm(u1, win[l, :, cols]).astype(bf16)
    same = ((iota((256, 128), 0) & 127) >> 4) == (iota((256, 128), 1) >> 4)
    for g in range(rows // 128):
        part = slice(128 * g, 128 * g + 128)
        for p in range(3):
            q2 = S["qkv"][l, part, 128 * p : 128 * p + 128]
            k2 = S["qkv"][l, part, D + 128 * p : D + 128 * p + 128]
            v2 = S["qkv"][l, part, 2 * D + 128 * p : 2 * D + 128 * p + 128]
            scores = mm(two_heads(q2), k2, 1, 1) * SCALE
            scores = jnp.where(same, scores, -1e30)
            grown = jnp.exp(scores - jnp.max(scores, axis=-1, keepdims=True))
            prob = grown / jnp.sum(grown, axis=-1, keepdims=True)
            S["prob"][l, 3 * g + p] = prob
            S["att"][l, part, 128 * p : 128 * p + 128] = merge_heads(mm(prob.astype(bf16), v2)).astype(bf16)
    x1 = S["x"][l] + mm(S["att"][l], win[l, :, 3 * D : 4 * D])
    S["x1"][l] = x1
    hat, _ = norm(x1)
    u2 = hat.astype(bf16)
    S["u2"][l] = u2
    for n in range(4):
        pre = mm(u2, win[l, :, 4 * D + D * n : 5 * D + D * n])
        S["pre"][l, :, D * n : D * n + D] = pre
        bent = jnp.tanh(GELU_A * (pre + GELU_B * pre * pre * pre))
        S["h"][l, :, D * n : D * n + D] = (0.5 * pre * (1.0 + bent)).astype(bf16)
    return S["x1"][l] + mm(S["h"][l], wdn[l])


def block_backward(l, rows, S, win, wdn, dy_ref):
    dyb = dy_ref[...].astype(bf16)
    S["dyb"][l] = dyb
    for n in range(4):
        cols = slice(D * n, D * n + D)
        dh = rounded(mm(dyb, wdn[l, cols, :], 1, 1))
        pre = S["pre"][l, :, cols]
        bent = jnp.tanh(GELU_A * (pre + GELU_B * pre * pre * pre))
        slope = 0.5 * (1.0 + bent) + 0.5 * pre * (1.0 - bent * bent) * GELU_A * (1.0 + 3.0 * GELU_B * pre * pre)
        S["dpre"][l, :, cols] = (dh * slope).astype(bf16)
    du2 = rounded(mm(S["dpre"][l], win[l, :, 4 * D :], 1, 1))
    dx1 = dy_ref[...] + norm_back(S["x1"][l], du2)
    dy_ref[...] = dx1
    dx1b = dx1.astype(bf16)
    S["dx1b"][l] = dx1b
    S["datt"][...] = mm(dx1b, win[l, :, 3 * D : 4 * D], 1, 1).astype(bf16)
    for g in range(rows // 128):
        part = slice(128 * g, 128 * g + 128)
        for p in range(3):
            cq = slice(128 * p, 128 * p + 128)
            ck = slice(D + 128 * p, D + 128 * p + 128)
            cv = slice(2 * D + 128 * p, 2 * D + 128 * p + 128)
            qs = two_heads(S["qkv"][l, part, cq])
            dos = two_heads(S["datt"][part, cq])
            prob = S["prob"][l, 3 * g + p]
            dprob = mm(dos, S["qkv"][l, part, cv], 1, 1)
            dscore = prob * (dprob - jnp.sum(prob * dprob, axis=-1, keepdims=True)) * SCALE
            dsb = dscore.astype(bf16)
            S["dqkv"][l, part, cq] = merge_heads(mm(dsb, S["qkv"][l, part, ck])).astype(bf16)
            S["dqkv"][l, part, ck] = mm(dsb, qs, 0, 0).astype(bf16)
            S["dqkv"][l, part, cv] = mm(prob.astype(bf16), dos, 0, 0).astype(bf16)
    du1 = rounded(mm(S["dqkv"][l], win[l, :, : 3 * D], 1, 1))
    dy_ref[...] = dy_ref[...] + norm_back(S["x"][l], du1)


def weight_pairs(S, l):
    pairs = []
    for n in range(3):
        pairs.append((n, S["u1"].at[l], S["dqkv"].at[l, :, pl.ds(D * n, D)]))
    pairs.append((3, S["att"].at[l], S["dx1b"].at[l]))
    for n in range(4):
        pairs.append((4 + n, S["u2"].at[l], S["dpre"].at[l, :, pl.ds(D * n, D)]))
    return pairs


def block_shapes(layers, rows):
    return dict(
        x=((layers + 1, rows, D), f32),
        x1=((layers, rows, D), f32),
        u1=((layers, rows, D), bf16),
        u2=((layers, rows, D), bf16),
        qkv=((layers, rows, 3 * D), bf16),
        prob=((layers, 3 * rows // 128, 256, 128), f32),
        att=((layers, rows, D), bf16),
        pre=((layers, rows, FF), f32),
        h=((layers, rows, FF), bf16),
        dyb=((layers, rows, D), bf16),
        dpre=((layers, rows, FF), bf16),
        dx1b=((layers, rows, D), bf16),
        datt=((rows, D), bf16),
        dqkv=((layers, rows, 3 * D), bf16),
        dy=((rows, D), f32),
    )


class Place:
    def __init__(self):
        me = lax.axis_index("client")
        self.me = me
        self.c, self.y, self.z, self.x = me % 2, me // 2 % 4, me // 8 % 4, me // 32
        self.r, self.group = me % 8, me // 8 * 8
        self.partner = me + 1 - 2 * self.c
        self.yp, self.ym = self.at(0, 0, 1), self.at(0, 0, 3)
        self.xp, self.xm = self.at(1, 0, 0), self.at(3, 0, 0)
        self.zp, self.zm = self.at(0, 1, 0), self.at(0, 3, 0)

    def at(self, dx, dz, dy):
        x, z, y = (self.x + dx) % 4, (self.z + dz) % 4, (self.y + dy) % 4
        return ((x * 4 + z) * 4 + y) * 2 + self.c

    def greet(self, group, plane):
        peers = []
        if group:
            peers += [self.group + (self.r + i) % 8 for i in range(1, 8)]
        if plane:
            peers += [self.xp, self.xm, self.zp, self.zm]
        barrier = pltpu.get_barrier_semaphore()
        for peer in peers:
            pl.semaphore_signal(barrier, inc=1, device_id=(peer,), device_id_type=MESH)
        pl.semaphore_wait(barrier, len(peers))


class Wire:
    def __init__(self, send_sem, recv_sem):
        self.send_sem, self.recv_sem, self.sent = send_sem, recv_sem, []

    def make(self, src, dst, k, device):
        return pltpu.make_async_remote_copy(
            src_ref=src,
            dst_ref=dst,
            send_sem=self.send_sem.at[k],
            recv_sem=self.recv_sem.at[k],
            device_id=(device,),
            device_id_type=MESH,
        )

    def send(self, src, dst, k, device):
        copy = self.make(src, dst, k, device)
        copy.start()
        self.sent.append(copy)

    def wait(self, landed, k, device):
        self.make(landed, landed, k, device).wait_recv()

    def finish(self):
        for copy in self.sent:
            copy.wait_send()


def plane_gather(wire, place, buf, count, k0):
    half, quarter = count // 2, count // 4
    x, z = place.x, place.z
    xm, xp, zm, zp = (x + 3) % 4, (x + 1) % 4, (z + 3) % 4, (z + 1) % 4
    xo, zo = (x + 2) % 4, (z + 2) % 4
    X, XA, XB = pl.ds(0, half), pl.ds(0, quarter), pl.ds(quarter, quarter)
    Z, ZA, ZB = pl.ds(half, half), pl.ds(half, quarter), pl.ds(half + quarter, quarter)

    def both(ref, k, device):
        wire.send(ref, ref, k0 + k, device)

    def first():
        both(buf.at[x, z, X], 0, place.xp)
        both(buf.at[x, z, X], 1, place.xm)
        both(buf.at[x, z, Z], 2, place.zp)
        both(buf.at[x, z, Z], 3, place.zm)

    def second():
        wire.wait(buf.at[xm, z, X], k0 + 0, place.xm)
        both(buf.at[xm, z, XA], 4, place.xp)
        wire.wait(buf.at[xp, z, X], k0 + 1, place.xp)
        both(buf.at[xp, z, XB], 5, place.xm)
        wire.wait(buf.at[x, zm, Z], k0 + 2, place.zm)
        both(buf.at[x, zm, ZA], 6, place.zp)
        wire.wait(buf.at[x, zp, Z], k0 + 3, place.zp)
        both(buf.at[x, zp, ZB], 7, place.zm)

    def third():
        wire.wait(buf.at[xo, z, XA], k0 + 4, place.xm)
        wire.wait(buf.at[xo, z, XB], k0 + 5, place.xp)
        both(buf.at[:, z, X], 8, place.zp)
        both(buf.at[:, z, X], 9, place.zm)
        wire.wait(buf.at[x, zo, ZA], k0 + 6, place.zm)
        wire.wait(buf.at[x, zo, ZB], k0 + 7, place.zp)
        both(buf.at[x, :, Z], 10, place.xp)
        both(buf.at[x, :, Z], 11, place.xm)

    def fourth():
        wire.wait(buf.at[:, zm, X], k0 + 8, place.zm)
        both(buf.at[0:2, zm, X], 12, place.zp)
        wire.wait(buf.at[:, zp, X], k0 + 9, place.zp)
        both(buf.at[2:4, zp, X], 13, place.zm)
        wire.wait(buf.at[xm, :, Z], k0 + 10, place.xm)
        both(buf.at[xm, 0:2, Z], 14, place.xp)
        wire.wait(buf.at[xp, :, Z], k0 + 11, place.xp)
        both(buf.at[xp, 2:4, Z], 15, place.xm)

    def fifth():
        wire.wait(buf.at[0:2, zo, X], k0 + 12, place.zm)
        wire.wait(buf.at[2:4, zo, X], k0 + 13, place.zp)
        wire.wait(buf.at[xo, 0:2, Z], k0 + 14, place.xm)
        wire.wait(buf.at[xo, 2:4, Z], k0 + 15, place.xp)

    return first, second, third, fourth, fifth


def add_rows(start, stop, step, body):
    def run(i, carry):
        body(pl.ds(pl.multiple_of(start + i * step, 16), step))
        return carry

    lax.fori_loop(0, (stop - start) // step, run, 0)


def route(arow, labels, shard, rank_in):
    eye = iota((128, 128), 0) == iota((128, 128), 1)
    acol = jnp.sum(jnp.where(eye, arow.astype(f32), 0.0), axis=1, keepdims=True).astype(jnp.int32)
    earlier = (acol == arow) & (iota((128, 128), 0) < iota((128, 128), 1))
    rank = jnp.sum(earlier.astype(f32), axis=0, keepdims=True).astype(jnp.int32)
    chosen = (jnp.broadcast_to(arow, (CAP, 128)) == shard) & (
        jnp.broadcast_to(rank, (CAP, 128)) == iota((CAP, 128), 0)
    )
    selector = chosen.astype(f32).astype(bf16)
    take = (iota((128, 16), 0) == iota((128, 16), 1) * IMG + rank_in).astype(f32).astype(bf16)
    by_row = mm(labels.astype(f32).astype(bf16), take).astype(bf16)
    lift = ((iota((128, 8), 0) >> 4) == iota((128, 8), 1)).astype(f32).astype(bf16)
    tall = mm(lift, by_row)
    mine = (iota((128, 16), 0) & 15) == iota((128, 16), 1)
    label = jnp.sum(jnp.where(mine, tall, 0.0), axis=1, keepdims=True)
    onehot = (label == iota((128, CLASSES), 1).astype(f32)).astype(f32).astype(bf16)
    return selector, mm(selector, onehot)


def slot_rows(selector, arrived):
    spread = (iota((128, 2048), 0) == (iota((128, 2048), 1) >> 4)).astype(f32).astype(bf16)
    wide = mm(selector, spread).astype(bf16)
    repeat = ((iota((256, CAP), 0) >> 4) == iota((256, CAP), 1)).astype(f32).astype(bf16)
    tall = mm(repeat, wide)
    same = (iota((256, 2048), 0) & 15) == (iota((256, 2048), 1) & 15)
    return mm(jnp.where(same, tall, 0.0).astype(bf16), arrived)


def head_loss(last, classes, hot):
    filled = jnp.sum(hot, axis=1, keepdims=True)
    mean = jnp.mean(last.reshape(CAP, TOK, D), axis=1)
    hat, _ = norm(mean)
    pooled = hat.astype(bf16)
    logits = mm(pooled, classes, 1, 1)
    top = jnp.max(logits, axis=1, keepdims=True)
    grown = jnp.exp(logits - top)
    total = jnp.sum(grown, axis=1, keepdims=True)
    per = (jnp.log(total) + top - jnp.sum(hot * logits, axis=1, keepdims=True)) * filled
    eye = iota((CAP, CAP), 0) == iota((CAP, CAP), 1)
    losses = jnp.sum(jnp.where(eye, per, 0.0), axis=0, keepdims=True)
    dlogits = ((grown / total) * filled - hot).astype(bf16)
    gcls = mm(pooled, dlogits, 0, 0).astype(bf16)
    dpooled = rounded(mm(dlogits, classes))
    dmean = norm_back(mean, dpooled) * (1.0 / TOK)
    dlast = jnp.broadcast_to(dmean[:, None, :], (CAP, TOK, D)).reshape(CAP * TOK, D)
    return losses, gcls, dlast


CLIENT = block_shapes(1, 128)
SERVER = block_shapes(LAYERS, 256)
BUFFERS = dict(
    arrived=((4, 4, IMG, TOK, D), bf16),
    win=((LAYERS, D, 4 * D + FF), bf16),
    wdn=((LAYERS, FF, D), bf16),
    cls=((CLASSES, D), bf16),
    cut=((IMG, TOK, D), bf16),
    packed=((8, PACK, D), bf16),
    swapped=((4, PACK, D), bf16),
    from_m=((CUT_A, D), bf16),
    from_p=((PACK - CUT_A, D), bf16),
    fin_p=((PACK, D), bf16),
    fin_m=((PACK, D), bf16),
    line_x=((4, 8, TOK, D), bf16),
    line_z=((4, 8, TOK, D), bf16),
    pick_x=((4, 8, TOK, D), bf16),
    pick_z=((4, 8, TOK, D), bf16),
    got_x=((3, 8, TOK, D), bf16),
    got_z=((3, 8, TOK, D), bf16),
    picked=((8, TOK, D), bf16),
    own=((IMG, TOK, D), bf16),
    order=((D, 512), bf16),
    dperm=((128, 512), bf16),
    pp=((128, D), bf16),
    cpack=((16, 2, BLOCK, D), bf16),
    cswap=((16, BLOCK, D), bf16),
    cmine=((4, 4, BLOCK, D), bf16),
    hop_x=((2, 2, MAIN, D), bf16),
    hop_z=((2, 2, TAIL, D), bf16),
    end_x=((2, 4, MAIN, D), bf16),
    end_z=((2, 4, TAIL, D), bf16),
    half_x=((4, MAIN, D), bf16),
    half_z=((4, TAIL, D), bf16),
    two_x=((3, MAIN, D), bf16),
    two_z=((3, TAIL, D), bf16),
    low_x=((4, 24, D), bf16),
    low_z=((4, 16, D), bf16),
    three_x=((3, 24, D), bf16),
    three_z=((3, 16, D), bf16),
)
N_SEM = 160


def step_kernel(patches_t, embed, positions, win_c, wdn_c, win_s, wdn_s, arow, labels, source, classes, *refs):
    losses, gin, gdn, gcls_out, out_in, out_dn, out_pe, out_pos = refs[:8]
    refs = list(refs[8:])
    C = dict(zip(CLIENT, refs[: len(CLIENT)]))
    refs = refs[len(CLIENT) :]
    S = dict(zip(SERVER, refs[: len(SERVER)]))
    refs = refs[len(SERVER) :]
    B = dict(zip(BUFFERS, refs[: len(BUFFERS)]))
    send_sem, recv_sem, local_sem = refs[len(BUFFERS) :]
    place = Place()
    x, z, y, c, r = place.x, place.z, place.y, place.c, place.r
    shard = place.me // 8
    win, wdn, arrived, packed = B["win"], B["wdn"], B["arrived"], B["packed"]
    place.greet(True, True)
    wire = Wire(send_sem, recv_sem)

    def owner(dy, other=False):
        return (y + dy) % 4 * 2 + (1 - c if other else c)

    def window(l, down, rank, part):
        if down:
            low, size = {None: (0, 192), 0: (0, 96), 1: (96, 96)}[part]
            return wdn.at[l, pl.ds(pl.multiple_of(rank * 192 + low, 16), size), :]
        cols = {None: pl.ds(0, 3072), 0: pl.ds(0, 1536), 1: pl.ds(1536, 1536)}[part]
        return win.at[l, pl.ds(pl.multiple_of(rank * 48, 16), 48), cols]

    pieces = [(l, down) for l in range(LAYERS) for down in (False, True)]
    base = {piece: 8 + 9 * n for n, piece in enumerate(pieces)}
    for piece in pieces:
        l, down = piece
        mine = (wdn_s if down else win_s).at[l]
        here = window(l, down, r, None)
        wire.send(mine, here, base[piece] + 0, place.yp)
        wire.send(mine, here, base[piece] + 1, place.ym)
        wire.send(mine, here, base[piece] + 4, place.partner)
        here[...] = mine[...]
    copy = pltpu.make_async_copy(classes.at[shard], B["cls"], local_sem)
    copy.start()

    def forward(piece):
        l, down = piece
        b = base[piece]
        left, right = owner(3), owner(1)
        whole, half = window(l, down, left, None), window(l, down, left, 0)
        wire.wait(whole, b + 0, place.ym)
        wire.send(half, half, b + 2, place.yp)
        wire.send(whole, whole, b + 5, place.partner)
        whole, half = window(l, down, right, None), window(l, down, right, 1)
        wire.wait(whole, b + 1, place.yp)
        wire.send(half, half, b + 3, place.ym)
        wire.send(whole, whole, b + 6, place.partner)

    def across(piece):
        l, down = piece
        b = base[piece]
        for part, device in ((0, place.ym), (1, place.yp)):
            half = window(l, down, owner(2), part)
            wire.wait(half, b + 2 + part, device)
            wire.send(half, half, b + 7 + part, place.partner)

    def settle(piece):
        l, down = piece
        b = base[piece]
        wire.wait(window(l, down, owner(0, True), None), b + 4, place.partner)
        wire.wait(window(l, down, owner(3, True), None), b + 5, place.partner)
        wire.wait(window(l, down, owner(1, True), None), b + 6, place.partner)
        for part in range(2):
            wire.wait(window(l, down, owner(2, True), part), b + 7 + part, place.partner)

    tiled = jnp.concatenate([positions[...].astype(f32)] * IMG, axis=0)
    C["x"][0] = mm(patches_t[...], embed[...], 0, 0) + tiled
    cut = block_forward(0, 128, C, win_c, wdn_c).astype(bf16)
    B["cut"][...] = cut.reshape(IMG, TOK, D)
    for i in range(1, 8):
        j = (r + i) % 8
        wire.send(B["cut"].at[j], arrived.at[x, z, r], i, place.group + j)
    arrived[x, z, r] = B["cut"][r]
    first, second, third, fourth, fifth = plane_gather(wire, place, arrived, IMG, 44)
    forward(pieces[0])
    for i in range(1, 8):
        j = (r - i + 8) % 8
        wire.wait(arrived.at[x, z, j], i, place.group + j)
    first()
    forward(pieces[1])
    second()
    selector, hot = route(arow[...], labels[...], shard, r)
    col = iota((1, 512), 1)
    at = col & 15
    wanted = ((col >> 4) & 15) * 24 + (at // 3) * 6 + (col >> 8) * 3 + at % 3
    B["order"][...] = ((iota((D, 512), 0) == wanted) & (at < 12)).astype(f32).astype(bf16)
    B["pp"][...] = (iota((128, D), 1) - 256 == (iota((128, D), 0) & 15)).astype(f32).astype(bf16)
    B["pp"][:, 0:192] = patches_t[...].T
    packed[:, PACK - 48 :, :] = jnp.zeros((8, 48, D), bf16)
    third()
    across(pieces[0])
    forward(pieces[2])
    across(pieces[1])
    fourth()
    forward(pieces[3])
    fifth()
    across(pieces[2])
    settle(pieces[0])
    settle(pieces[1])

    S["x"][0] = slot_rows(selector, arrived[...].reshape(2048, D))
    S["x"][1] = block_forward(0, 256, S, win, wdn)
    across(pieces[3])
    settle(pieces[2])
    settle(pieces[3])
    S["x"][2] = block_forward(1, 256, S, win, wdn)
    copy.wait()
    loss, gcls, dlast = head_loss(S["x"][LAYERS], B["cls"][...], hot)
    losses[...] = loss
    for k in range(8):
        packed[k, PACK - 48 :, 0:CLASSES] = gcls[48 * k : 48 * k + 48]
    S["dy"][...] = dlast

    def backward(i, carry):
        block_backward(LAYERS - 1 - i, 256, S, win, wdn, S["dy"])
        return carry

    lax.fori_loop(0, LAYERS, backward, 0)

    line_x, line_z = B["line_x"], B["line_z"]
    gcut = S["dy"][...].astype(bf16).reshape(CAP, TOK, D)
    line_x[x] = gcut[:8]
    line_z[z] = gcut[8:]
    lo, hi, all8 = pl.ds(0, 4), pl.ds(4, 4), pl.ds(0, 8)
    lines = ((line_x, x, place.xp, place.xm, 60), (line_z, z, place.zp, place.zm, 64))
    for buf, me, up, down, k0 in lines:
        wire.send(buf.at[me], buf.at[me], k0, up)
        wire.send(buf.at[me], buf.at[me], k0 + 1, down)

    def server_weights(l):
        for b, u, dout in weight_pairs(S, l):
            val = mm(u[...], dout[...], 0, 0).astype(bf16)
            for k in range(8):
                packed[k, 576 * l + 48 * b : 576 * l + 48 * b + 48, :] = val[48 * k : 48 * k + 48]
        for n in range(4):
            val = mm(S["h"][l, :, D * n : D * n + D], S["dyb"][l], 0, 0).astype(bf16)
            for j in range(2):
                packed[2 * n + j, 576 * l + D : 576 * l + 576, :] = val[192 * j : 192 * j + 192]

    rows_a, rows_b = pl.ds(0, CUT_A), pl.ds(CUT_A, PACK - CUT_A)

    def row(k, core):
        return (y + k) % 4 * 2 + core

    def swap(part, k0):
        for k in (2, 1, 3, 0):
            wire.send(packed.at[row(k, 1 - c), part], B["swapped"].at[k, part], k0 + k, place.partner)

    def combine(k, part, k0, start, stop):
        wire.wait(B["swapped"].at[k, part], k0 + k, place.partner)

        def body(rows):
            total = packed[row(k, c), rows, :].astype(f32) + B["swapped"][k, rows, :].astype(f32)
            packed[row(k, c), rows, :] = total.astype(bf16)

        add_rows(start, stop, 48, body)

    def combine_a(k):
        combine(k, rows_a, 80, 0, CUT_A)

    def combine_b(k):
        combine(k, rows_b, 84, CUT_A, PACK)

    server_weights(1)
    swap(rows_b, 84)
    for buf, me, up, down, k0 in lines:
        left, right = (me + 3) % 4, (me + 1) % 4
        wire.wait(buf.at[left], k0, down)
        wire.send(buf.at[left, lo], buf.at[left, lo], k0 + 2, up)
        wire.wait(buf.at[right], k0 + 1, up)
        wire.send(buf.at[right, hi], buf.at[right, hi], k0 + 3, down)
    combine_b(2)
    wire.send(packed.at[row(2, c), rows_b], B["from_p"], 88, place.ym)
    combine_b(1)
    wire.send(packed.at[row(1, c), rows_b], B["fin_p"].at[rows_b], 89, place.yp)
    for buf, me, up, down, k0 in lines:
        far = (me + 2) % 4
        wire.wait(buf.at[far, lo], k0 + 2, down)
        wire.wait(buf.at[far, hi], k0 + 3, up)
    for k in (2, 1, 3, 0):
        for m in range(8):
            zd, xd = (z + k) % 4, (x + k) % 4
            at = source[(x * 4 + zd) * 8 + m]
            here = (at // 16 % 4 == z) & (at % 16 < 8)
            B["pick_x"][k, m] = jnp.where(here, line_x[at // 64, at % 8].astype(f32), 0.0).astype(bf16)
            at = source[(xd * 4 + z) * 8 + m]
            here = (at // 64 == x) & (at % 16 >= 8)
            B["pick_z"][k, m] = jnp.where(here, line_z[at // 16 % 4, at % 8].astype(f32), 0.0).astype(bf16)
        if k:
            wire.send(B["pick_x"].at[k], B["got_x"].at[k - 1], 67 + k, place.at(0, k, 0))
            wire.send(B["pick_z"].at[k], B["got_z"].at[k - 1], 70 + k, place.at(k, 0, 0))
    server_weights(0)
    swap(rows_a, 80)
    for k in range(1, 4):
        wire.wait(B["got_x"].at[k - 1], 67 + k, place.at(0, 4 - k, 0))
        wire.wait(B["got_z"].at[k - 1], 70 + k, place.at(4 - k, 0, 0))
    for m in range(8):
        piece = B["pick_x"][0, m].astype(f32) + B["pick_z"][0, m].astype(f32)
        for k in range(3):
            piece = piece + B["got_x"][k, m].astype(f32) + B["got_z"][k, m].astype(f32)
        B["picked"][m] = piece.astype(bf16)
    own = B["own"]
    own[r] = B["picked"][r]
    for i in range(1, 8):
        m = (r + i) % 8
        wire.send(B["picked"].at[m], own.at[r], 91 + i, place.group + m)
    combine_a(2)
    wire.send(packed.at[row(2, c), rows_a], B["from_m"], 90, place.yp)
    combine_a(3)
    wire.send(packed.at[row(3, c), rows_a], B["fin_m"].at[rows_a], 91, place.ym)
    combine_a(1)
    combine_b(3)
    for i in range(1, 8):
        j = (r - i + 8) % 8
        wire.wait(own.at[j], 91 + i, place.group + j)

    C["dy"][...] = own[...].reshape(128, D).astype(f32)
    block_backward(0, 128, C, win_c, wdn_c, C["dy"])
    cpack, cswap, cmine = B["cpack"], B["cswap"], B["cmine"]
    B["dperm"][...] = mm(C["dyb"][0], B["order"][...]).astype(bf16)
    for q in range(5):
        if q == 4:
            B["dperm"][...] = mm(C["dy"][...].astype(bf16), B["order"][...]).astype(bf16)
        right = B["pp"][...] if q == 4 else C["h"][0, :, D * q : D * q + D]
        val = mm(B["dperm"][...], right, 0, 0).astype(bf16)
        for core in range(2):
            for i in range(16):
                cpack[i, core, MAIN + 16 * q : MAIN + 16 * q + 16] = val[256 * core + 16 * i : 256 * core + 16 * i + 16]
    wire.send(cpack.at[:, 1 - c, pl.ds(MAIN, TAIL)], cswap.at[:, pl.ds(MAIN, TAIL)], 108, place.partner)
    for b, u, dout in weight_pairs(C, 0):
        val = mm(dout[...], u[...], 0, 0).astype(bf16)
        for i in range(2):
            for k in range(4):
                for core in range(2):
                    low = 192 * i + 48 * k + 24 * core
                    cpack[2 * b + i, core, 24 * k : 24 * k + 24] = val[low : low + 24]
        pair = pl.ds(2 * b, 2)
        wire.send(cpack.at[pair, 1 - c, pl.ds(0, MAIN)], cswap.at[pair, pl.ds(0, MAIN)], 100 + b, place.partner)

    X, Z = pl.ds(0, MAIN), pl.ds(MAIN, TAIL)

    def fold(low, high):
        for i in range(16):
            total = cpack[i, c, low:high].astype(f32) + cswap[i, low:high].astype(f32)
            cmine[i // 4, i % 4, low:high] = total.astype(bf16)

    def src_x(k, part):
        return cmine.at[(x + k) % 4, pl.ds(2 * part, 2), X]

    def src_z(k, part):
        return cmine.at[pl.ds(2 * part, 2), (z + k) % 4, Z]

    def ring_one(src, hop, end, up, down, k0):
        wire.send(src(2, 0), hop.at[0], k0, up)
        wire.send(src(2, 1), hop.at[1], k0 + 1, down)
        wire.send(src(1, 1), end.at[0, pl.ds(2, 2)], k0 + 2, up)
        wire.send(src(3, 0), end.at[1, pl.ds(0, 2)], k0 + 3, down)

    def ring_two(src, load, hop, end, up, down, k0):
        wire.wait(hop.at[0], k0, down)
        load(1, 0, hop)
        wire.send(src(1, 0), end.at[0, pl.ds(0, 2)], k0 + 4, up)
        wire.wait(hop.at[1], k0 + 1, up)
        load(3, 1, hop)
        wire.send(src(3, 1), end.at[1, pl.ds(2, 2)], k0 + 5, down)

    def ring_three(end, up, down, k0):
        wire.wait(end.at[0, pl.ds(2, 2)], k0 + 2, down)
        wire.wait(end.at[1, pl.ds(0, 2)], k0 + 3, up)
        wire.wait(end.at[0, pl.ds(0, 2)], k0 + 4, down)
        wire.wait(end.at[1, pl.ds(2, 2)], k0 + 5, up)

    def load_x(k, part, hop):
        to = (x + k) % 4
        for i in range(2):
            at = 2 * part + i
            cmine[to, at, :MAIN] = (cmine[to, at, :MAIN].astype(f32) + hop[part, i].astype(f32)).astype(bf16)

    def load_z(k, part, hop):
        to = (z + k) % 4
        for i in range(2):
            at = 2 * part + i
            cmine[at, to, MAIN:] = (cmine[at, to, MAIN:].astype(f32) + hop[part, i].astype(f32)).astype(bf16)

    wire.wait(cswap.at[:, Z], 108, place.partner)
    fold(MAIN, BLOCK)
    ring_one(src_z, B["hop_z"], B["end_z"], place.zp, place.zm, 116)
    for b in range(8):
        wire.wait(cswap.at[pl.ds(2 * b, 2), X], 100 + b, place.partner)
    fold(0, MAIN)
    ring_one(src_x, B["hop_x"], B["end_x"], place.xp, place.xm, 110)

    wire.wait(B["from_m"], 90, place.ym)

    def add_a(rows):
        packed[row(1, c), rows, :] = (packed[row(1, c), rows, :].astype(f32) + B["from_m"][rows, :].astype(f32)).astype(bf16)

    add_rows(0, CUT_A, 48, add_a)
    wire.send(packed.at[row(1, c), rows_a], B["fin_p"].at[rows_a], 122, place.yp)
    wire.wait(B["from_p"], 88, place.yp)

    def add_b(i, carry):
        here = pl.ds(pl.multiple_of(i * 48, 16), 48)
        rows = pl.ds(pl.multiple_of(CUT_A + i * 48, 16), 48)
        packed[row(3, c), rows, :] = (packed[row(3, c), rows, :].astype(f32) + B["from_p"][here, :].astype(f32)).astype(bf16)
        return carry

    lax.fori_loop(0, (PACK - CUT_A) // 48, add_b, 0)
    wire.send(packed.at[row(3, c), rows_b], B["fin_m"].at[rows_b], 123, place.ym)

    ring_two(src_z, load_z, B["hop_z"], B["end_z"], place.zp, place.zm, 116)
    ring_two(src_x, load_x, B["hop_x"], B["end_x"], place.xp, place.xm, 110)
    half_x, half_z = B["half_x"], B["half_z"]
    ring_three(B["end_z"], place.zp, place.zm, 116)
    for i in range(4):
        total = cmine[i, z, MAIN:].astype(f32) + B["end_z"][0, i].astype(f32) + B["end_z"][1, i].astype(f32)
        half_z[i] = total.astype(bf16)
    for k in (2, 1, 3):
        wire.send(half_z.at[(x + k) % 4], B["two_z"].at[k - 1], 127 + k, place.at(k, 0, 0))
    ring_three(B["end_x"], place.xp, place.xm, 110)
    for i in range(4):
        total = cmine[x, i, :MAIN].astype(f32) + B["end_x"][0, i].astype(f32) + B["end_x"][1, i].astype(f32)
        half_x[i] = total.astype(bf16)
    for k in (2, 1, 3):
        wire.send(half_x.at[(z + k) % 4], B["two_x"].at[k - 1], 124 + k, place.at(0, k, 0))
    combine_a(0)
    combine_b(0)
    for k in range(1, 4):
        wire.wait(B["two_z"].at[k - 1], 127 + k, place.at(4 - k, 0, 0))
    tail = half_z[x].astype(f32)
    for k in range(3):
        tail = tail + B["two_z"][k].astype(f32)
    line, column = iota((64, TAIL), 0), iota((64, TAIL), 1)
    inside = line & 15
    pick = (column == (inside // 3) * 16 + (line >> 4) * 3 + inside % 3) & (inside < 15)
    ordered = mm(pick.astype(f32).astype(bf16), tail.astype(bf16)).astype(bf16)
    for k in range(4):
        B["low_z"][k] = ordered[16 * k : 16 * k + 16]
    for k in range(1, 4):
        wire.wait(B["two_x"].at[k - 1], 124 + k, place.at(0, 4 - k, 0))
    main = half_x[z].astype(f32)
    for k in range(3):
        main = main + B["two_x"][k].astype(f32)
    for k in range(4):
        B["low_x"][k] = main[24 * k : 24 * k + 24].astype(bf16)
    for k in (2, 1, 3):
        to = (y + k) % 4
        wire.send(B["low_x"].at[to], B["three_x"].at[k - 1], 130 + k, place.at(0, 0, k))
        wire.send(B["low_z"].at[to], B["three_z"].at[k - 1], 133 + k, place.at(0, 0, k))

    wire.wait(B["fin_p"].at[rows_b], 89, place.ym)
    wire.wait(B["fin_m"].at[rows_a], 91, place.yp)
    wire.wait(B["fin_p"].at[rows_a], 122, place.ym)
    wire.wait(B["fin_m"].at[rows_b], 123, place.yp)

    def total_of(first_row, rows):
        at = pl.ds(first_row, rows)
        return packed[row(0, c), at, :].astype(f32) + B["fin_p"][at, :].astype(f32) + B["fin_m"][at, :].astype(f32)

    for l in range(LAYERS):
        for b in range(8):
            gin[l, :, D * b : D * b + D] = total_of(576 * l + 48 * b, 48)
        for b in range(4):
            gdn[l, 48 * b : 48 * b + 48, :] = total_of(576 * l + D + 48 * b, 48)
    gcls_out[...] = total_of(PACK - 48, 48)[:, 0:CLASSES]

    for k in range(1, 4):
        wire.wait(B["three_x"].at[k - 1], 130 + k, place.at(0, 0, 4 - k))
        wire.wait(B["three_z"].at[k - 1], 133 + k, place.at(0, 0, 4 - k))
    main = B["low_x"][y].astype(f32)
    tail = B["low_z"][y].astype(f32)
    for k in range(3):
        main = main + B["three_x"][k].astype(f32)
        tail = tail + B["three_z"][k].astype(f32)
    out_in[...] = main
    for q in range(4):
        out_dn[:, D * q : D * q + D] = tail[3 * q : 3 * q + 3]
    out_pe[...] = tail[12:15, 0:192]
    out_pos[...] = tail[12:15, 256:272]
    wire.finish()


def per_device(patches, labels, assign, patch_embed, positions, client_in, client_down, server_in, server_down, classifier):
    routes = assign[:, 0]
    places = jnp.arange(128, dtype=jnp.int32)
    earlier = (routes[:, None] == routes[None, :]) & (places[:, None] < places[None, :])
    source = routes * CAP + jnp.sum(earlier.astype(jnp.int32), axis=0)
    shapes = [
        ((1, CAP), f32),
        ((LAYERS, 48, 4 * D + FF), f32),
        ((LAYERS, 192, D), f32),
        ((48, CLASSES), f32),
        ((24, D), f32),
        ((3, FF), f32),
        ((3, 192), f32),
        ((3, TOK), f32),
    ]
    scratch = list(CLIENT.values()) + list(SERVER.values()) + list(BUFFERS.values())
    losses, gin, gdn, gcls, out_in, out_dn, out_pe, out_pos = pl.pallas_call(
        step_kernel,
        out_shape=[jax.ShapeDtypeStruct(*s) for s in shapes],
        in_specs=[VMEM] * 9 + [SMEM, ANY],
        out_specs=[VMEM] * len(shapes),
        scratch_shapes=[pltpu.VMEM(*s) for s in scratch]
        + [pltpu.SemaphoreType.DMA((N_SEM,)), pltpu.SemaphoreType.DMA((N_SEM,)), pltpu.SemaphoreType.DMA],
        compiler_params=pltpu.CompilerParams(collective_id=0, has_side_effects=True, vmem_limit_bytes=67043328),
        name="step",
    )(
        patches.T,
        patch_embed,
        positions,
        client_in[None],
        client_down[None],
        server_in,
        server_down,
        assign.reshape(1, 128),
        labels.reshape(8, 128),
        source,
        classifier.transpose(0, 2, 1),
    )
    return losses, out_pe.T, out_pos.T, out_in.T, out_dn.T, gin, gdn, gcls


def solution(mesh):
    in_specs = (
        P("client", None),
        P(),
        P(),
        P(),
        P(),
        P(),
        P(),
        P(None, "client", None),
        P(None, "client", None),
        P(),
    )
    out_specs = (
        P("client", None),
        P(None, "client"),
        P(None, "client"),
        P(None, "client"),
        P(None, "client"),
        P(None, "client", None),
        P(None, "client", None),
        P("client", None),
    )
    return jax.shard_map(per_device, mesh=mesh, in_specs=in_specs, out_specs=out_specs, check_vma=False)
```

```python
import math

import jax
import jax.numpy as jnp
from jax import lax
from jax.experimental import pallas as pl
from jax.experimental.pallas import tpu as pltpu
from jax.sharding import PartitionSpec as P

D = 384
FF = 1536
TOK = 16
IMG = 8
CLASSES = 10
SHARDS = 16
LAYERS = 2
CAP = 16
EPSILON = 1e-06
SCALE = 0.125
GELU_A = math.sqrt(2.0 / math.pi)
GELU_B = 0.044715
PACK = LAYERS * (D + FF // 8) + D // 8
CUT_A = 576
MAIN = 96
TAIL = 80
BLOCK = MAIN + TAIL

bf16 = jnp.bfloat16
f32 = jnp.float32
MESH = pl.DeviceIdType.MESH
VMEM = pl.BlockSpec(memory_space=pltpu.VMEM)
SMEM = pl.BlockSpec(memory_space=pltpu.SMEM)
ANY = pl.BlockSpec(memory_space=pl.ANY)
HBM = pl.BlockSpec(memory_space=pltpu.HBM)


def mm(a, b, ca=1, cb=0):
    return lax.dot_general(a, b, (((ca,), (cb,)), ((), ())), preferred_element_type=f32)


def iota(shape, dim):
    return lax.broadcasted_iota(jnp.int32, shape, dim)


def norm(v):
    centre = v - jnp.mean(v, axis=-1, keepdims=True)
    rstd = lax.rsqrt(jnp.mean(centre * centre, axis=-1, keepdims=True) + EPSILON)
    return centre * rstd, rstd


def norm_back(v, grad):
    hat, rstd = norm(v)
    along = jnp.mean(grad * hat, axis=-1, keepdims=True)
    return rstd * (grad - jnp.mean(grad, axis=-1, keepdims=True) - hat * along)


def rounded(v):
    return v.astype(bf16).astype(f32)


def head_masks(rows):
    low = (iota((rows, 128), 1) < 64).astype(f32)
    return low.astype(bf16), (1.0 - low).astype(bf16)


def two_heads(v):
    low, high = head_masks(v.shape[0])
    return jnp.concatenate([v * low, v * high], axis=0)


def merge_heads(v):
    rows = v.shape[0] // 2
    return jnp.where(iota((rows, 128), 1) < 64, v[:rows], v[rows:])


def block_forward(l, rows, S, win, wdn):
    x = S["x"][l]
    hat, _ = norm(x)
    u1 = hat.astype(bf16)
    S["u1"][l] = u1
    for n in range(3):
        cols = slice(D * n, D * n + D)
        S["qkv"][l, :, cols] = mm(u1, win[l, :, cols]).astype(bf16)
    same = ((iota((256, 128), 0) & 127) >> 4) == (iota((256, 128), 1) >> 4)
    for g in range(rows // 128):
        part = slice(128 * g, 128 * g + 128)
        for p in range(3):
            q2 = S["qkv"][l, part, 128 * p : 128 * p + 128]
            k2 = S["qkv"][l, part, D + 128 * p : D + 128 * p + 128]
            v2 = S["qkv"][l, part, 2 * D + 128 * p : 2 * D + 128 * p + 128]
            scores = mm(two_heads(q2), k2, 1, 1) * SCALE
            scores = jnp.where(same, scores, -1e30)
            grown = jnp.exp(scores - jnp.max(scores, axis=-1, keepdims=True))
            prob = grown / jnp.sum(grown, axis=-1, keepdims=True)
            S["prob"][l, 3 * g + p] = prob
            S["att"][l, part, 128 * p : 128 * p + 128] = merge_heads(mm(prob.astype(bf16), v2)).astype(bf16)
    x1 = S["x"][l] + mm(S["att"][l], win[l, :, 3 * D : 4 * D])
    S["x1"][l] = x1
    hat, _ = norm(x1)
    u2 = hat.astype(bf16)
    S["u2"][l] = u2
    for n in range(4):
        pre = mm(u2, win[l, :, 4 * D + D * n : 5 * D + D * n])
        S["pre"][l, :, D * n : D * n + D] = pre
        bent = jnp.tanh(GELU_A * (pre + GELU_B * pre * pre * pre))
        S["h"][l, :, D * n : D * n + D] = (0.5 * pre * (1.0 + bent)).astype(bf16)
    return S["x1"][l] + mm(S["h"][l], wdn[l])


def block_backward(l, rows, S, win, wdn, dy_ref):
    dyb = dy_ref[...].astype(bf16)
    S["dyb"][l] = dyb
    for n in range(4):
        cols = slice(D * n, D * n + D)
        dh = rounded(mm(dyb, wdn[l, cols, :], 1, 1))
        pre = S["pre"][l, :, cols]
        bent = jnp.tanh(GELU_A * (pre + GELU_B * pre * pre * pre))
        slope = 0.5 * (1.0 + bent) + 0.5 * pre * (1.0 - bent * bent) * GELU_A * (1.0 + 3.0 * GELU_B * pre * pre)
        S["dpre"][l, :, cols] = (dh * slope).astype(bf16)
    du2 = rounded(mm(S["dpre"][l], win[l, :, 4 * D :], 1, 1))
    dx1 = dy_ref[...] + norm_back(S["x1"][l], du2)
    dy_ref[...] = dx1
    dx1b = dx1.astype(bf16)
    S["dx1b"][l] = dx1b
    S["datt"][...] = mm(dx1b, win[l, :, 3 * D : 4 * D], 1, 1).astype(bf16)
    for g in range(rows // 128):
        part = slice(128 * g, 128 * g + 128)
        for p in range(3):
            cq = slice(128 * p, 128 * p + 128)
            ck = slice(D + 128 * p, D + 128 * p + 128)
            cv = slice(2 * D + 128 * p, 2 * D + 128 * p + 128)
            qs = two_heads(S["qkv"][l, part, cq])
            dos = two_heads(S["datt"][part, cq])
            prob = S["prob"][l, 3 * g + p]
            dprob = mm(dos, S["qkv"][l, part, cv], 1, 1)
            dscore = prob * (dprob - jnp.sum(prob * dprob, axis=-1, keepdims=True)) * SCALE
            dsb = dscore.astype(bf16)
            S["dqkv"][l, part, cq] = merge_heads(mm(dsb, S["qkv"][l, part, ck])).astype(bf16)
            S["dqkv"][l, part, ck] = mm(dsb, qs, 0, 0).astype(bf16)
            S["dqkv"][l, part, cv] = mm(prob.astype(bf16), dos, 0, 0).astype(bf16)
    du1 = rounded(mm(S["dqkv"][l], win[l, :, : 3 * D], 1, 1))
    dy_ref[...] = dy_ref[...] + norm_back(S["x"][l], du1)


def weight_pairs(S, l):
    pairs = []
    for n in range(3):
        pairs.append((n, S["u1"].at[l], S["dqkv"].at[l, :, pl.ds(D * n, D)]))
    pairs.append((3, S["att"].at[l], S["dx1b"].at[l]))
    for n in range(4):
        pairs.append((4 + n, S["u2"].at[l], S["dpre"].at[l, :, pl.ds(D * n, D)]))
    return pairs


def block_shapes(layers, rows):
    return dict(
        x=((layers + 1, rows, D), f32),
        x1=((layers, rows, D), f32),
        u1=((layers, rows, D), bf16),
        u2=((layers, rows, D), bf16),
        qkv=((layers, rows, 3 * D), bf16),
        prob=((layers, 3 * rows // 128, 256, 128), f32),
        att=((layers, rows, D), bf16),
        pre=((layers, rows, FF), f32),
        h=((layers, rows, FF), bf16),
        dyb=((layers, rows, D), bf16),
        dpre=((layers, rows, FF), bf16),
        dx1b=((layers, rows, D), bf16),
        datt=((rows, D), bf16),
        dqkv=((layers, rows, 3 * D), bf16),
        dy=((rows, D), f32),
    )


class Place:
    def __init__(self):
        me = lax.axis_index("client")
        self.me = me
        self.c, self.y, self.z, self.x = me % 2, me // 2 % 4, me // 8 % 4, me // 32
        self.r, self.group = me % 8, me // 8 * 8
        self.partner = me + 1 - 2 * self.c
        self.yp, self.ym = self.at(0, 0, 1), self.at(0, 0, 3)
        self.xp, self.xm = self.at(1, 0, 0), self.at(3, 0, 0)
        self.zp, self.zm = self.at(0, 1, 0), self.at(0, 3, 0)

    def at(self, dx, dz, dy):
        x, z, y = (self.x + dx) % 4, (self.z + dz) % 4, (self.y + dy) % 4
        return ((x * 4 + z) * 4 + y) * 2 + self.c

    def greet(self, group, plane):
        peers = []
        if group:
            peers += [self.group + (self.r + i) % 8 for i in range(1, 8)]
        if plane:
            peers += [self.xp, self.xm, self.zp, self.zm]
        barrier = pltpu.get_barrier_semaphore()
        for peer in peers:
            pl.semaphore_signal(barrier, inc=1, device_id=(peer,), device_id_type=MESH)
        pl.semaphore_wait(barrier, len(peers))


class Wire:
    def __init__(self, send_sem, recv_sem):
        self.send_sem, self.recv_sem, self.sent = send_sem, recv_sem, []

    def make(self, src, dst, k, device):
        return pltpu.make_async_remote_copy(
            src_ref=src,
            dst_ref=dst,
            send_sem=self.send_sem.at[k],
            recv_sem=self.recv_sem.at[k],
            device_id=(device,),
            device_id_type=MESH,
        )

    def send(self, src, dst, k, device):
        copy = self.make(src, dst, k, device)
        copy.start()
        self.sent.append(copy)

    def wait(self, landed, k, device):
        self.make(landed, landed, k, device).wait_recv()

    def finish(self):
        for copy in self.sent:
            copy.wait_send()


def plane_gather(wire, place, buf, count, k0):
    half, quarter = count // 2, count // 4
    x, z = place.x, place.z
    xm, xp, zm, zp = (x + 3) % 4, (x + 1) % 4, (z + 3) % 4, (z + 1) % 4
    xo, zo = (x + 2) % 4, (z + 2) % 4
    X, XA, XB = pl.ds(0, half), pl.ds(0, quarter), pl.ds(quarter, quarter)
    Z, ZA, ZB = pl.ds(half, half), pl.ds(half, quarter), pl.ds(half + quarter, quarter)

    def both(ref, k, device):
        wire.send(ref, ref, k0 + k, device)

    def first():
        both(buf.at[x, z, X], 0, place.xp)
        both(buf.at[x, z, X], 1, place.xm)
        both(buf.at[x, z, Z], 2, place.zp)
        both(buf.at[x, z, Z], 3, place.zm)

    def second():
        wire.wait(buf.at[xm, z, X], k0 + 0, place.xm)
        both(buf.at[xm, z, XA], 4, place.xp)
        wire.wait(buf.at[xp, z, X], k0 + 1, place.xp)
        both(buf.at[xp, z, XB], 5, place.xm)
        wire.wait(buf.at[x, zm, Z], k0 + 2, place.zm)
        both(buf.at[x, zm, ZA], 6, place.zp)
        wire.wait(buf.at[x, zp, Z], k0 + 3, place.zp)
        both(buf.at[x, zp, ZB], 7, place.zm)

    def third():
        wire.wait(buf.at[xo, z, XA], k0 + 4, place.xm)
        wire.wait(buf.at[xo, z, XB], k0 + 5, place.xp)
        both(buf.at[:, z, X], 8, place.zp)
        both(buf.at[:, z, X], 9, place.zm)
        wire.wait(buf.at[x, zo, ZA], k0 + 6, place.zm)
        wire.wait(buf.at[x, zo, ZB], k0 + 7, place.zp)
        both(buf.at[x, :, Z], 10, place.xp)
        both(buf.at[x, :, Z], 11, place.xm)

    def fourth():
        wire.wait(buf.at[:, zm, X], k0 + 8, place.zm)
        both(buf.at[0:2, zm, X], 12, place.zp)
        wire.wait(buf.at[:, zp, X], k0 + 9, place.zp)
        both(buf.at[2:4, zp, X], 13, place.zm)
        wire.wait(buf.at[xm, :, Z], k0 + 10, place.xm)
        both(buf.at[xm, 0:2, Z], 14, place.xp)
        wire.wait(buf.at[xp, :, Z], k0 + 11, place.xp)
        both(buf.at[xp, 2:4, Z], 15, place.xm)

    def fifth():
        wire.wait(buf.at[0:2, zo, X], k0 + 12, place.zm)
        wire.wait(buf.at[2:4, zo, X], k0 + 13, place.zp)
        wire.wait(buf.at[xo, 0:2, Z], k0 + 14, place.xm)
        wire.wait(buf.at[xo, 2:4, Z], k0 + 15, place.xp)

    return first, second, third, fourth, fifth


def add_rows(start, stop, step, body):
    def run(i, carry):
        body(pl.ds(pl.multiple_of(start + i * step, 16), step))
        return carry

    lax.fori_loop(0, (stop - start) // step, run, 0)


def route(arow, labels, shard, rank_in):
    eye = iota((128, 128), 0) == iota((128, 128), 1)
    acol = jnp.sum(jnp.where(eye, arow.astype(f32), 0.0), axis=1, keepdims=True).astype(jnp.int32)
    earlier = (acol == arow) & (iota((128, 128), 0) < iota((128, 128), 1))
    rank = jnp.sum(earlier.astype(f32), axis=0, keepdims=True).astype(jnp.int32)
    chosen = (jnp.broadcast_to(arow, (CAP, 128)) == shard) & (
        jnp.broadcast_to(rank, (CAP, 128)) == iota((CAP, 128), 0)
    )
    selector = chosen.astype(f32).astype(bf16)
    take = (iota((128, 16), 0) == iota((128, 16), 1) * IMG + rank_in).astype(f32).astype(bf16)
    by_row = mm(labels.astype(f32).astype(bf16), take).astype(bf16)
    lift = ((iota((128, 8), 0) >> 4) == iota((128, 8), 1)).astype(f32).astype(bf16)
    tall = mm(lift, by_row)
    mine = (iota((128, 16), 0) & 15) == iota((128, 16), 1)
    label = jnp.sum(jnp.where(mine, tall, 0.0), axis=1, keepdims=True)
    onehot = (label == iota((128, CLASSES), 1).astype(f32)).astype(f32).astype(bf16)
    return selector, mm(selector, onehot), arow * CAP + rank


def slot_rows(selector, arrived):
    spread = (iota((128, 2048), 0) == (iota((128, 2048), 1) >> 4)).astype(f32).astype(bf16)
    wide = mm(selector, spread).astype(bf16)
    repeat = ((iota((256, CAP), 0) >> 4) == iota((256, CAP), 1)).astype(f32).astype(bf16)
    tall = mm(repeat, wide)
    same = (iota((256, 2048), 0) & 15) == (iota((256, 2048), 1) & 15)
    return mm(jnp.where(same, tall, 0.0).astype(bf16), arrived)


def head_loss(last, classes, hot):
    filled = jnp.sum(hot, axis=1, keepdims=True)
    mean = jnp.mean(last.reshape(CAP, TOK, D), axis=1)
    hat, _ = norm(mean)
    pooled = hat.astype(bf16)
    logits = mm(pooled, classes, 1, 1)
    top = jnp.max(logits, axis=1, keepdims=True)
    grown = jnp.exp(logits - top)
    total = jnp.sum(grown, axis=1, keepdims=True)
    per = (jnp.log(total) + top - jnp.sum(hot * logits, axis=1, keepdims=True)) * filled
    eye = iota((CAP, CAP), 0) == iota((CAP, CAP), 1)
    losses = jnp.sum(jnp.where(eye, per, 0.0), axis=0, keepdims=True)
    dlogits = ((grown / total) * filled - hot).astype(bf16)
    gcls = mm(pooled, dlogits, 0, 0).astype(bf16)
    dpooled = rounded(mm(dlogits, classes))
    dmean = norm_back(mean, dpooled) * (1.0 / TOK)
    dlast = jnp.broadcast_to(dmean[:, None, :], (CAP, TOK, D)).reshape(CAP * TOK, D)
    return losses, gcls, dlast


CLIENT = block_shapes(1, 128)
SERVER = block_shapes(LAYERS, 256)
BUFFERS = dict(
    arrived=((4, 4, IMG, TOK, D), bf16),
    win=((LAYERS, D, 4 * D + FF), bf16),
    wdn=((LAYERS, FF, D), bf16),
    win_c=((1, D, 4 * D + FF), bf16),
    wdn_c=((1, FF, D), bf16),
    win_s=((LAYERS, 48, 4 * D + FF), bf16),
    wdn_s=((LAYERS, 192, D), bf16),
    table=((1, 128), jnp.int32),
    cut=((IMG, TOK, D), bf16),
    packed=((8, PACK, D), bf16),
    swapped=((4, PACK, D), bf16),
    from_m=((CUT_A, D), bf16),
    from_p=((PACK - CUT_A, D), bf16),
    fin_p=((PACK, D), bf16),
    fin_m=((PACK, D), bf16),
    line_x=((4, 8, TOK, D), bf16),
    line_z=((4, 8, TOK, D), bf16),
    pick_x=((4, 8, TOK, D), bf16),
    pick_z=((4, 8, TOK, D), bf16),
    got_x=((3, 8, TOK, D), bf16),
    got_z=((3, 8, TOK, D), bf16),
    picked=((8, TOK, D), bf16),
    own=((IMG, TOK, D), bf16),
    order=((D, 512), bf16),
    dperm=((128, 512), bf16),
    pp=((128, D), bf16),
    cpack=((16, 2, BLOCK, D), bf16),
    cswap=((16, BLOCK, D), bf16),
    cmine=((4, 4, BLOCK, D), bf16),
    hop_x=((2, 2, MAIN, D), bf16),
    hop_z=((2, 2, TAIL, D), bf16),
    end_x=((2, 4, MAIN, D), bf16),
    end_z=((2, 4, TAIL, D), bf16),
    half_x=((4, MAIN, D), bf16),
    half_z=((4, TAIL, D), bf16),
    two_x=((3, MAIN, D), bf16),
    two_z=((3, TAIL, D), bf16),
    low_x=((4, 24, D), bf16),
    low_z=((4, 16, D), bf16),
    three_x=((3, 24, D), bf16),
    three_z=((3, 16, D), bf16),
)
N_SEM = 160


def step_kernel(patches_t, embed, positions, arow, labels, classes, *refs):
    sources, refs = refs[:4], refs[4:]
    losses, gin, gdn, gcls_out, out_in, out_dn, out_pe, out_pos = refs[:8]
    refs = list(refs[8:])
    C = dict(zip(CLIENT, refs[: len(CLIENT)]))
    refs = refs[len(CLIENT) :]
    S = dict(zip(SERVER, refs[: len(SERVER)]))
    refs = refs[len(SERVER) :]
    B = dict(zip(BUFFERS, refs[: len(BUFFERS)]))
    send_sem, recv_sem, local_sem, source = refs[len(BUFFERS) :]
    win_c, wdn_c, win_s, wdn_s = B["win_c"], B["wdn_c"], B["win_s"], B["wdn_s"]
    loads = []
    for n, (src, dst) in enumerate(zip(sources, (win_c, wdn_c, win_s, wdn_s))):
        loads.append(pltpu.make_async_copy(src, dst, local_sem.at[n]))
    for n in (2, 3, 0, 1):
        loads[n].start()
    place = Place()
    x, z, y, c, r = place.x, place.z, place.y, place.c, place.r
    shard = place.me // 8
    win, wdn, arrived, packed = B["win"], B["wdn"], B["arrived"], B["packed"]
    place.greet(True, True)
    wire = Wire(send_sem, recv_sem)

    def owner(dy, other=False):
        return (y + dy) % 4 * 2 + (1 - c if other else c)

    def window(l, down, rank, part):
        if down:
            low, size = {None: (0, 192), 0: (0, 96), 1: (96, 96)}[part]
            return wdn.at[l, pl.ds(pl.multiple_of(rank * 192 + low, 16), size), :]
        cols = {None: pl.ds(0, 3072), 0: pl.ds(0, 1536), 1: pl.ds(1536, 1536)}[part]
        return win.at[l, pl.ds(pl.multiple_of(rank * 48, 16), 48), cols]

    pieces = [(l, down) for l in range(LAYERS) for down in (False, True)]
    base = {piece: 8 + 9 * n for n, piece in enumerate(pieces)}

    def spread_own(piece):
        l, down = piece
        mine = (wdn_s if down else win_s).at[l]
        here = window(l, down, r, None)
        wire.send(mine, here, base[piece] + 0, place.yp)
        wire.send(mine, here, base[piece] + 1, place.ym)
        wire.send(mine, here, base[piece] + 4, place.partner)
        here[...] = mine[...]

    loads[2].wait()
    spread_own(pieces[0])
    for n in (3, 0, 1):
        loads[n].wait()

    def forward(piece):
        l, down = piece
        b = base[piece]
        left, right = owner(3), owner(1)
        whole, half = window(l, down, left, None), window(l, down, left, 0)
        wire.wait(whole, b + 0, place.ym)
        wire.send(half, half, b + 2, place.yp)
        wire.send(whole, whole, b + 5, place.partner)
        whole, half = window(l, down, right, None), window(l, down, right, 1)
        wire.wait(whole, b + 1, place.yp)
        wire.send(half, half, b + 3, place.ym)
        wire.send(whole, whole, b + 6, place.partner)

    def across(piece):
        l, down = piece
        b = base[piece]
        for part, device in ((0, place.ym), (1, place.yp)):
            half = window(l, down, owner(2), part)
            wire.wait(half, b + 2 + part, device)
            wire.send(half, half, b + 7 + part, place.partner)

    def settle(piece):
        l, down = piece
        b = base[piece]
        wire.wait(window(l, down, owner(0, True), None), b + 4, place.partner)
        wire.wait(window(l, down, owner(3, True), None), b + 5, place.partner)
        wire.wait(window(l, down, owner(1, True), None), b + 6, place.partner)
        for part in range(2):
            wire.wait(window(l, down, owner(2, True), part), b + 7 + part, place.partner)

    tiled = jnp.concatenate([positions[...].astype(f32)] * IMG, axis=0)
    C["x"][0] = mm(patches_t[...], embed[...], 0, 0) + tiled
    cut = block_forward(0, 128, C, win_c, wdn_c).astype(bf16)
    B["cut"][...] = cut.reshape(IMG, TOK, D)
    for i in range(1, 8):
        j = (r + i) % 8
        wire.send(B["cut"].at[j], arrived.at[x, z, r], i, place.group + j)
    for piece in pieces[1:]:
        spread_own(piece)
    arrived[x, z, r] = B["cut"][r]
    selector, hot, table = route(arow[...], labels[...], shard, r)
    B["table"][...] = table
    to_scalar = pltpu.make_async_copy(B["table"], source, local_sem.at[4])
    to_scalar.start()
    first, second, third, fourth, fifth = plane_gather(wire, place, arrived, IMG, 44)
    forward(pieces[0])
    for i in range(1, 8):
        j = (r - i + 8) % 8
        wire.wait(arrived.at[x, z, j], i, place.group + j)
    first()
    forward(pieces[1])
    second()
    col = iota((1, 512), 1)
    at = col & 15
    wanted = ((col >> 4) & 15) * 24 + (at // 3) * 6 + (col >> 8) * 3 + at % 3
    B["order"][...] = ((iota((D, 512), 0) == wanted) & (at < 12)).astype(f32).astype(bf16)
    B["pp"][...] = (iota((128, D), 1) - 256 == (iota((128, D), 0) & 15)).astype(f32).astype(bf16)
    B["pp"][:, 0:192] = patches_t[...].T
    packed[:, PACK - 48 :, :] = jnp.zeros((8, 48, D), bf16)
    third()
    across(pieces[0])
    forward(pieces[2])
    across(pieces[1])
    fourth()
    forward(pieces[3])
    fifth()
    across(pieces[2])
    settle(pieces[0])
    settle(pieces[1])

    S["x"][0] = slot_rows(selector, arrived[...].reshape(2048, D))
    S["x"][1] = block_forward(0, 256, S, win, wdn)
    across(pieces[3])
    settle(pieces[2])
    settle(pieces[3])
    S["x"][2] = block_forward(1, 256, S, win, wdn)
    to_scalar.wait()
    ours = iota((CLASSES, SHARDS, D), 1) == shard
    table = jnp.sum(jnp.where(ours, classes[...].astype(f32), 0.0), axis=1).astype(bf16)
    loss, gcls, dlast = head_loss(S["x"][LAYERS], table, hot)
    losses[...] = loss
    for k in range(8):
        packed[k, PACK - 48 :, 0:CLASSES] = gcls[48 * k : 48 * k + 48]
    S["dy"][...] = dlast

    def backward(i, carry):
        block_backward(LAYERS - 1 - i, 256, S, win, wdn, S["dy"])
        return carry

    lax.fori_loop(0, LAYERS, backward, 0)

    line_x, line_z = B["line_x"], B["line_z"]
    gcut = S["dy"][...].astype(bf16).reshape(CAP, TOK, D)
    line_x[x] = gcut[:8]
    line_z[z] = gcut[8:]
    lo, hi, all8 = pl.ds(0, 4), pl.ds(4, 4), pl.ds(0, 8)
    lines = ((line_x, x, place.xp, place.xm, 60), (line_z, z, place.zp, place.zm, 64))
    for buf, me, up, down, k0 in lines:
        wire.send(buf.at[me], buf.at[me], k0, up)
        wire.send(buf.at[me], buf.at[me], k0 + 1, down)

    def server_weights(l):
        for b, u, dout in weight_pairs(S, l):
            val = mm(u[...], dout[...], 0, 0).astype(bf16)
            for k in range(8):
                packed[k, 576 * l + 48 * b : 576 * l + 48 * b + 48, :] = val[48 * k : 48 * k + 48]
        for n in range(4):
            val = mm(S["h"][l, :, D * n : D * n + D], S["dyb"][l], 0, 0).astype(bf16)
            for j in range(2):
                packed[2 * n + j, 576 * l + D : 576 * l + 576, :] = val[192 * j : 192 * j + 192]

    rows_a, rows_b = pl.ds(0, CUT_A), pl.ds(CUT_A, PACK - CUT_A)

    def row(k, core):
        return (y + k) % 4 * 2 + core

    def swap(part, k0):
        for k in (2, 1, 3, 0):
            wire.send(packed.at[row(k, 1 - c), part], B["swapped"].at[k, part], k0 + k, place.partner)

    def combine(k, part, k0, start, stop):
        wire.wait(B["swapped"].at[k, part], k0 + k, place.partner)

        def body(rows):
            total = packed[row(k, c), rows, :].astype(f32) + B["swapped"][k, rows, :].astype(f32)
            packed[row(k, c), rows, :] = total.astype(bf16)

        add_rows(start, stop, 48, body)

    def combine_a(k):
        combine(k, rows_a, 80, 0, CUT_A)

    def combine_b(k):
        combine(k, rows_b, 84, CUT_A, PACK)

    server_weights(1)
    swap(rows_b, 84)
    for buf, me, up, down, k0 in lines:
        left, right = (me + 3) % 4, (me + 1) % 4
        wire.wait(buf.at[left], k0, down)
        wire.send(buf.at[left, lo], buf.at[left, lo], k0 + 2, up)
        wire.wait(buf.at[right], k0 + 1, up)
        wire.send(buf.at[right, hi], buf.at[right, hi], k0 + 3, down)
    combine_b(2)
    wire.send(packed.at[row(2, c), rows_b], B["from_p"], 88, place.ym)
    combine_b(1)
    wire.send(packed.at[row(1, c), rows_b], B["fin_p"].at[rows_b], 89, place.yp)
    for buf, me, up, down, k0 in lines:
        far = (me + 2) % 4
        wire.wait(buf.at[far, lo], k0 + 2, down)
        wire.wait(buf.at[far, hi], k0 + 3, up)
    for k in (2, 1, 3, 0):
        for m in range(8):
            zd, xd = (z + k) % 4, (x + k) % 4
            at = source[0, (x * 4 + zd) * 8 + m]
            here = ((at >> 4) & 3 == z) & ((at & 15) < 8)
            B["pick_x"][k, m] = jnp.where(here, line_x[(at >> 6) & 3, at & 7].astype(f32), 0.0).astype(bf16)
            at = source[0, (xd * 4 + z) * 8 + m]
            here = ((at >> 6) & 3 == x) & ((at & 15) >= 8)
            B["pick_z"][k, m] = jnp.where(here, line_z[(at >> 4) & 3, at & 7].astype(f32), 0.0).astype(bf16)
        if k:
            wire.send(B["pick_x"].at[k], B["got_x"].at[k - 1], 67 + k, place.at(0, k, 0))
            wire.send(B["pick_z"].at[k], B["got_z"].at[k - 1], 70 + k, place.at(k, 0, 0))
    server_weights(0)
    swap(rows_a, 80)
    for k in range(1, 4):
        wire.wait(B["got_x"].at[k - 1], 67 + k, place.at(0, 4 - k, 0))
        wire.wait(B["got_z"].at[k - 1], 70 + k, place.at(4 - k, 0, 0))
    for m in range(8):
        piece = B["pick_x"][0, m].astype(f32) + B["pick_z"][0, m].astype(f32)
        for k in range(3):
            piece = piece + B["got_x"][k, m].astype(f32) + B["got_z"][k, m].astype(f32)
        B["picked"][m] = piece.astype(bf16)
    own = B["own"]
    own[r] = B["picked"][r]
    for i in range(1, 8):
        m = (r + i) % 8
        wire.send(B["picked"].at[m], own.at[r], 91 + i, place.group + m)
    combine_a(2)
    wire.send(packed.at[row(2, c), rows_a], B["from_m"], 90, place.yp)
    combine_a(3)
    wire.send(packed.at[row(3, c), rows_a], B["fin_m"].at[rows_a], 91, place.ym)
    combine_a(1)
    combine_b(3)
    for i in range(1, 8):
        j = (r - i + 8) % 8
        wire.wait(own.at[j], 91 + i, place.group + j)

    C["dy"][...] = own[...].reshape(128, D).astype(f32)
    block_backward(0, 128, C, win_c, wdn_c, C["dy"])
    cpack, cswap, cmine = B["cpack"], B["cswap"], B["cmine"]
    B["dperm"][...] = mm(C["dyb"][0], B["order"][...]).astype(bf16)
    for q in range(5):
        if q == 4:
            B["dperm"][...] = mm(C["dy"][...].astype(bf16), B["order"][...]).astype(bf16)
        right = B["pp"][...] if q == 4 else C["h"][0, :, D * q : D * q + D]
        val = mm(B["dperm"][...], right, 0, 0).astype(bf16)
        for core in range(2):
            for i in range(16):
                cpack[i, core, MAIN + 16 * q : MAIN + 16 * q + 16] = val[256 * core + 16 * i : 256 * core + 16 * i + 16]
    wire.send(cpack.at[:, 1 - c, pl.ds(MAIN, TAIL)], cswap.at[:, pl.ds(MAIN, TAIL)], 108, place.partner)
    for b, u, dout in weight_pairs(C, 0):
        val = mm(dout[...], u[...], 0, 0).astype(bf16)
        for i in range(2):
            for k in range(4):
                for core in range(2):
                    low = 192 * i + 48 * k + 24 * core
                    cpack[2 * b + i, core, 24 * k : 24 * k + 24] = val[low : low + 24]
        pair = pl.ds(2 * b, 2)
        wire.send(cpack.at[pair, 1 - c, pl.ds(0, MAIN)], cswap.at[pair, pl.ds(0, MAIN)], 100 + b, place.partner)

    X, Z = pl.ds(0, MAIN), pl.ds(MAIN, TAIL)

    def fold(low, high):
        for i in range(16):
            total = cpack[i, c, low:high].astype(f32) + cswap[i, low:high].astype(f32)
            cmine[i // 4, i % 4, low:high] = total.astype(bf16)

    def src_x(k, part):
        return cmine.at[(x + k) % 4, pl.ds(2 * part, 2), X]

    def src_z(k, part):
        return cmine.at[pl.ds(2 * part, 2), (z + k) % 4, Z]

    def ring_one(src, hop, end, up, down, k0):
        wire.send(src(2, 0), hop.at[0], k0, up)
        wire.send(src(2, 1), hop.at[1], k0 + 1, down)
        wire.send(src(1, 1), end.at[0, pl.ds(2, 2)], k0 + 2, up)
        wire.send(src(3, 0), end.at[1, pl.ds(0, 2)], k0 + 3, down)

    def ring_two(src, load, hop, end, up, down, k0):
        wire.wait(hop.at[0], k0, down)
        load(1, 0, hop)
        wire.send(src(1, 0), end.at[0, pl.ds(0, 2)], k0 + 4, up)
        wire.wait(hop.at[1], k0 + 1, up)
        load(3, 1, hop)
        wire.send(src(3, 1), end.at[1, pl.ds(2, 2)], k0 + 5, down)

    def ring_three(end, up, down, k0):
        wire.wait(end.at[0, pl.ds(2, 2)], k0 + 2, down)
        wire.wait(end.at[1, pl.ds(0, 2)], k0 + 3, up)
        wire.wait(end.at[0, pl.ds(0, 2)], k0 + 4, down)
        wire.wait(end.at[1, pl.ds(2, 2)], k0 + 5, up)

    def load_x(k, part, hop):
        to = (x + k) % 4
        for i in range(2):
            at = 2 * part + i
            cmine[to, at, :MAIN] = (cmine[to, at, :MAIN].astype(f32) + hop[part, i].astype(f32)).astype(bf16)

    def load_z(k, part, hop):
        to = (z + k) % 4
        for i in range(2):
            at = 2 * part + i
            cmine[at, to, MAIN:] = (cmine[at, to, MAIN:].astype(f32) + hop[part, i].astype(f32)).astype(bf16)

    wire.wait(cswap.at[:, Z], 108, place.partner)
    fold(MAIN, BLOCK)
    ring_one(src_z, B["hop_z"], B["end_z"], place.zp, place.zm, 116)
    for b in range(8):
        wire.wait(cswap.at[pl.ds(2 * b, 2), X], 100 + b, place.partner)
    fold(0, MAIN)
    ring_one(src_x, B["hop_x"], B["end_x"], place.xp, place.xm, 110)

    wire.wait(B["from_m"], 90, place.ym)

    def add_a(rows):
        packed[row(1, c), rows, :] = (packed[row(1, c), rows, :].astype(f32) + B["from_m"][rows, :].astype(f32)).astype(bf16)

    add_rows(0, CUT_A, 48, add_a)
    wire.send(packed.at[row(1, c), rows_a], B["fin_p"].at[rows_a], 122, place.yp)
    wire.wait(B["from_p"], 88, place.yp)

    def add_b(i, carry):
        here = pl.ds(pl.multiple_of(i * 48, 16), 48)
        rows = pl.ds(pl.multiple_of(CUT_A + i * 48, 16), 48)
        packed[row(3, c), rows, :] = (packed[row(3, c), rows, :].astype(f32) + B["from_p"][here, :].astype(f32)).astype(bf16)
        return carry

    lax.fori_loop(0, (PACK - CUT_A) // 48, add_b, 0)
    wire.send(packed.at[row(3, c), rows_b], B["fin_m"].at[rows_b], 123, place.ym)

    ring_two(src_z, load_z, B["hop_z"], B["end_z"], place.zp, place.zm, 116)
    ring_two(src_x, load_x, B["hop_x"], B["end_x"], place.xp, place.xm, 110)
    half_x, half_z = B["half_x"], B["half_z"]
    ring_three(B["end_z"], place.zp, place.zm, 116)
    for i in range(4):
        total = cmine[i, z, MAIN:].astype(f32) + B["end_z"][0, i].astype(f32) + B["end_z"][1, i].astype(f32)
        half_z[i] = total.astype(bf16)
    for k in (2, 1, 3):
        wire.send(half_z.at[(x + k) % 4], B["two_z"].at[k - 1], 127 + k, place.at(k, 0, 0))
    ring_three(B["end_x"], place.xp, place.xm, 110)
    for i in range(4):
        total = cmine[x, i, :MAIN].astype(f32) + B["end_x"][0, i].astype(f32) + B["end_x"][1, i].astype(f32)
        half_x[i] = total.astype(bf16)
    for k in (2, 1, 3):
        wire.send(half_x.at[(z + k) % 4], B["two_x"].at[k - 1], 124 + k, place.at(0, k, 0))
    combine_a(0)
    combine_b(0)
    for k in range(1, 4):
        wire.wait(B["two_z"].at[k - 1], 127 + k, place.at(4 - k, 0, 0))
    tail = half_z[x].astype(f32)
    for k in range(3):
        tail = tail + B["two_z"][k].astype(f32)
    line, column = iota((64, TAIL), 0), iota((64, TAIL), 1)
    inside = line & 15
    pick = (column == (inside // 3) * 16 + (line >> 4) * 3 + inside % 3) & (inside < 15)
    ordered = mm(pick.astype(f32).astype(bf16), tail.astype(bf16)).astype(bf16)
    for k in range(4):
        B["low_z"][k] = ordered[16 * k : 16 * k + 16]
    for k in range(1, 4):
        wire.wait(B["two_x"].at[k - 1], 124 + k, place.at(0, 4 - k, 0))
    main = half_x[z].astype(f32)
    for k in range(3):
        main = main + B["two_x"][k].astype(f32)
    for k in range(4):
        B["low_x"][k] = main[24 * k : 24 * k + 24].astype(bf16)
    for k in (2, 1, 3):
        to = (y + k) % 4
        wire.send(B["low_x"].at[to], B["three_x"].at[k - 1], 130 + k, place.at(0, 0, k))
        wire.send(B["low_z"].at[to], B["three_z"].at[k - 1], 133 + k, place.at(0, 0, k))

    wire.wait(B["fin_p"].at[rows_b], 89, place.ym)
    wire.wait(B["fin_m"].at[rows_a], 91, place.yp)
    wire.wait(B["fin_p"].at[rows_a], 122, place.ym)
    wire.wait(B["fin_m"].at[rows_b], 123, place.yp)

    def total_of(first_row, rows):
        at = pl.ds(first_row, rows)
        return packed[row(0, c), at, :].astype(f32) + B["fin_p"][at, :].astype(f32) + B["fin_m"][at, :].astype(f32)

    for l in range(LAYERS):
        for b in range(8):
            gin[l, :, D * b : D * b + D] = total_of(576 * l + 48 * b, 48)
        for b in range(4):
            gdn[l, 48 * b : 48 * b + 48, :] = total_of(576 * l + D + 48 * b, 48)
    gcls_out[...] = total_of(PACK - 48, 48)[:, 0:128].T[0:CLASSES]

    for k in range(1, 4):
        wire.wait(B["three_x"].at[k - 1], 130 + k, place.at(0, 0, 4 - k))
        wire.wait(B["three_z"].at[k - 1], 133 + k, place.at(0, 0, 4 - k))
    main = B["low_x"][y].astype(f32)
    tail = B["low_z"][y].astype(f32)
    for k in range(3):
        main = main + B["three_x"][k].astype(f32)
        tail = tail + B["three_z"][k].astype(f32)
    out_in[...] = main
    for q in range(4):
        out_dn[:, D * q : D * q + D] = tail[3 * q : 3 * q + 3]
    out_pe[...] = tail[12:15, 0:192]
    out_pos[...] = tail[12:15, 256:272]
    wire.finish()


def finish_kernel(*refs):
    count = len(refs) // 3
    given, results, held = refs[:count], refs[count : 2 * count], refs[2 * count : 3 * count]
    sem = refs[-1]
    inward = [pltpu.make_async_copy(given[n], held[n], sem.at[0, n]) for n in range(count)]
    outward = [pltpu.make_async_copy(held[n], results[n], sem.at[1, n]) for n in range(count)]
    for copy in inward:
        copy.start()
    for copy, onward in zip(inward, outward):
        copy.wait()
        onward.start()
    for copy in outward:
        copy.wait()


def per_device(patches, labels, assign, patch_embed, positions, client_in, client_down, server_in, server_down, classifier):
    shapes = [
        ((1, CAP), f32),
        ((LAYERS, 48, 4 * D + FF), f32),
        ((LAYERS, 192, D), f32),
        ((CLASSES, 48), f32),
        ((24, D), f32),
        ((3, FF), f32),
        ((3, 192), f32),
        ((3, TOK), f32),
    ]
    scratch = list(CLIENT.values()) + list(SERVER.values()) + list(BUFFERS.values())
    results = pl.pallas_call(
        step_kernel,
        out_shape=[jax.ShapeDtypeStruct(*s) for s in shapes],
        in_specs=[VMEM] * 6 + [ANY] * 4,
        out_specs=[VMEM] * len(shapes),
        scratch_shapes=[pltpu.VMEM(*s) for s in scratch]
        + [
            pltpu.SemaphoreType.DMA((N_SEM,)),
            pltpu.SemaphoreType.DMA((N_SEM,)),
            pltpu.SemaphoreType.DMA((5,)),
            pltpu.SMEM((1, 128), jnp.int32),
        ],
        compiler_params=pltpu.CompilerParams(collective_id=0, has_side_effects=True, vmem_limit_bytes=67043328),
        name="step",
    )(
        patches.T,
        patch_embed,
        positions,
        assign.reshape(1, 128),
        labels.reshape(8, 128),
        classifier.transpose(2, 0, 1),
        client_in[None],
        client_down[None],
        server_in,
        server_down,
    )
    losses, gin, gdn, gcls, out_in, out_dn, out_pe, out_pos = pl.pallas_call(
        finish_kernel,
        out_shape=[jax.ShapeDtypeStruct(*s) for s in shapes],
        in_specs=[HBM] * len(shapes),
        out_specs=[HBM] * len(shapes),
        scratch_shapes=[pltpu.VMEM(*s) for s in shapes] + [pltpu.SemaphoreType.DMA((2, len(shapes)))],
        compiler_params=pltpu.CompilerParams(vmem_limit_bytes=67043328),
        name="finish",
    )(*results)
    return losses, out_pe.T, out_pos.T, out_in.T, out_dn.T, gin, gdn, gcls.T


def solution(mesh):
    in_specs = (
        P("client", None),
        P(),
        P(),
        P(),
        P(),
        P(),
        P(),
        P(None, "client", None),
        P(None, "client", None),
        P(),
    )
    out_specs = (
        P("client", None),
        P(None, "client"),
        P(None, "client"),
        P(None, "client"),
        P(None, "client"),
        P(None, "client", None),
        P(None, "client", None),
        P("client", None),
    )
    return jax.shard_map(per_device, mesh=mesh, in_specs=in_specs, out_specs=out_specs, check_vma=False)
```

```python
import math

import jax
import jax.numpy as jnp
from jax import lax
from jax.experimental import pallas as pl
from jax.experimental.pallas import tpu as pltpu
from jax.sharding import PartitionSpec as P

D = 384
FF = 1536
TOK = 16
IMG = 8
CLASSES = 10
SHARDS = 16
LAYERS = 2
CAP = 16
EPSILON = 1e-06
SCALE = 0.125
GELU_A = math.sqrt(2.0 / math.pi)
GELU_B = 0.044715
PACK = LAYERS * (D + FF // 8) + D // 8
CUT_A = 576
MAIN = 96
TAIL = 64
PART = 80
BLOCK = MAIN + TAIL

bf16 = jnp.bfloat16
f32 = jnp.float32
MESH = pl.DeviceIdType.MESH
VMEM = pl.BlockSpec(memory_space=pltpu.VMEM)
SMEM = pl.BlockSpec(memory_space=pltpu.SMEM)
ANY = pl.BlockSpec(memory_space=pl.ANY)
HBM = pl.BlockSpec(memory_space=pltpu.HBM)


def mm(a, b, ca=1, cb=0):
    return lax.dot_general(a, b, (((ca,), (cb,)), ((), ())), preferred_element_type=f32)


def iota(shape, dim):
    return lax.broadcasted_iota(jnp.int32, shape, dim)


def norm(v):
    centre = v - jnp.mean(v, axis=-1, keepdims=True)
    rstd = lax.rsqrt(jnp.mean(centre * centre, axis=-1, keepdims=True) + EPSILON)
    return centre * rstd, rstd


def norm_back(v, grad):
    hat, rstd = norm(v)
    along = jnp.mean(grad * hat, axis=-1, keepdims=True)
    return rstd * (grad - jnp.mean(grad, axis=-1, keepdims=True) - hat * along)


def rounded(v):
    return v.astype(bf16).astype(f32)


def head_masks(rows):
    low = (iota((rows, 128), 1) < 64).astype(f32)
    return low.astype(bf16), (1.0 - low).astype(bf16)


def two_heads(v):
    low, high = head_masks(v.shape[0])
    return jnp.concatenate([v * low, v * high], axis=0)


def merge_heads(v):
    rows = v.shape[0] // 2
    return jnp.where(iota((rows, 128), 1) < 64, v[:rows], v[rows:])


def block_forward(l, rows, S, win, wdn):
    x = S["x"][l]
    hat, _ = norm(x)
    u1 = hat.astype(bf16)
    S["u1"][l] = u1
    for n in range(3):
        cols = slice(D * n, D * n + D)
        S["qkv"][l, :, cols] = mm(u1, win[l, :, cols]).astype(bf16)
    same = ((iota((256, 128), 0) & 127) >> 4) == (iota((256, 128), 1) >> 4)
    for g in range(rows // 128):
        part = slice(128 * g, 128 * g + 128)
        for p in range(3):
            q2 = S["qkv"][l, part, 128 * p : 128 * p + 128]
            k2 = S["qkv"][l, part, D + 128 * p : D + 128 * p + 128]
            v2 = S["qkv"][l, part, 2 * D + 128 * p : 2 * D + 128 * p + 128]
            scores = mm(two_heads(q2), k2, 1, 1) * SCALE
            scores = jnp.where(same, scores, -1e30)
            grown = jnp.exp(scores - jnp.max(scores, axis=-1, keepdims=True))
            prob = grown / jnp.sum(grown, axis=-1, keepdims=True)
            S["prob"][l, 3 * g + p] = prob
            S["att"][l, part, 128 * p : 128 * p + 128] = merge_heads(mm(prob.astype(bf16), v2)).astype(bf16)
    x1 = S["x"][l] + mm(S["att"][l], win[l, :, 3 * D : 4 * D])
    S["x1"][l] = x1
    hat, _ = norm(x1)
    u2 = hat.astype(bf16)
    S["u2"][l] = u2
    for n in range(4):
        pre = mm(u2, win[l, :, 4 * D + D * n : 5 * D + D * n])
        S["pre"][l, :, D * n : D * n + D] = pre
        bent = jnp.tanh(GELU_A * (pre + GELU_B * pre * pre * pre))
        S["h"][l, :, D * n : D * n + D] = (0.5 * pre * (1.0 + bent)).astype(bf16)
    return S["x1"][l] + mm(S["h"][l], wdn[l])


def block_backward(l, rows, S, win, wdn, dy_ref, early=None):
    dyb = dy_ref[...].astype(bf16)
    S["dyb"][l] = dyb
    for n in range(4):
        cols = slice(D * n, D * n + D)
        dh = rounded(mm(dyb, wdn[l, cols, :], 1, 1))
        pre = S["pre"][l, :, cols]
        bent = jnp.tanh(GELU_A * (pre + GELU_B * pre * pre * pre))
        slope = 0.5 * (1.0 + bent) + 0.5 * pre * (1.0 - bent * bent) * GELU_A * (1.0 + 3.0 * GELU_B * pre * pre)
        S["dpre"][l, :, cols] = (dh * slope).astype(bf16)
    if early is not None:
        early()
    du2 = rounded(mm(S["dpre"][l], win[l, :, 4 * D :], 1, 1))
    dx1 = dy_ref[...] + norm_back(S["x1"][l], du2)
    dy_ref[...] = dx1
    dx1b = dx1.astype(bf16)
    S["dx1b"][l] = dx1b
    S["datt"][...] = mm(dx1b, win[l, :, 3 * D : 4 * D], 1, 1).astype(bf16)
    for g in range(rows // 128):
        part = slice(128 * g, 128 * g + 128)
        for p in range(3):
            cq = slice(128 * p, 128 * p + 128)
            ck = slice(D + 128 * p, D + 128 * p + 128)
            cv = slice(2 * D + 128 * p, 2 * D + 128 * p + 128)
            qs = two_heads(S["qkv"][l, part, cq])
            dos = two_heads(S["datt"][part, cq])
            prob = S["prob"][l, 3 * g + p]
            dprob = mm(dos, S["qkv"][l, part, cv], 1, 1)
            dscore = prob * (dprob - jnp.sum(prob * dprob, axis=-1, keepdims=True)) * SCALE
            dsb = dscore.astype(bf16)
            S["dqkv"][l, part, cq] = merge_heads(mm(dsb, S["qkv"][l, part, ck])).astype(bf16)
            S["dqkv"][l, part, ck] = mm(dsb, qs, 0, 0).astype(bf16)
            S["dqkv"][l, part, cv] = mm(prob.astype(bf16), dos, 0, 0).astype(bf16)
    du1 = rounded(mm(S["dqkv"][l], win[l, :, : 3 * D], 1, 1))
    dy_ref[...] = dy_ref[...] + norm_back(S["x"][l], du1)


def weight_pairs(S, l):
    pairs = []
    for n in range(3):
        pairs.append((n, S["u1"].at[l], S["dqkv"].at[l, :, pl.ds(D * n, D)]))
    pairs.append((3, S["att"].at[l], S["dx1b"].at[l]))
    for n in range(4):
        pairs.append((4 + n, S["u2"].at[l], S["dpre"].at[l, :, pl.ds(D * n, D)]))
    return pairs


def block_shapes(layers, rows):
    return dict(
        x=((layers + 1, rows, D), f32),
        x1=((layers, rows, D), f32),
        u1=((layers, rows, D), bf16),
        u2=((layers, rows, D), bf16),
        qkv=((layers, rows, 3 * D), bf16),
        prob=((layers, 3 * rows // 128, 256, 128), f32),
        att=((layers, rows, D), bf16),
        pre=((layers, rows, FF), f32),
        h=((layers, rows, FF), bf16),
        dyb=((layers, rows, D), bf16),
        dpre=((layers, rows, FF), bf16),
        dx1b=((layers, rows, D), bf16),
        datt=((rows, D), bf16),
        dqkv=((layers, rows, 3 * D), bf16),
        dy=((rows, D), f32),
    )


class Place:
    def __init__(self):
        me = lax.axis_index("client")
        self.me = me
        self.c, self.y, self.z, self.x = me % 2, me // 2 % 4, me // 8 % 4, me // 32
        self.r, self.group = me % 8, me // 8 * 8
        self.partner = me + 1 - 2 * self.c
        self.yp, self.ym = self.at(0, 0, 1), self.at(0, 0, 3)
        self.xp, self.xm = self.at(1, 0, 0), self.at(3, 0, 0)
        self.zp, self.zm = self.at(0, 1, 0), self.at(0, 3, 0)

    def at(self, dx, dz, dy):
        x, z, y = (self.x + dx) % 4, (self.z + dz) % 4, (self.y + dy) % 4
        return ((x * 4 + z) * 4 + y) * 2 + self.c

    def greet(self, group, plane):
        peers = []
        if group:
            peers += [self.group + (self.r + i) % 8 for i in range(1, 8)]
        if plane:
            peers += [self.xp, self.xm, self.zp, self.zm]
        barrier = pltpu.get_barrier_semaphore()
        for peer in peers:
            pl.semaphore_signal(barrier, inc=1, device_id=(peer,), device_id_type=MESH)
        pl.semaphore_wait(barrier, len(peers))


class Wire:
    def __init__(self, send_sem, recv_sem):
        self.send_sem, self.recv_sem, self.sent = send_sem, recv_sem, []

    def make(self, src, dst, k, device):
        return pltpu.make_async_remote_copy(
            src_ref=src,
            dst_ref=dst,
            send_sem=self.send_sem.at[k],
            recv_sem=self.recv_sem.at[k],
            device_id=(device,),
            device_id_type=MESH,
        )

    def send(self, src, dst, k, device):
        copy = self.make(src, dst, k, device)
        copy.start()
        self.sent.append(copy)

    def wait(self, landed, k, device):
        self.make(landed, landed, k, device).wait_recv()

    def finish(self):
        for copy in self.sent:
            copy.wait_send()


class Line:
    def __init__(self, wire, me, up, down, k, view):
        self.wire, self.me, self.up, self.down, self.k, self.view = wire, me, up, down, k, view

    def both(self, ref, k, device):
        self.wire.send(ref, ref, self.k + k, device)

    def send(self):
        self.both(self.view(self.me, 0), 0, self.up)
        self.both(self.view(self.me, 1), 1, self.down)
        self.both(self.view(self.me, 1), 2, self.up)
        self.both(self.view(self.me, 0), 3, self.down)

    def relay(self):
        left, right = (self.me + 3) % 4, (self.me + 1) % 4
        self.wire.wait(self.view(left, 0), self.k, self.down)
        self.both(self.view(left, 0), 4, self.up)
        self.wire.wait(self.view(right, 1), self.k + 1, self.up)
        self.both(self.view(right, 1), 5, self.down)

    def rest(self):
        left, right, far = (self.me + 3) % 4, (self.me + 1) % 4, (self.me + 2) % 4
        self.wire.wait(self.view(left, 1), self.k + 2, self.down)
        self.wire.wait(self.view(right, 0), self.k + 3, self.up)
        self.wire.wait(self.view(far, 0), self.k + 4, self.down)
        self.wire.wait(self.view(far, 1), self.k + 5, self.up)


def plane_gather(wire, place, buf, k0):
    x, z = place.x, place.z
    lines = (
        Line(wire, x, place.xp, place.xm, k0, lambda at, h: buf.at[at, z, pl.ds(2 * h, 2)]),
        Line(wire, z, place.zp, place.zm, k0 + 6, lambda at, h: buf.at[x, at, pl.ds(4 + 2 * h, 2)]),
        Line(wire, z, place.zp, place.zm, k0 + 12, lambda at, h: buf.at[pl.ds(2 * h, 2), at, pl.ds(0, 4)]),
        Line(wire, x, place.xp, place.xm, k0 + 18, lambda at, h: buf.at[at, pl.ds(2 * h, 2), pl.ds(4, 4)]),
    )

    def first():
        lines[0].send()
        lines[1].send()

    def second():
        lines[0].relay()
        lines[1].relay()

    def third():
        lines[0].rest()
        lines[2].send()
        lines[1].rest()
        lines[3].send()

    def fourth():
        lines[2].relay()
        lines[3].relay()

    def fifth():
        lines[2].rest()
        lines[3].rest()

    return first, second, third, fourth, fifth


def add_rows(start, stop, step, body):
    def run(i, carry):
        body(pl.ds(pl.multiple_of(start + i * step, 16), step))
        return carry

    lax.fori_loop(0, (stop - start) // step, run, 0)


def route(arow, labels, shard, rank_in):
    eye = iota((128, 128), 0) == iota((128, 128), 1)
    acol = jnp.sum(jnp.where(eye, arow.astype(f32), 0.0), axis=1, keepdims=True).astype(jnp.int32)
    earlier = (acol == arow) & (iota((128, 128), 0) < iota((128, 128), 1))
    rank = jnp.sum(earlier.astype(f32), axis=0, keepdims=True).astype(jnp.int32)
    chosen = (jnp.broadcast_to(arow, (CAP, 128)) == shard) & (
        jnp.broadcast_to(rank, (CAP, 128)) == iota((CAP, 128), 0)
    )
    selector = chosen.astype(f32).astype(bf16)
    take = (iota((128, 16), 0) == iota((128, 16), 1) * IMG + rank_in).astype(f32).astype(bf16)
    by_row = mm(labels.astype(f32).astype(bf16), take).astype(bf16)
    lift = ((iota((128, 8), 0) >> 4) == iota((128, 8), 1)).astype(f32).astype(bf16)
    tall = mm(lift, by_row)
    mine = (iota((128, 16), 0) & 15) == iota((128, 16), 1)
    label = jnp.sum(jnp.where(mine, tall, 0.0), axis=1, keepdims=True)
    onehot = (label == iota((128, CLASSES), 1).astype(f32)).astype(f32).astype(bf16)
    return selector, mm(selector, onehot), arow * CAP + rank


def slot_rows(selector, arrived):
    spread = (iota((128, 2048), 0) == (iota((128, 2048), 1) >> 4)).astype(f32).astype(bf16)
    wide = mm(selector, spread).astype(bf16)
    repeat = ((iota((256, CAP), 0) >> 4) == iota((256, CAP), 1)).astype(f32).astype(bf16)
    tall = mm(repeat, wide)
    same = (iota((256, 2048), 0) & 15) == (iota((256, 2048), 1) & 15)
    return mm(jnp.where(same, tall, 0.0).astype(bf16), arrived)


def head_loss(last, classes, hot):
    filled = jnp.sum(hot, axis=1, keepdims=True)
    mean = jnp.mean(last.reshape(CAP, TOK, D), axis=1)
    hat, _ = norm(mean)
    pooled = hat.astype(bf16)
    logits = mm(pooled, classes, 1, 1)
    top = jnp.max(logits, axis=1, keepdims=True)
    grown = jnp.exp(logits - top)
    total = jnp.sum(grown, axis=1, keepdims=True)
    per = (jnp.log(total) + top - jnp.sum(hot * logits, axis=1, keepdims=True)) * filled
    eye = iota((CAP, CAP), 0) == iota((CAP, CAP), 1)
    losses = jnp.sum(jnp.where(eye, per, 0.0), axis=0, keepdims=True)
    dlogits = ((grown / total) * filled - hot).astype(bf16)
    gcls = mm(pooled, dlogits, 0, 0).astype(bf16)
    dpooled = rounded(mm(dlogits, classes))
    dmean = norm_back(mean, dpooled) * (1.0 / TOK)
    dlast = jnp.broadcast_to(dmean[:, None, :], (CAP, TOK, D)).reshape(CAP * TOK, D)
    return losses, gcls, dlast


CLIENT = block_shapes(1, 128)
SERVER = block_shapes(LAYERS, 256)
BUFFERS = dict(
    arrived=((4, 4, IMG, TOK, D), bf16),
    win=((LAYERS, D, 4 * D + FF), bf16),
    wdn=((LAYERS, FF, D), bf16),
    win_c=((1, D, 4 * D + FF), bf16),
    wdn_c=((1, FF, D), bf16),
    win_s=((LAYERS, 48, 4 * D + FF), bf16),
    wdn_s=((LAYERS, 192, D), bf16),
    table=((1, 128), jnp.int32),
    cut=((IMG, TOK, D), bf16),
    packed=((8, PACK, D), bf16),
    swapped=((4, PACK, D), bf16),
    from_m=((CUT_A, D), bf16),
    from_p=((PACK - CUT_A, D), bf16),
    fin_p=((PACK, D), bf16),
    fin_m=((PACK, D), bf16),
    line_x=((4, 8, TOK, D), bf16),
    line_z=((4, 8, TOK, D), bf16),
    pick_x=((4, 8, TOK, D), bf16),
    pick_z=((4, 8, TOK, D), bf16),
    got_x=((3, 8, TOK, D), bf16),
    got_z=((3, 8, TOK, D), bf16),
    picked=((8, TOK, D), bf16),
    own=((IMG, TOK, D), bf16),
    order=((4, D, 512), bf16),
    dperm=((2, 128, 512), bf16),
    pp=((128, D), bf16),
    cpack=((16, 2, BLOCK, D), bf16),
    cswap=((16, BLOCK, D), bf16),
    cmine=((4, 4, BLOCK, D), bf16),
    hop_x=((2, 2, PART, D), bf16),
    hop_z=((2, 2, PART, D), bf16),
    end_x=((2, 4, PART, D), bf16),
    end_z=((2, 4, PART, D), bf16),
    half_x=((4, PART, D), bf16),
    half_z=((4, PART, D), bf16),
    two_x=((3, PART, D), bf16),
    two_z=((3, PART, D), bf16),
    low_x=((4, 24, D), bf16),
    low_z=((4, 16, D), bf16),
    three_x=((3, 24, D), bf16),
    three_z=((3, 16, D), bf16),
    gin=((LAYERS, 48, 4 * D + FF), f32),
    gdn=((LAYERS, 192, D), f32),
)
N_SEM = 160


def step_kernel(patches_t, embed, positions, arow, labels, classes, *refs):
    sources, refs = refs[:4], refs[4:]
    losses, gin, gdn, gcls_out, out_in, out_dn, out_pe, out_pos = refs[:8]
    refs = list(refs[8:])
    C = dict(zip(CLIENT, refs[: len(CLIENT)]))
    refs = refs[len(CLIENT) :]
    S = dict(zip(SERVER, refs[: len(SERVER)]))
    refs = refs[len(SERVER) :]
    B = dict(zip(BUFFERS, refs[: len(BUFFERS)]))
    send_sem, recv_sem, local_sem, source = refs[len(BUFFERS) :]
    win_c, wdn_c, win_s, wdn_s = B["win_c"], B["wdn_c"], B["win_s"], B["wdn_s"]
    loads = []
    for n, (src, dst) in enumerate(zip(sources, (win_c, wdn_c, win_s, wdn_s))):
        loads.append(pltpu.make_async_copy(src, dst, local_sem.at[n]))
    for n in (2, 3, 0, 1):
        loads[n].start()
    place = Place()
    x, z, y, c, r = place.x, place.z, place.y, place.c, place.r
    shard = place.me // 8
    win, wdn, arrived, packed = B["win"], B["wdn"], B["arrived"], B["packed"]
    place.greet(True, True)
    wire = Wire(send_sem, recv_sem)

    def owner(dy, other=False):
        return (y + dy) % 4 * 2 + (1 - c if other else c)

    def window(l, down, rank, part):
        if down:
            low, size = {None: (0, 192), 0: (0, 96), 1: (96, 96)}[part]
            return wdn.at[l, pl.ds(pl.multiple_of(rank * 192 + low, 16), size), :]
        cols = {None: pl.ds(0, 3072), 0: pl.ds(0, 1536), 1: pl.ds(1536, 1536)}[part]
        return win.at[l, pl.ds(pl.multiple_of(rank * 48, 16), 48), cols]

    pieces = [(l, down) for l in range(LAYERS) for down in (False, True)]
    base = {piece: 8 + 11 * n for n, piece in enumerate(pieces)}

    def own_part(piece, part):
        l, down = piece
        if down:
            return wdn_s.at[l, pl.ds(96 * part, 96), :]
        return win_s.at[l, :, pl.ds(1536 * part, 1536)]

    def spread_first(piece):
        for part, device in ((0, place.yp), (1, place.ym)):
            wire.send(own_part(piece, part), window(*piece, r, part), base[piece] + part, device)

    def spread_last(piece):
        for part, device in ((1, place.yp), (0, place.ym)):
            wire.send(own_part(piece, part), window(*piece, r, part), base[piece] + 3 - part, device)
        l, down = piece
        mine = (wdn_s if down else win_s).at[l]
        here = window(l, down, r, None)
        wire.send(mine, here, base[piece] + 6, place.partner)
        here[...] = mine[...]

    loads[2].wait()
    spread_first(pieces[0])
    for n in (3, 0, 1):
        loads[n].wait()

    def forward(piece):
        l, down = piece
        b = base[piece]
        left, right = owner(3), owner(1)
        half = window(l, down, left, 0)
        wire.wait(half, b + 0, place.ym)
        wire.send(half, half, b + 4, place.yp)
        half = window(l, down, right, 1)
        wire.wait(half, b + 1, place.yp)
        wire.send(half, half, b + 5, place.ym)

    def across(piece):
        l, down = piece
        b = base[piece]
        left, right, far = owner(3), owner(1), owner(2)
        wire.wait(window(l, down, left, 1), b + 2, place.ym)
        whole = window(l, down, left, None)
        wire.send(whole, whole, b + 7, place.partner)
        wire.wait(window(l, down, right, 0), b + 3, place.yp)
        whole = window(l, down, right, None)
        wire.send(whole, whole, b + 8, place.partner)
        for part, device in ((0, place.ym), (1, place.yp)):
            half = window(l, down, far, part)
            wire.wait(half, b + 4 + part, device)
            wire.send(half, half, b + 9 + part, place.partner)

    def settle(piece):
        l, down = piece
        b = base[piece]
        wire.wait(window(l, down, owner(0, True), None), b + 6, place.partner)
        wire.wait(window(l, down, owner(3, True), None), b + 7, place.partner)
        wire.wait(window(l, down, owner(1, True), None), b + 8, place.partner)
        for part in range(2):
            wire.wait(window(l, down, owner(2, True), part), b + 9 + part, place.partner)

    tiled = jnp.concatenate([positions[...].astype(f32)] * IMG, axis=0)
    C["x"][0] = mm(patches_t[...], embed[...], 0, 0) + tiled
    cut = block_forward(0, 128, C, win_c, wdn_c).astype(bf16)
    B["cut"][...] = cut.reshape(IMG, TOK, D)
    for i in range(1, 8):
        j = (r + i) % 8
        wire.send(B["cut"].at[j], arrived.at[x, z, r], i, place.group + j)
    spread_last(pieces[0])
    for piece in pieces[1:]:
        spread_first(piece)
        spread_last(piece)
    arrived[x, z, r] = B["cut"][r]
    selector, hot, table = route(arow[...], labels[...], shard, r)
    B["table"][...] = table
    to_scalar = pltpu.make_async_copy(B["table"], source, local_sem.at[4])
    to_scalar.start()
    first, second, third, fourth, fifth = plane_gather(wire, place, arrived, 52)
    for i in range(1, 8):
        j = (r - i + 8) % 8
        wire.wait(arrived.at[x, z, j], i, place.group + j)
    first()
    forward(pieces[0])
    second()
    col = iota((1, 512), 1)
    at = col & 15
    lane = ((col >> 4) & 15) * 24 + (col >> 8) * 3
    wanted = lane + (at // 3) * 6 + at % 3
    B["order"][0] = ((iota((D, 512), 0) == wanted) & (at < 12)).astype(f32).astype(bf16)
    for q in range(3):
        entry = jnp.maximum(at - 12, 0) + 4 * q
        wanted = lane + (entry // 3) * 6 + entry % 3
        B["order"][1 + q] = ((iota((D, 512), 0) == wanted) & (at >= 12)).astype(f32).astype(bf16)
    B["pp"][...] = (iota((128, D), 1) - 256 == (iota((128, D), 0) & 15)).astype(f32).astype(bf16)
    B["pp"][:, 0:192] = patches_t[...].T
    packed[:, PACK - 48 :, :] = jnp.zeros((8, 48, D), bf16)
    forward(pieces[1])
    third()
    forward(pieces[2])
    fourth()
    forward(pieces[3])
    across(pieces[0])
    fifth()
    across(pieces[1])
    settle(pieces[0])
    settle(pieces[1])

    S["x"][0] = slot_rows(selector, arrived[...].reshape(2048, D))
    S["x"][1] = block_forward(0, 256, S, win, wdn)
    across(pieces[2])
    across(pieces[3])
    settle(pieces[2])
    settle(pieces[3])
    S["x"][2] = block_forward(1, 256, S, win, wdn)
    to_scalar.wait()
    ours = iota((CLASSES, SHARDS, D), 1) == shard
    table = jnp.sum(jnp.where(ours, classes[...].astype(f32), 0.0), axis=1).astype(bf16)
    loss, gcls, dlast = head_loss(S["x"][LAYERS], table, hot)
    losses[...] = loss
    for k in range(8):
        packed[k, PACK - 48 :, 0:CLASSES] = gcls[48 * k : 48 * k + 48]
    S["dy"][...] = dlast

    def backward(i, carry):
        block_backward(LAYERS - 1 - i, 256, S, win, wdn, S["dy"])
        return carry

    lax.fori_loop(0, LAYERS, backward, 0)

    line_x, line_z = B["line_x"], B["line_z"]
    gcut = S["dy"][...].astype(bf16).reshape(CAP, TOK, D)
    line_x[x] = gcut[:8]
    line_z[z] = gcut[8:]
    lines = (
        Line(wire, x, place.xp, place.xm, 76, lambda at, h: line_x.at[at, pl.ds(4 * h, 4)]),
        Line(wire, z, place.zp, place.zm, 82, lambda at, h: line_z.at[at, pl.ds(4 * h, 4)]),
    )
    for line in lines:
        line.send()

    def server_weights(l):
        for b, u, dout in weight_pairs(S, l):
            val = mm(u[...], dout[...], 0, 0).astype(bf16)
            for k in range(8):
                packed[k, 576 * l + 48 * b : 576 * l + 48 * b + 48, :] = val[48 * k : 48 * k + 48]
        for n in range(4):
            val = mm(S["h"][l, :, D * n : D * n + D], S["dyb"][l], 0, 0).astype(bf16)
            for j in range(2):
                packed[2 * n + j, 576 * l + D : 576 * l + 576, :] = val[192 * j : 192 * j + 192]

    rows_a, rows_b = pl.ds(0, CUT_A), pl.ds(CUT_A, PACK - CUT_A)

    def row(k, core):
        return (y + k) % 4 * 2 + core

    def swap(part, k0):
        for k in (2, 1, 3, 0):
            wire.send(packed.at[row(k, 1 - c), part], B["swapped"].at[k, part], k0 + k, place.partner)

    def combine(k, part, k0, start, stop):
        wire.wait(B["swapped"].at[k, part], k0 + k, place.partner)

        def body(rows):
            total = packed[row(k, c), rows, :].astype(f32) + B["swapped"][k, rows, :].astype(f32)
            packed[row(k, c), rows, :] = total.astype(bf16)

        add_rows(start, stop, 48, body)

    def combine_a(k):
        combine(k, rows_a, 94, 0, CUT_A)

    def combine_b(k):
        combine(k, rows_b, 98, CUT_A, PACK)

    server_weights(1)
    swap(rows_b, 98)
    for line in lines:
        line.relay()
    combine_b(2)
    wire.send(packed.at[row(2, c), rows_b], B["from_p"], 102, place.ym)
    combine_b(1)
    wire.send(packed.at[row(1, c), rows_b], B["fin_p"].at[rows_b], 103, place.yp)
    for line in lines:
        line.rest()
    for k in (2, 1, 3, 0):
        for m in range(8):
            zd, xd = (z + k) % 4, (x + k) % 4
            at = source[0, (x * 4 + zd) * 8 + m]
            here = ((at >> 4) & 3 == z) & ((at & 15) < 8)
            B["pick_x"][k, m] = jnp.where(here, line_x[(at >> 6) & 3, at & 7].astype(f32), 0.0).astype(bf16)
            at = source[0, (xd * 4 + z) * 8 + m]
            here = ((at >> 6) & 3 == x) & ((at & 15) >= 8)
            B["pick_z"][k, m] = jnp.where(here, line_z[(at >> 4) & 3, at & 7].astype(f32), 0.0).astype(bf16)
        if k:
            wire.send(B["pick_x"].at[k], B["got_x"].at[k - 1], 87 + k, place.at(0, k, 0))
            wire.send(B["pick_z"].at[k], B["got_z"].at[k - 1], 90 + k, place.at(k, 0, 0))
    server_weights(0)
    swap(rows_a, 94)
    for k in range(1, 4):
        wire.wait(B["got_x"].at[k - 1], 87 + k, place.at(0, 4 - k, 0))
        wire.wait(B["got_z"].at[k - 1], 90 + k, place.at(4 - k, 0, 0))
    for m in range(8):
        piece = B["pick_x"][0, m].astype(f32) + B["pick_z"][0, m].astype(f32)
        for k in range(3):
            piece = piece + B["got_x"][k, m].astype(f32) + B["got_z"][k, m].astype(f32)
        B["picked"][m] = piece.astype(bf16)
    own = B["own"]
    own[r] = B["picked"][r]
    for i in range(1, 8):
        m = (r + i) % 8
        wire.send(B["picked"].at[m], own.at[r], 108 + i, place.group + m)
    combine_a(2)
    wire.send(packed.at[row(2, c), rows_a], B["from_m"], 104, place.yp)
    combine_a(3)
    wire.send(packed.at[row(3, c), rows_a], B["fin_m"].at[rows_a], 105, place.ym)
    combine_a(1)
    combine_b(3)
    for i in range(1, 8):
        j = (r - i + 8) % 8
        wire.wait(own.at[j], 108 + i, place.group + j)

    C["dy"][...] = own[...].reshape(128, D).astype(f32)
    cpack, cswap, cmine = B["cpack"], B["cswap"], B["cmine"]
    pairs = weight_pairs(C, 0)

    def emit(b, u, dout):
        val = mm(dout[...], u[...], 0, 0).astype(bf16)
        for i in range(2):
            for k in range(4):
                for core in range(2):
                    low = 192 * i + 48 * k + 24 * core
                    cpack[2 * b + i, core, 24 * k : 24 * k + 24] = val[low : low + 24]
        pair = pl.ds(2 * b, 2)
        wire.send(cpack.at[pair, 1 - c, pl.ds(0, MAIN)], cswap.at[pair, pl.ds(0, MAIN)], 116 + b, place.partner)

    def early():
        for pair in pairs[4:]:
            emit(*pair)
        B["dperm"][0] = mm(C["dyb"][0], B["order"][0]).astype(bf16)

    block_backward(0, 128, C, win_c, wdn_c, C["dy"], early)
    for pair in pairs[:4]:
        emit(*pair)
    last = C["dy"][...].astype(bf16)
    for q in range(4):
        val = mm(B["dperm"][0], C["h"][0, :, D * q : D * q + D], 0, 0)
        if q < 3:
            B["dperm"][1] = mm(last, B["order"][1 + q]).astype(bf16)
            val = val + mm(B["dperm"][1], B["pp"][...], 0, 0)
        val = val.astype(bf16)
        for core in range(2):
            for i in range(16):
                low = 256 * core + 16 * i
                cpack[i, core, MAIN + 16 * q : MAIN + 16 * q + 16] = val[low : low + 16]
    wire.send(cpack.at[:, 1 - c, pl.ds(MAIN, TAIL)], cswap.at[:, pl.ds(MAIN, TAIL)], 124, place.partner)

    X, Z = pl.ds(0, PART), pl.ds(PART, PART)

    def fold(low, high):
        for i in range(16):
            total = cpack[i, c, low:high].astype(f32) + cswap[i, low:high].astype(f32)
            cmine[i // 4, i % 4, low:high] = total.astype(bf16)

    def src_x(k, part):
        return cmine.at[(x + k) % 4, pl.ds(2 * part, 2), X]

    def src_z(k, part):
        return cmine.at[pl.ds(2 * part, 2), (z + k) % 4, Z]

    def ring_one(src, hop, end, up, down, k0):
        wire.send(src(2, 0), hop.at[0], k0, up)
        wire.send(src(2, 1), hop.at[1], k0 + 1, down)
        wire.send(src(1, 1), end.at[0, pl.ds(2, 2)], k0 + 2, up)
        wire.send(src(3, 0), end.at[1, pl.ds(0, 2)], k0 + 3, down)

    def ring_two(src, load, hop, end, up, down, k0):
        wire.wait(hop.at[0], k0, down)
        load(1, 0, hop)
        wire.send(src(1, 0), end.at[0, pl.ds(0, 2)], k0 + 4, up)
        wire.wait(hop.at[1], k0 + 1, up)
        load(3, 1, hop)
        wire.send(src(3, 1), end.at[1, pl.ds(2, 2)], k0 + 5, down)

    def ring_three(end, up, down, k0):
        wire.wait(end.at[0, pl.ds(2, 2)], k0 + 2, down)
        wire.wait(end.at[1, pl.ds(0, 2)], k0 + 3, up)
        wire.wait(end.at[0, pl.ds(0, 2)], k0 + 4, down)
        wire.wait(end.at[1, pl.ds(2, 2)], k0 + 5, up)

    def load_x(k, part, hop):
        to = (x + k) % 4
        for i in range(2):
            at = 2 * part + i
            cmine[to, at, :PART] = (cmine[to, at, :PART].astype(f32) + hop[part, i].astype(f32)).astype(bf16)

    def load_z(k, part, hop):
        to = (z + k) % 4
        for i in range(2):
            at = 2 * part + i
            cmine[at, to, PART:] = (cmine[at, to, PART:].astype(f32) + hop[part, i].astype(f32)).astype(bf16)

    for b in (4, 5, 6, 7, 0, 1, 2, 3):
        wire.wait(cswap.at[pl.ds(2 * b, 2), pl.ds(0, MAIN)], 116 + b, place.partner)
    fold(0, PART)
    ring_one(src_x, B["hop_x"], B["end_x"], place.xp, place.xm, 125)
    wire.wait(cswap.at[:, pl.ds(MAIN, TAIL)], 124, place.partner)
    fold(PART, BLOCK)
    ring_one(src_z, B["hop_z"], B["end_z"], place.zp, place.zm, 131)

    wire.wait(B["from_m"], 104, place.ym)

    def add_a(rows):
        packed[row(1, c), rows, :] = (packed[row(1, c), rows, :].astype(f32) + B["from_m"][rows, :].astype(f32)).astype(bf16)

    add_rows(0, CUT_A, 48, add_a)
    wire.send(packed.at[row(1, c), rows_a], B["fin_p"].at[rows_a], 106, place.yp)
    wire.wait(B["from_p"], 102, place.yp)

    def add_b(i, carry):
        here = pl.ds(pl.multiple_of(i * 48, 16), 48)
        rows = pl.ds(pl.multiple_of(CUT_A + i * 48, 16), 48)
        packed[row(3, c), rows, :] = (packed[row(3, c), rows, :].astype(f32) + B["from_p"][here, :].astype(f32)).astype(bf16)
        return carry

    lax.fori_loop(0, (PACK - CUT_A) // 48, add_b, 0)
    wire.send(packed.at[row(3, c), rows_b], B["fin_m"].at[rows_b], 107, place.ym)

    ring_two(src_x, load_x, B["hop_x"], B["end_x"], place.xp, place.xm, 125)
    ring_two(src_z, load_z, B["hop_z"], B["end_z"], place.zp, place.zm, 131)
    half_x, half_z = B["half_x"], B["half_z"]
    ring_three(B["end_x"], place.xp, place.xm, 125)
    for i in range(4):
        total = cmine[x, i, :PART].astype(f32) + B["end_x"][0, i].astype(f32) + B["end_x"][1, i].astype(f32)
        half_x[i] = total.astype(bf16)
    for k in (2, 1, 3):
        wire.send(half_x.at[(z + k) % 4], B["two_x"].at[k - 1], 136 + k, place.at(0, k, 0))
    ring_three(B["end_z"], place.zp, place.zm, 131)
    for i in range(4):
        total = cmine[i, z, PART:].astype(f32) + B["end_z"][0, i].astype(f32) + B["end_z"][1, i].astype(f32)
        half_z[i] = total.astype(bf16)
    for k in (2, 1, 3):
        wire.send(half_z.at[(x + k) % 4], B["two_z"].at[k - 1], 139 + k, place.at(k, 0, 0))
    combine_a(0)
    combine_b(0)
    for k in range(1, 4):
        wire.wait(B["two_x"].at[k - 1], 136 + k, place.at(0, 4 - k, 0))
    upper = half_x[z].astype(f32)
    for k in range(3):
        upper = upper + B["two_x"][k].astype(f32)
    for k in range(1, 4):
        wire.wait(B["two_z"].at[k - 1], 139 + k, place.at(4 - k, 0, 0))
    lower = half_z[x].astype(f32)
    for k in range(3):
        lower = lower + B["two_z"][k].astype(f32)
    line, column = iota((64, TAIL), 0), iota((64, TAIL), 1)
    inside, owner_y = line & 15, line >> 4
    entry = owner_y * 3 + inside % 3
    spot = jnp.where(inside < 12, (inside // 3) * 16 + entry, (entry // 4) * 16 + 12 + entry % 4)
    pick = (column == spot) & (inside < 15)
    ordered = mm(pick.astype(f32).astype(bf16), lower[16:].astype(bf16)).astype(bf16)
    main = jnp.concatenate([upper, lower[:16]], axis=0).astype(bf16)
    for k in range(4):
        B["low_x"][k] = main[24 * k : 24 * k + 24]
        B["low_z"][k] = ordered[16 * k : 16 * k + 16]
    for k in (2, 1, 3):
        to = (y + k) % 4
        wire.send(B["low_x"].at[to], B["three_x"].at[k - 1], 142 + k, place.at(0, 0, k))
        wire.send(B["low_z"].at[to], B["three_z"].at[k - 1], 145 + k, place.at(0, 0, k))

    wire.wait(B["fin_p"].at[rows_b], 103, place.ym)
    wire.wait(B["fin_m"].at[rows_a], 105, place.yp)
    wire.wait(B["fin_p"].at[rows_a], 106, place.ym)
    wire.wait(B["fin_m"].at[rows_b], 107, place.yp)

    def total_of(first_row, rows):
        at = pl.ds(first_row, rows)
        return packed[row(0, c), at, :].astype(f32) + B["fin_p"][at, :].astype(f32) + B["fin_m"][at, :].astype(f32)

    for l in range(LAYERS):
        for b in range(8):
            B["gin"][l, :, D * b : D * b + D] = total_of(576 * l + 48 * b, 48)
        for b in range(4):
            B["gdn"][l, 48 * b : 48 * b + 48, :] = total_of(576 * l + D + 48 * b, 48)
    leaving = [
        pltpu.make_async_copy(B["gin"], gin, local_sem.at[5]),
        pltpu.make_async_copy(B["gdn"], gdn, local_sem.at[6]),
    ]
    for copy in leaving:
        copy.start()
    gcls_out[...] = total_of(PACK - 48, 48)[:, 0:128].T[0:CLASSES]

    for k in range(1, 4):
        wire.wait(B["three_x"].at[k - 1], 142 + k, place.at(0, 0, 4 - k))
        wire.wait(B["three_z"].at[k - 1], 145 + k, place.at(0, 0, 4 - k))
    main = B["low_x"][y].astype(f32)
    tail = B["low_z"][y].astype(f32)
    for k in range(3):
        main = main + B["three_x"][k].astype(f32)
        tail = tail + B["three_z"][k].astype(f32)
    out_in[...] = main
    for q in range(4):
        out_dn[:, D * q : D * q + D] = tail[3 * q : 3 * q + 3]
    out_pe[...] = tail[12:15, 0:192]
    out_pos[...] = tail[12:15, 256:272]
    for copy in leaving:
        copy.wait()
    wire.finish()


def finish_kernel(*refs):
    count = len(refs) // 3
    given, results, held = refs[:count], refs[count : 2 * count], refs[2 * count : 3 * count]
    sem = refs[-1]
    inward = [pltpu.make_async_copy(given[n], held[n], sem.at[0, n]) for n in range(count)]
    outward = [pltpu.make_async_copy(held[n], results[n], sem.at[1, n]) for n in range(count)]
    for copy in inward:
        copy.start()
    for copy, onward in zip(inward, outward):
        copy.wait()
        onward.start()
    for copy in outward:
        copy.wait()


def per_device(patches, labels, assign, patch_embed, positions, client_in, client_down, server_in, server_down, classifier):
    shapes = [
        ((1, CAP), f32),
        ((LAYERS, 48, 4 * D + FF), f32),
        ((LAYERS, 192, D), f32),
        ((CLASSES, 48), f32),
        ((24, D), f32),
        ((3, FF), f32),
        ((3, 192), f32),
        ((3, TOK), f32),
    ]
    scratch = list(CLIENT.values()) + list(SERVER.values()) + list(BUFFERS.values())
    results = pl.pallas_call(
        step_kernel,
        out_shape=[jax.ShapeDtypeStruct(*s) for s in shapes],
        in_specs=[VMEM] * 6 + [ANY] * 4,
        out_specs=[VMEM, HBM, HBM] + [VMEM] * 5,
        scratch_shapes=[pltpu.VMEM(*s) for s in scratch]
        + [
            pltpu.SemaphoreType.DMA((N_SEM,)),
            pltpu.SemaphoreType.DMA((N_SEM,)),
            pltpu.SemaphoreType.DMA((7,)),
            pltpu.SMEM((1, 128), jnp.int32),
        ],
        compiler_params=pltpu.CompilerParams(collective_id=0, has_side_effects=True, vmem_limit_bytes=67043328),
        name="step",
    )(
        patches.T,
        patch_embed,
        positions,
        assign.reshape(1, 128),
        labels.reshape(8, 128),
        classifier.transpose(2, 0, 1),
        client_in[None],
        client_down[None],
        server_in,
        server_down,
    )
    losses, gin, gdn, gcls, out_in, out_dn, out_pe, out_pos = pl.pallas_call(
        finish_kernel,
        out_shape=[jax.ShapeDtypeStruct(*s) for s in shapes],
        in_specs=[HBM] * len(shapes),
        out_specs=[HBM] * len(shapes),
        scratch_shapes=[pltpu.VMEM(*s) for s in shapes] + [pltpu.SemaphoreType.DMA((2, len(shapes)))],
        compiler_params=pltpu.CompilerParams(vmem_limit_bytes=67043328),
        name="finish",
    )(*results)
    return losses, out_pe.T, out_pos.T, out_in.T, out_dn.T, gin, gdn, gcls.T


def solution(mesh):
    in_specs = (
        P("client", None),
        P(),
        P(),
        P(),
        P(),
        P(),
        P(),
        P(None, "client", None),
        P(None, "client", None),
        P(),
    )
    out_specs = (
        P("client", None),
        P(None, "client"),
        P(None, "client"),
        P(None, "client"),
        P(None, "client"),
        P(None, "client", None),
        P(None, "client", None),
        P("client", None),
    )
    return jax.shard_map(per_device, mesh=mesh, in_specs=in_specs, out_specs=out_specs, check_vma=False)
```

```python
import math

import jax
import jax.numpy as jnp
from jax import lax
from jax.experimental import pallas as pl
from jax.experimental.pallas import tpu as pltpu
from jax.sharding import PartitionSpec as P

D = 384
FF = 1536
TOK = 16
IMG = 8
CLASSES = 10
SHARDS = 16
LAYERS = 2
CAP = 16
EPSILON = 1e-06
SCALE = 0.125
GELU_A = math.sqrt(2.0 / math.pi)
GELU_B = 0.044715
PACK = LAYERS * (D + FF // 8) + D // 8
CUT_A = 576
MAIN = 96
TAIL = 64
PART = 80
BLOCK = MAIN + TAIL

bf16 = jnp.bfloat16
f32 = jnp.float32
MESH = pl.DeviceIdType.MESH
VMEM = pl.BlockSpec(memory_space=pltpu.VMEM)
SMEM = pl.BlockSpec(memory_space=pltpu.SMEM)
ANY = pl.BlockSpec(memory_space=pl.ANY)
HBM = pl.BlockSpec(memory_space=pltpu.HBM)


def mm(a, b, ca=1, cb=0):
    return lax.dot_general(a, b, (((ca,), (cb,)), ((), ())), preferred_element_type=f32)


def iota(shape, dim):
    return lax.broadcasted_iota(jnp.int32, shape, dim)


def norm(v):
    centre = v - jnp.mean(v, axis=-1, keepdims=True)
    rstd = lax.rsqrt(jnp.mean(centre * centre, axis=-1, keepdims=True) + EPSILON)
    return centre * rstd, rstd


def norm_back(v, grad):
    hat, rstd = norm(v)
    along = jnp.mean(grad * hat, axis=-1, keepdims=True)
    return rstd * (grad - jnp.mean(grad, axis=-1, keepdims=True) - hat * along)


def rounded(v):
    return v.astype(bf16).astype(f32)


def head_masks(rows):
    low = (iota((rows, 128), 1) < 64).astype(f32)
    return low.astype(bf16), (1.0 - low).astype(bf16)


def two_heads(v):
    low, high = head_masks(v.shape[0])
    return jnp.concatenate([v * low, v * high], axis=0)


def merge_heads(v):
    rows = v.shape[0] // 2
    return jnp.where(iota((rows, 128), 1) < 64, v[:rows], v[rows:])


def block_forward(l, rows, S, win, middle=None):
    x = S["x"][l]
    hat, _ = norm(x)
    u1 = hat.astype(bf16)
    S["u1"][l] = u1
    for n in range(3):
        cols = slice(D * n, D * n + D)
        S["qkv"][l, :, cols] = mm(u1, win[l, :, cols]).astype(bf16)
    same = ((iota((256, 128), 0) & 127) >> 4) == (iota((256, 128), 1) >> 4)
    for g in range(rows // 128):
        part = slice(128 * g, 128 * g + 128)
        for p in range(3):
            q2 = S["qkv"][l, part, 128 * p : 128 * p + 128]
            k2 = S["qkv"][l, part, D + 128 * p : D + 128 * p + 128]
            v2 = S["qkv"][l, part, 2 * D + 128 * p : 2 * D + 128 * p + 128]
            scores = mm(two_heads(q2), k2, 1, 1) * SCALE
            scores = jnp.where(same, scores, -1e30)
            grown = jnp.exp(scores - jnp.max(scores, axis=-1, keepdims=True))
            prob = grown / jnp.sum(grown, axis=-1, keepdims=True)
            S["prob"][l, 3 * g + p] = prob
            S["att"][l, part, 128 * p : 128 * p + 128] = merge_heads(mm(prob.astype(bf16), v2)).astype(bf16)
    x1 = S["x"][l] + mm(S["att"][l], win[l, :, 3 * D : 4 * D])
    S["x1"][l] = x1
    hat, _ = norm(x1)
    u2 = hat.astype(bf16)
    S["u2"][l] = u2
    if middle is not None:
        middle()
    for n in range(4):
        pre = mm(u2, win[l, :, 4 * D + D * n : 5 * D + D * n])
        S["pre"][l, :, D * n : D * n + D] = pre
        bent = jnp.tanh(GELU_A * (pre + GELU_B * pre * pre * pre))
        S["h"][l, :, D * n : D * n + D] = (0.5 * pre * (1.0 + bent)).astype(bf16)


def block_end(l, S, wdn):
    return S["x1"][l] + mm(S["h"][l], wdn[l])


def block_backward(l, rows, S, win, wdn, dy_ref, early=None):
    dyb = dy_ref[...].astype(bf16)
    S["dyb"][l] = dyb
    for n in range(4):
        cols = slice(D * n, D * n + D)
        dh = rounded(mm(dyb, wdn[l, cols, :], 1, 1))
        pre = S["pre"][l, :, cols]
        bent = jnp.tanh(GELU_A * (pre + GELU_B * pre * pre * pre))
        slope = 0.5 * (1.0 + bent) + 0.5 * pre * (1.0 - bent * bent) * GELU_A * (1.0 + 3.0 * GELU_B * pre * pre)
        S["dpre"][l, :, cols] = (dh * slope).astype(bf16)
    if early is not None:
        early()
    du2 = rounded(mm(S["dpre"][l], win[l, :, 4 * D :], 1, 1))
    dx1 = dy_ref[...] + norm_back(S["x1"][l], du2)
    dy_ref[...] = dx1
    dx1b = dx1.astype(bf16)
    S["dx1b"][l] = dx1b
    S["datt"][...] = mm(dx1b, win[l, :, 3 * D : 4 * D], 1, 1).astype(bf16)
    for g in range(rows // 128):
        part = slice(128 * g, 128 * g + 128)
        for p in range(3):
            cq = slice(128 * p, 128 * p + 128)
            ck = slice(D + 128 * p, D + 128 * p + 128)
            cv = slice(2 * D + 128 * p, 2 * D + 128 * p + 128)
            qs = two_heads(S["qkv"][l, part, cq])
            dos = two_heads(S["datt"][part, cq])
            prob = S["prob"][l, 3 * g + p]
            dprob = mm(dos, S["qkv"][l, part, cv], 1, 1)
            dscore = prob * (dprob - jnp.sum(prob * dprob, axis=-1, keepdims=True)) * SCALE
            dsb = dscore.astype(bf16)
            S["dqkv"][l, part, cq] = merge_heads(mm(dsb, S["qkv"][l, part, ck])).astype(bf16)
            S["dqkv"][l, part, ck] = mm(dsb, qs, 0, 0).astype(bf16)
            S["dqkv"][l, part, cv] = mm(prob.astype(bf16), dos, 0, 0).astype(bf16)
    du1 = rounded(mm(S["dqkv"][l], win[l, :, : 3 * D], 1, 1))
    dy_ref[...] = dy_ref[...] + norm_back(S["x"][l], du1)


def weight_pairs(S, l):
    pairs = []
    for n in range(3):
        pairs.append((n, S["u1"].at[l], S["dqkv"].at[l, :, pl.ds(D * n, D)]))
    pairs.append((3, S["att"].at[l], S["dx1b"].at[l]))
    for n in range(4):
        pairs.append((4 + n, S["u2"].at[l], S["dpre"].at[l, :, pl.ds(D * n, D)]))
    return pairs


def block_shapes(layers, rows):
    return dict(
        x=((layers + 1, rows, D), f32),
        x1=((layers, rows, D), f32),
        u1=((layers, rows, D), bf16),
        u2=((layers, rows, D), bf16),
        qkv=((layers, rows, 3 * D), bf16),
        prob=((layers, 3 * rows // 128, 256, 128), f32),
        att=((layers, rows, D), bf16),
        pre=((layers, rows, FF), f32),
        h=((layers, rows, FF), bf16),
        dyb=((layers, rows, D), bf16),
        dpre=((layers, rows, FF), bf16),
        dx1b=((layers, rows, D), bf16),
        datt=((rows, D), bf16),
        dqkv=((layers, rows, 3 * D), bf16),
        dy=((rows, D), f32),
    )


class Place:
    def __init__(self):
        me = lax.axis_index("client")
        self.me = me
        self.c, self.y, self.z, self.x = me % 2, me // 2 % 4, me // 8 % 4, me // 32
        self.r, self.group = me % 8, me // 8 * 8
        self.partner = me + 1 - 2 * self.c
        self.yp, self.ym = self.at(0, 0, 1), self.at(0, 0, 3)
        self.xp, self.xm = self.at(1, 0, 0), self.at(3, 0, 0)
        self.zp, self.zm = self.at(0, 1, 0), self.at(0, 3, 0)

    def at(self, dx, dz, dy):
        x, z, y = (self.x + dx) % 4, (self.z + dz) % 4, (self.y + dy) % 4
        return ((x * 4 + z) * 4 + y) * 2 + self.c

    def greet(self, group, plane):
        peers = []
        if group:
            peers += [self.group + (self.r + i) % 8 for i in range(1, 8)]
        if plane:
            peers += [self.xp, self.xm, self.zp, self.zm]
        barrier = pltpu.get_barrier_semaphore()
        for peer in peers:
            pl.semaphore_signal(barrier, inc=1, device_id=(peer,), device_id_type=MESH)
        pl.semaphore_wait(barrier, len(peers))


class Wire:
    def __init__(self, send_sem, recv_sem):
        self.send_sem, self.recv_sem, self.sent = send_sem, recv_sem, []

    def make(self, src, dst, k, device):
        return pltpu.make_async_remote_copy(
            src_ref=src,
            dst_ref=dst,
            send_sem=self.send_sem.at[k],
            recv_sem=self.recv_sem.at[k],
            device_id=(device,),
            device_id_type=MESH,
        )

    def send(self, src, dst, k, device):
        copy = self.make(src, dst, k, device)
        copy.start()
        self.sent.append(copy)

    def wait(self, landed, k, device):
        self.make(landed, landed, k, device).wait_recv()

    def finish(self):
        for copy in self.sent:
            copy.wait_send()


class Line:
    def __init__(self, wire, me, up, down, k, view):
        self.wire, self.me, self.up, self.down, self.k, self.view = wire, me, up, down, k, view

    def both(self, ref, k, device):
        self.wire.send(ref, ref, self.k + k, device)

    def send(self):
        self.both(self.view(self.me, 0), 0, self.up)
        self.both(self.view(self.me, 1), 1, self.down)
        self.both(self.view(self.me, 1), 2, self.up)
        self.both(self.view(self.me, 0), 3, self.down)

    def relay(self):
        left, right = (self.me + 3) % 4, (self.me + 1) % 4
        self.wire.wait(self.view(left, 0), self.k, self.down)
        self.both(self.view(left, 0), 4, self.up)
        self.wire.wait(self.view(right, 1), self.k + 1, self.up)
        self.both(self.view(right, 1), 5, self.down)

    def rest(self):
        left, right, far = (self.me + 3) % 4, (self.me + 1) % 4, (self.me + 2) % 4
        self.wire.wait(self.view(left, 1), self.k + 2, self.down)
        self.wire.wait(self.view(right, 0), self.k + 3, self.up)
        self.wire.wait(self.view(far, 0), self.k + 4, self.down)
        self.wire.wait(self.view(far, 1), self.k + 5, self.up)


def plane_gather(wire, place, buf, k0):
    x, z = place.x, place.z
    lines = (
        Line(wire, x, place.xp, place.xm, k0, lambda at, h: buf.at[at, z, pl.ds(2 * h, 2)]),
        Line(wire, z, place.zp, place.zm, k0 + 6, lambda at, h: buf.at[x, at, pl.ds(4 + 2 * h, 2)]),
        Line(wire, z, place.zp, place.zm, k0 + 12, lambda at, h: buf.at[pl.ds(2 * h, 2), at, pl.ds(0, 4)]),
        Line(wire, x, place.xp, place.xm, k0 + 18, lambda at, h: buf.at[at, pl.ds(2 * h, 2), pl.ds(4, 4)]),
    )

    def first():
        lines[0].send()
        lines[1].send()

    def second():
        lines[0].relay()
        lines[1].relay()

    def third():
        lines[0].rest()
        lines[2].send()
        lines[1].rest()
        lines[3].send()

    def fourth():
        lines[2].relay()
        lines[3].relay()

    def fifth():
        lines[2].rest()
        lines[3].rest()

    return first, second, third, fourth, fifth


def add_rows(start, stop, step, body):
    def run(i, carry):
        body(pl.ds(pl.multiple_of(start + i * step, 16), step))
        return carry

    lax.fori_loop(0, (stop - start) // step, run, 0)


def route(arow, labels, shard, rank_in):
    eye = iota((128, 128), 0) == iota((128, 128), 1)
    acol = jnp.sum(jnp.where(eye, arow.astype(f32), 0.0), axis=1, keepdims=True).astype(jnp.int32)
    earlier = (acol == arow) & (iota((128, 128), 0) < iota((128, 128), 1))
    rank = jnp.sum(earlier.astype(f32), axis=0, keepdims=True).astype(jnp.int32)
    chosen = (jnp.broadcast_to(arow, (CAP, 128)) == shard) & (
        jnp.broadcast_to(rank, (CAP, 128)) == iota((CAP, 128), 0)
    )
    selector = chosen.astype(f32).astype(bf16)
    take = (iota((128, 16), 0) == iota((128, 16), 1) * IMG + rank_in).astype(f32).astype(bf16)
    by_row = mm(labels.astype(f32).astype(bf16), take).astype(bf16)
    lift = ((iota((128, 8), 0) >> 4) == iota((128, 8), 1)).astype(f32).astype(bf16)
    tall = mm(lift, by_row)
    mine = (iota((128, 16), 0) & 15) == iota((128, 16), 1)
    label = jnp.sum(jnp.where(mine, tall, 0.0), axis=1, keepdims=True)
    onehot = (label == iota((128, CLASSES), 1).astype(f32)).astype(f32).astype(bf16)
    return selector, mm(selector, onehot), arow * CAP + rank


def slot_rows(selector, arrived):
    spread = (iota((128, 2048), 0) == (iota((128, 2048), 1) >> 4)).astype(f32).astype(bf16)
    wide = mm(selector, spread).astype(bf16)
    repeat = ((iota((256, CAP), 0) >> 4) == iota((256, CAP), 1)).astype(f32).astype(bf16)
    tall = mm(repeat, wide)
    same = (iota((256, 2048), 0) & 15) == (iota((256, 2048), 1) & 15)
    return mm(jnp.where(same, tall, 0.0).astype(bf16), arrived)


def head_loss(last, classes, hot):
    filled = jnp.sum(hot, axis=1, keepdims=True)
    mean = jnp.mean(last.reshape(CAP, TOK, D), axis=1)
    hat, _ = norm(mean)
    pooled = hat.astype(bf16)
    logits = mm(pooled, classes, 1, 1)
    top = jnp.max(logits, axis=1, keepdims=True)
    grown = jnp.exp(logits - top)
    total = jnp.sum(grown, axis=1, keepdims=True)
    per = (jnp.log(total) + top - jnp.sum(hot * logits, axis=1, keepdims=True)) * filled
    eye = iota((CAP, CAP), 0) == iota((CAP, CAP), 1)
    losses = jnp.sum(jnp.where(eye, per, 0.0), axis=0, keepdims=True)
    dlogits = ((grown / total) * filled - hot).astype(bf16)
    gcls = mm(pooled, dlogits, 0, 0).astype(bf16)
    dpooled = rounded(mm(dlogits, classes))
    dmean = norm_back(mean, dpooled) * (1.0 / TOK)
    dlast = jnp.broadcast_to(dmean[:, None, :], (CAP, TOK, D)).reshape(CAP * TOK, D)
    return losses, gcls, dlast


CLIENT = block_shapes(1, 128)
SERVER = block_shapes(LAYERS, 256)
BUFFERS = dict(
    arrived=((4, 4, IMG, TOK, D), bf16),
    win=((LAYERS, D, 4 * D + FF), bf16),
    wdn=((LAYERS, FF, D), bf16),
    win_c=((1, D, 4 * D + FF), bf16),
    wdn_c=((1, FF, D), bf16),
    win_s=((LAYERS, 48, 4 * D + FF), bf16),
    wdn_s=((LAYERS, 192, D), bf16),
    table=((1, 128), jnp.int32),
    pout=((IMG, TOK, 256), bf16),
    pin=((IMG, TOK, 256), bf16),
    packed=((8, PACK, D), bf16),
    swapped=((4, PACK, D), bf16),
    from_m=((CUT_A, D), bf16),
    from_p=((PACK - CUT_A, D), bf16),
    fin_p=((PACK, D), bf16),
    fin_m=((PACK, D), bf16),
    line_x=((4, 8, TOK, D), bf16),
    line_z=((4, 8, TOK, D), bf16),
    pick_x=((4, 8, TOK, D), bf16),
    pick_z=((4, 8, TOK, D), bf16),
    ret_x=((2, 4, TOK, D), bf16),
    ret_z=((2, 4, TOK, D), bf16),
    got_x=((2, 8, TOK, D), bf16),
    got_z=((2, 8, TOK, D), bf16),
    order=((4, D, 512), bf16),
    dperm=((2, 128, 512), bf16),
    pp=((128, D), bf16),
    cpack=((16, 2, BLOCK, D), bf16),
    cswap=((16, BLOCK, D), bf16),
    cmine=((4, 4, BLOCK, D), bf16),
    hop_x=((2, 2, PART, D), bf16),
    hop_z=((2, 2, PART, D), bf16),
    end_x=((2, 4, PART, D), bf16),
    end_z=((2, 4, PART, D), bf16),
    half_x=((4, PART, D), bf16),
    half_z=((4, PART, D), bf16),
    two_x=((3, PART, D), bf16),
    two_z=((3, PART, D), bf16),
    low_x=((4, 24, D), bf16),
    low_z=((4, 16, D), bf16),
    three_x=((3, 24, D), bf16),
    three_z=((3, 16, D), bf16),
    gin=((LAYERS, 48, 4 * D + FF), f32),
    gdn=((LAYERS, 192, D), f32),
)
N_SEM = 160


def step_kernel(patches_t, embed, positions, arow, labels, classes, *refs):
    sources, refs = refs[:4], refs[4:]
    losses, gin, gdn, gcls_out, out_in, out_dn, out_pe, out_pos = refs[:8]
    refs = list(refs[8:])
    C = dict(zip(CLIENT, refs[: len(CLIENT)]))
    refs = refs[len(CLIENT) :]
    S = dict(zip(SERVER, refs[: len(SERVER)]))
    refs = refs[len(SERVER) :]
    B = dict(zip(BUFFERS, refs[: len(BUFFERS)]))
    send_sem, recv_sem, local_sem, source = refs[len(BUFFERS) :]
    win_c, wdn_c, win_s, wdn_s = B["win_c"], B["wdn_c"], B["win_s"], B["wdn_s"]
    loads = []
    for n, (src, dst) in enumerate(zip(sources, (win_c, wdn_c, win_s, wdn_s))):
        loads.append(pltpu.make_async_copy(src, dst, local_sem.at[n]))
    for n in (2, 3, 0, 1):
        loads[n].start()
    place = Place()
    x, z, y, c, r = place.x, place.z, place.y, place.c, place.r
    shard = place.me // 8
    win, wdn, arrived, packed = B["win"], B["wdn"], B["arrived"], B["packed"]
    B["pout"][...] = jnp.zeros_like(B["pout"])
    B["pout"][:, :, 0:192] = patches_t[...].T.reshape(IMG, TOK, 192)
    place.greet(True, True)
    wire = Wire(send_sem, recv_sem)

    for i in range(1, 8):
        j = (r + i) % 8
        wire.send(B["pout"].at[j], B["pin"].at[r], i, place.group + j)
    B["pin"][r] = B["pout"][r]

    def owner(dy, other=False):
        return (y + dy) % 4 * 2 + (1 - c if other else c)

    def window(l, down, rank, part):
        if down:
            low, size = {None: (0, 192), 0: (0, 96), 1: (96, 96)}[part]
            return wdn.at[l, pl.ds(pl.multiple_of(rank * 192 + low, 16), size), :]
        cols = {None: pl.ds(0, 3072), 0: pl.ds(0, 1536), 1: pl.ds(1536, 1536)}[part]
        return win.at[l, pl.ds(pl.multiple_of(rank * 48, 16), 48), cols]

    pieces = [(l, down) for l in range(LAYERS) for down in (False, True)]
    base = {piece: 8 + 11 * n for n, piece in enumerate(pieces)}

    def own_part(piece, part):
        l, down = piece
        if down:
            return wdn_s.at[l, pl.ds(96 * part, 96), :]
        return win_s.at[l, :, pl.ds(1536 * part, 1536)]

    def spread_first(piece):
        for part, device in ((0, place.yp), (1, place.ym)):
            wire.send(own_part(piece, part), window(*piece, r, part), base[piece] + part, device)

    def spread_last(piece):
        for part, device in ((1, place.yp), (0, place.ym)):
            wire.send(own_part(piece, part), window(*piece, r, part), base[piece] + 3 - part, device)
        l, down = piece
        mine = (wdn_s if down else win_s).at[l]
        here = window(l, down, r, None)
        wire.send(mine, here, base[piece] + 6, place.partner)
        here[...] = mine[...]

    loads[2].wait()
    spread_first(pieces[0])
    spread_last(pieces[0])
    for n in (3, 0, 1):
        loads[n].wait()

    def forward(piece):
        l, down = piece
        b = base[piece]
        left, right = owner(3), owner(1)
        half = window(l, down, left, 0)
        wire.wait(half, b + 0, place.ym)
        wire.send(half, half, b + 4, place.yp)
        half = window(l, down, right, 1)
        wire.wait(half, b + 1, place.yp)
        wire.send(half, half, b + 5, place.ym)

    def across(piece):
        l, down = piece
        b = base[piece]
        left, right, far = owner(3), owner(1), owner(2)
        wire.wait(window(l, down, left, 1), b + 2, place.ym)
        whole = window(l, down, left, None)
        wire.send(whole, whole, b + 7, place.partner)
        wire.wait(window(l, down, right, 0), b + 3, place.yp)
        whole = window(l, down, right, None)
        wire.send(whole, whole, b + 8, place.partner)
        for part, device in ((0, place.ym), (1, place.yp)):
            half = window(l, down, far, part)
            wire.wait(half, b + 4 + part, device)
            wire.send(half, half, b + 9 + part, place.partner)

    def settle(piece):
        l, down = piece
        b = base[piece]
        wire.wait(window(l, down, owner(0, True), None), b + 6, place.partner)
        wire.wait(window(l, down, owner(3, True), None), b + 7, place.partner)
        wire.wait(window(l, down, owner(1, True), None), b + 8, place.partner)
        for part in range(2):
            wire.wait(window(l, down, owner(2, True), part), b + 9 + part, place.partner)

    for i in range(1, 8):
        j = (r - i + 8) % 8
        wire.wait(B["pin"].at[j], i, place.group + j)
    patch_rows = B["pin"][:, :, 0:192].reshape(128, 192)
    tiled = jnp.concatenate([positions[...].astype(f32)] * IMG, axis=0)
    C["x"][0] = mm(patch_rows, embed[...]) + tiled
    block_forward(0, 128, C, win_c)
    cut = block_end(0, C, wdn_c).astype(bf16)
    arrived[x, z] = cut.reshape(IMG, TOK, D)
    first, second, third, fourth, fifth = plane_gather(wire, place, arrived, 52)
    first()
    for piece in pieces[1:]:
        spread_first(piece)
        spread_last(piece)
    selector, hot, table = route(arow[...], labels[...], shard, r)
    B["table"][...] = table
    to_scalar = pltpu.make_async_copy(B["table"], source, local_sem.at[4])
    to_scalar.start()
    forward(pieces[0])
    second()
    col = iota((1, 512), 1)
    at = col & 15
    lane = ((col >> 4) & 15) * 24 + (col >> 8) * 3
    wanted = lane + (at // 3) * 6 + at % 3
    B["order"][0] = ((iota((D, 512), 0) == wanted) & (at < 12)).astype(f32).astype(bf16)
    for q in range(3):
        entry = jnp.maximum(at - 12, 0) + 4 * q
        wanted = lane + (entry // 3) * 6 + entry % 3
        B["order"][1 + q] = ((iota((D, 512), 0) == wanted) & (at >= 12)).astype(f32).astype(bf16)
    B["pp"][...] = (iota((128, D), 1) - 256 == (iota((128, D), 0) & 15)).astype(f32).astype(bf16)
    B["pp"][:, 0:192] = B["pin"][:, :, 0:192].reshape(128, 192)
    packed[:, PACK - 48 :, :] = jnp.zeros((8, 48, D), bf16)
    forward(pieces[1])
    third()
    forward(pieces[2])
    fourth()
    forward(pieces[3])
    across(pieces[0])
    fifth()
    across(pieces[1])
    settle(pieces[0])

    S["x"][0] = slot_rows(selector, arrived[...].reshape(2048, D))
    block_forward(0, 256, S, win)
    settle(pieces[1])
    S["x"][1] = block_end(0, S, wdn)
    across(pieces[2])
    settle(pieces[2])
    block_forward(1, 256, S, win, lambda: across(pieces[3]))
    settle(pieces[3])
    S["x"][2] = block_end(1, S, wdn)
    to_scalar.wait()
    ours = iota((CLASSES, SHARDS, D), 1) == shard
    table = jnp.sum(jnp.where(ours, classes[...].astype(f32), 0.0), axis=1).astype(bf16)
    loss, gcls, dlast = head_loss(S["x"][LAYERS], table, hot)
    losses[...] = loss
    for k in range(8):
        packed[k, PACK - 48 :, 0:CLASSES] = gcls[48 * k : 48 * k + 48]
    S["dy"][...] = dlast

    def backward(i, carry):
        block_backward(LAYERS - 1 - i, 256, S, win, wdn, S["dy"])
        return carry

    lax.fori_loop(0, LAYERS, backward, 0)

    line_x, line_z = B["line_x"], B["line_z"]
    gcut = S["dy"][...].astype(bf16).reshape(CAP, TOK, D)
    line_x[x] = gcut[:8]
    line_z[z] = gcut[8:]
    lines = (
        Line(wire, x, place.xp, place.xm, 76, lambda at, h: line_x.at[at, pl.ds(4 * h, 4)]),
        Line(wire, z, place.zp, place.zm, 82, lambda at, h: line_z.at[at, pl.ds(4 * h, 4)]),
    )
    for line in lines:
        line.send()

    def server_weights(l):
        for b, u, dout in weight_pairs(S, l):
            val = mm(u[...], dout[...], 0, 0).astype(bf16)
            for k in range(8):
                packed[k, 576 * l + 48 * b : 576 * l + 48 * b + 48, :] = val[48 * k : 48 * k + 48]
        for n in range(4):
            val = mm(S["h"][l, :, D * n : D * n + D], S["dyb"][l], 0, 0).astype(bf16)
            for j in range(2):
                packed[2 * n + j, 576 * l + D : 576 * l + 576, :] = val[192 * j : 192 * j + 192]

    rows_a, rows_b = pl.ds(0, CUT_A), pl.ds(CUT_A, PACK - CUT_A)

    def row(k, core):
        return (y + k) % 4 * 2 + core

    def swap(part, k0):
        for k in (2, 1, 3, 0):
            wire.send(packed.at[row(k, 1 - c), part], B["swapped"].at[k, part], k0 + k, place.partner)

    def combine(k, part, k0, start, stop):
        wire.wait(B["swapped"].at[k, part], k0 + k, place.partner)

        def body(rows):
            total = packed[row(k, c), rows, :].astype(f32) + B["swapped"][k, rows, :].astype(f32)
            packed[row(k, c), rows, :] = total.astype(bf16)

        add_rows(start, stop, 48, body)

    def combine_a(k):
        combine(k, rows_a, 94, 0, CUT_A)

    def combine_b(k):
        combine(k, rows_b, 98, CUT_A, PACK)

    server_weights(1)
    swap(rows_b, 98)
    for line in lines:
        line.relay()
    combine_b(2)
    wire.send(packed.at[row(2, c), rows_b], B["from_p"], 102, place.ym)
    combine_b(1)
    wire.send(packed.at[row(1, c), rows_b], B["fin_p"].at[rows_b], 103, place.yp)
    for line in lines:
        line.rest()
    pick_x, pick_z = B["pick_x"], B["pick_z"]

    def ring_one(src, hop, end, h, up, down, k0, k):
        if k == 2:
            wire.send(src(2, 0), hop.at[0], k0, up)
            wire.send(src(2, 1), hop.at[1], k0 + 1, down)
        if k == 1:
            wire.send(src(1, 1), end.at[0, pl.ds(h, h)], k0 + 2, up)
        if k == 3:
            wire.send(src(3, 0), end.at[1, pl.ds(0, h)], k0 + 3, down)

    def ring_two(src, load, hop, end, h, up, down, k0):
        wire.wait(hop.at[0], k0, down)
        load(1, 0, hop)
        wire.send(src(1, 0), end.at[0, pl.ds(0, h)], k0 + 4, up)
        wire.wait(hop.at[1], k0 + 1, up)
        load(3, 1, hop)
        wire.send(src(3, 1), end.at[1, pl.ds(h, h)], k0 + 5, down)

    def ring_three(end, h, up, down, k0):
        wire.wait(end.at[0, pl.ds(h, h)], k0 + 2, down)
        wire.wait(end.at[1, pl.ds(0, h)], k0 + 3, up)
        wire.wait(end.at[0, pl.ds(0, h)], k0 + 4, down)
        wire.wait(end.at[1, pl.ds(h, h)], k0 + 5, up)

    def part_of(pick):
        return lambda k, part: pick.at[k, pl.ds(4 * part, 4)]

    def load_of(pick):
        def load(k, part, hop):
            for i in range(4):
                at = 4 * part + i
                pick[k, at] = (pick[k, at].astype(f32) + hop[part, i].astype(f32)).astype(bf16)

        return load

    for k in (2, 1, 3, 0):
        zd, xd = (z + k) % 4, (x + k) % 4
        for m in range(8):
            at = source[0, (x * 4 + zd) * 8 + m]
            here = ((at >> 4) & 3 == z) & ((at & 15) < 8)
            pick_x[k, m] = jnp.where(here, line_x[(at >> 6) & 3, at & 7].astype(f32), 0.0).astype(bf16)
        ring_one(part_of(pick_x), B["ret_x"], B["got_x"], 4, place.zp, place.zm, 88, k)
        for m in range(8):
            at = source[0, (xd * 4 + z) * 8 + m]
            here = ((at >> 6) & 3 == x) & ((at & 15) >= 8)
            pick_z[k, m] = jnp.where(here, line_z[(at >> 4) & 3, at & 7].astype(f32), 0.0).astype(bf16)
        ring_one(part_of(pick_z), B["ret_z"], B["got_z"], 4, place.xp, place.xm, 109, k)
    server_weights(0)
    swap(rows_a, 94)
    ring_two(part_of(pick_x), load_of(pick_x), B["ret_x"], B["got_x"], 4, place.zp, place.zm, 88)
    ring_two(part_of(pick_z), load_of(pick_z), B["ret_z"], B["got_z"], 4, place.xp, place.xm, 109)
    combine_a(2)
    wire.send(packed.at[row(2, c), rows_a], B["from_m"], 104, place.yp)
    combine_a(3)
    wire.send(packed.at[row(3, c), rows_a], B["fin_m"].at[rows_a], 105, place.ym)
    combine_a(1)
    combine_b(3)
    ring_three(B["got_x"], 4, place.zp, place.zm, 88)
    ring_three(B["got_z"], 4, place.xp, place.xm, 109)
    for m in range(8):
        piece = pick_x[0, m].astype(f32) + pick_z[0, m].astype(f32)
        for k in range(2):
            piece = piece + B["got_x"][k, m].astype(f32) + B["got_z"][k, m].astype(f32)
        C["dy"][16 * m : 16 * m + 16] = piece
    cpack, cswap, cmine = B["cpack"], B["cswap"], B["cmine"]
    pairs = weight_pairs(C, 0)

    def emit(b, u, dout):
        val = mm(dout[...], u[...], 0, 0).astype(bf16)
        for i in range(2):
            for k in range(4):
                for core in range(2):
                    low = 192 * i + 48 * k + 24 * core
                    cpack[2 * b + i, core, 24 * k : 24 * k + 24] = val[low : low + 24]
        pair = pl.ds(2 * b, 2)
        wire.send(cpack.at[pair, 1 - c, pl.ds(0, MAIN)], cswap.at[pair, pl.ds(0, MAIN)], 116 + b, place.partner)

    def early():
        for pair in pairs[4:]:
            emit(*pair)
        B["dperm"][0] = mm(C["dyb"][0], B["order"][0]).astype(bf16)

    block_backward(0, 128, C, win_c, wdn_c, C["dy"], early)
    for pair in pairs[:4]:
        emit(*pair)
    last = C["dy"][...].astype(bf16)
    for q in range(4):
        val = mm(B["dperm"][0], C["h"][0, :, D * q : D * q + D], 0, 0)
        if q < 3:
            B["dperm"][1] = mm(last, B["order"][1 + q]).astype(bf16)
            val = val + mm(B["dperm"][1], B["pp"][...], 0, 0)
        val = val.astype(bf16)
        for core in range(2):
            for i in range(16):
                low = 256 * core + 16 * i
                cpack[i, core, MAIN + 16 * q : MAIN + 16 * q + 16] = val[low : low + 16]
    wire.send(cpack.at[:, 1 - c, pl.ds(MAIN, TAIL)], cswap.at[:, pl.ds(MAIN, TAIL)], 124, place.partner)

    X, Z = pl.ds(0, PART), pl.ds(PART, PART)

    def fold(low, high):
        for i in range(16):
            total = cpack[i, c, low:high].astype(f32) + cswap[i, low:high].astype(f32)
            cmine[i // 4, i % 4, low:high] = total.astype(bf16)

    def src_x(k, part):
        return cmine.at[(x + k) % 4, pl.ds(2 * part, 2), X]

    def src_z(k, part):
        return cmine.at[pl.ds(2 * part, 2), (z + k) % 4, Z]

    def load_x(k, part, hop):
        to = (x + k) % 4
        for i in range(2):
            at = 2 * part + i
            cmine[to, at, :PART] = (cmine[to, at, :PART].astype(f32) + hop[part, i].astype(f32)).astype(bf16)

    def load_z(k, part, hop):
        to = (z + k) % 4
        for i in range(2):
            at = 2 * part + i
            cmine[at, to, PART:] = (cmine[at, to, PART:].astype(f32) + hop[part, i].astype(f32)).astype(bf16)

    for b in (4, 5, 6, 7, 0, 1, 2, 3):
        wire.wait(cswap.at[pl.ds(2 * b, 2), pl.ds(0, MAIN)], 116 + b, place.partner)
    fold(0, PART)
    for k in (2, 1, 3):
        ring_one(src_x, B["hop_x"], B["end_x"], 2, place.xp, place.xm, 125, k)
    wire.wait(cswap.at[:, pl.ds(MAIN, TAIL)], 124, place.partner)
    fold(PART, BLOCK)
    for k in (2, 1, 3):
        ring_one(src_z, B["hop_z"], B["end_z"], 2, place.zp, place.zm, 131, k)

    wire.wait(B["from_m"], 104, place.ym)

    def add_a(rows):
        packed[row(1, c), rows, :] = (packed[row(1, c), rows, :].astype(f32) + B["from_m"][rows, :].astype(f32)).astype(bf16)

    add_rows(0, CUT_A, 48, add_a)
    wire.send(packed.at[row(1, c), rows_a], B["fin_p"].at[rows_a], 106, place.yp)
    wire.wait(B["from_p"], 102, place.yp)

    def add_b(i, carry):
        here = pl.ds(pl.multiple_of(i * 48, 16), 48)
        rows = pl.ds(pl.multiple_of(CUT_A + i * 48, 16), 48)
        packed[row(3, c), rows, :] = (packed[row(3, c), rows, :].astype(f32) + B["from_p"][here, :].astype(f32)).astype(bf16)
        return carry

    lax.fori_loop(0, (PACK - CUT_A) // 48, add_b, 0)
    wire.send(packed.at[row(3, c), rows_b], B["fin_m"].at[rows_b], 107, place.ym)

    ring_two(src_x, load_x, B["hop_x"], B["end_x"], 2, place.xp, place.xm, 125)
    ring_two(src_z, load_z, B["hop_z"], B["end_z"], 2, place.zp, place.zm, 131)
    half_x, half_z = B["half_x"], B["half_z"]
    ring_three(B["end_x"], 2, place.xp, place.xm, 125)
    for i in range(4):
        total = cmine[x, i, :PART].astype(f32) + B["end_x"][0, i].astype(f32) + B["end_x"][1, i].astype(f32)
        half_x[i] = total.astype(bf16)
    for k in (2, 1, 3):
        wire.send(half_x.at[(z + k) % 4], B["two_x"].at[k - 1], 136 + k, place.at(0, k, 0))
    ring_three(B["end_z"], 2, place.zp, place.zm, 131)
    for i in range(4):
        total = cmine[i, z, PART:].astype(f32) + B["end_z"][0, i].astype(f32) + B["end_z"][1, i].astype(f32)
        half_z[i] = total.astype(bf16)
    for k in (2, 1, 3):
        wire.send(half_z.at[(x + k) % 4], B["two_z"].at[k - 1], 139 + k, place.at(k, 0, 0))
    combine_a(0)
    combine_b(0)
    for k in range(1, 4):
        wire.wait(B["two_x"].at[k - 1], 136 + k, place.at(0, 4 - k, 0))
    upper = half_x[z].astype(f32)
    for k in range(3):
        upper = upper + B["two_x"][k].astype(f32)
    for k in range(1, 4):
        wire.wait(B["two_z"].at[k - 1], 139 + k, place.at(4 - k, 0, 0))
    lower = half_z[x].astype(f32)
    for k in range(3):
        lower = lower + B["two_z"][k].astype(f32)
    line, column = iota((64, TAIL), 0), iota((64, TAIL), 1)
    inside, owner_y = line & 15, line >> 4
    entry = owner_y * 3 + inside % 3
    spot = jnp.where(inside < 12, (inside // 3) * 16 + entry, (entry // 4) * 16 + 12 + entry % 4)
    pick = (column == spot) & (inside < 15)
    ordered = mm(pick.astype(f32).astype(bf16), lower[16:].astype(bf16)).astype(bf16)
    main = jnp.concatenate([upper, lower[:16]], axis=0).astype(bf16)
    for k in range(4):
        B["low_x"][k] = main[24 * k : 24 * k + 24]
        B["low_z"][k] = ordered[16 * k : 16 * k + 16]
    for k in (2, 1, 3):
        to = (y + k) % 4
        wire.send(B["low_x"].at[to], B["three_x"].at[k - 1], 142 + k, place.at(0, 0, k))
        wire.send(B["low_z"].at[to], B["three_z"].at[k - 1], 145 + k, place.at(0, 0, k))

    wire.wait(B["fin_p"].at[rows_b], 103, place.ym)
    wire.wait(B["fin_m"].at[rows_a], 105, place.yp)
    wire.wait(B["fin_p"].at[rows_a], 106, place.ym)
    wire.wait(B["fin_m"].at[rows_b], 107, place.yp)

    def total_of(first_row, rows):
        at = pl.ds(first_row, rows)
        return packed[row(0, c), at, :].astype(f32) + B["fin_p"][at, :].astype(f32) + B["fin_m"][at, :].astype(f32)

    for l in range(LAYERS):
        for b in range(8):
            B["gin"][l, :, D * b : D * b + D] = total_of(576 * l + 48 * b, 48)
        for b in range(4):
            B["gdn"][l, 48 * b : 48 * b + 48, :] = total_of(576 * l + D + 48 * b, 48)
    leaving = [
        pltpu.make_async_copy(B["gin"], gin, local_sem.at[5]),
        pltpu.make_async_copy(B["gdn"], gdn, local_sem.at[6]),
    ]
    for copy in leaving:
        copy.start()
    gcls_out[...] = total_of(PACK - 48, 48)[:, 0:128].T[0:CLASSES]

    for k in range(1, 4):
        wire.wait(B["three_x"].at[k - 1], 142 + k, place.at(0, 0, 4 - k))
        wire.wait(B["three_z"].at[k - 1], 145 + k, place.at(0, 0, 4 - k))
    main = B["low_x"][y].astype(f32)
    tail = B["low_z"][y].astype(f32)
    for k in range(3):
        main = main + B["three_x"][k].astype(f32)
        tail = tail + B["three_z"][k].astype(f32)
    out_in[...] = main
    for q in range(4):
        out_dn[:, D * q : D * q + D] = tail[3 * q : 3 * q + 3]
    out_pe[...] = tail[12:15, 0:192]
    out_pos[...] = tail[12:15, 256:272]
    for copy in leaving:
        copy.wait()
    wire.finish()


def finish_kernel(*refs):
    count = len(refs) // 3
    given, results, held = refs[:count], refs[count : 2 * count], refs[2 * count : 3 * count]
    sem = refs[-1]
    inward = [pltpu.make_async_copy(given[n], held[n], sem.at[0, n]) for n in range(count)]
    outward = [pltpu.make_async_copy(held[n], results[n], sem.at[1, n]) for n in range(count)]
    for copy in inward:
        copy.start()
    for copy, onward in zip(inward, outward):
        copy.wait()
        onward.start()
    for copy in outward:
        copy.wait()


def per_device(patches, labels, assign, patch_embed, positions, client_in, client_down, server_in, server_down, classifier):
    shapes = [
        ((1, CAP), f32),
        ((LAYERS, 48, 4 * D + FF), f32),
        ((LAYERS, 192, D), f32),
        ((CLASSES, 48), f32),
        ((24, D), f32),
        ((3, FF), f32),
        ((3, 192), f32),
        ((3, TOK), f32),
    ]
    scratch = list(CLIENT.values()) + list(SERVER.values()) + list(BUFFERS.values())
    results = pl.pallas_call(
        step_kernel,
        out_shape=[jax.ShapeDtypeStruct(*s) for s in shapes],
        in_specs=[VMEM] * 6 + [ANY] * 4,
        out_specs=[VMEM, HBM, HBM] + [VMEM] * 5,
        scratch_shapes=[pltpu.VMEM(*s) for s in scratch]
        + [
            pltpu.SemaphoreType.DMA((N_SEM,)),
            pltpu.SemaphoreType.DMA((N_SEM,)),
            pltpu.SemaphoreType.DMA((7,)),
            pltpu.SMEM((1, 128), jnp.int32),
        ],
        compiler_params=pltpu.CompilerParams(collective_id=0, has_side_effects=True, vmem_limit_bytes=67043328),
        name="step",
    )(
        patches.T,
        patch_embed,
        positions,
        assign.reshape(1, 128),
        labels.reshape(8, 128),
        classifier.transpose(2, 0, 1),
        client_in[None],
        client_down[None],
        server_in,
        server_down,
    )
    losses, gin, gdn, gcls, out_in, out_dn, out_pe, out_pos = pl.pallas_call(
        finish_kernel,
        out_shape=[jax.ShapeDtypeStruct(*s) for s in shapes],
        in_specs=[HBM] * len(shapes),
        out_specs=[HBM] * len(shapes),
        scratch_shapes=[pltpu.VMEM(*s) for s in shapes] + [pltpu.SemaphoreType.DMA((2, len(shapes)))],
        compiler_params=pltpu.CompilerParams(vmem_limit_bytes=67043328),
        name="finish",
    )(*results)
    return losses, out_pe.T, out_pos.T, out_in.T, out_dn.T, gin, gdn, gcls.T


def solution(mesh):
    in_specs = (
        P("client", None),
        P(),
        P(),
        P(),
        P(),
        P(),
        P(),
        P(None, "client", None),
        P(None, "client", None),
        P(),
    )
    out_specs = (
        P("client", None),
        P(None, "client"),
        P(None, "client"),
        P(None, "client"),
        P(None, "client"),
        P(None, "client", None),
        P(None, "client", None),
        P("client", None),
    )
    return jax.shard_map(per_device, mesh=mesh, in_specs=in_specs, out_specs=out_specs, check_vma=False)
```

```python
import math

import jax
import jax.numpy as jnp
from jax import lax
from jax.experimental import pallas as pl
from jax.experimental.pallas import tpu as pltpu
from jax.sharding import PartitionSpec as P

D = 384
FF = 1536
TOK = 16
IMG = 8
CLASSES = 10
SHARDS = 16
LAYERS = 2
CAP = 16
EPSILON = 1e-06
SCALE = 0.125
GELU_A = math.sqrt(2.0 / math.pi)
GELU_B = 0.044715
PACK = LAYERS * (D + FF // 8) + D // 8
CUT_A = 576
MAIN = 96
TAIL = 64
PART = 80
BLOCK = MAIN + TAIL

bf16 = jnp.bfloat16
f32 = jnp.float32
MESH = pl.DeviceIdType.MESH
VMEM = pl.BlockSpec(memory_space=pltpu.VMEM)
SMEM = pl.BlockSpec(memory_space=pltpu.SMEM)
ANY = pl.BlockSpec(memory_space=pl.ANY)
HBM = pl.BlockSpec(memory_space=pltpu.HBM)


def mm(a, b, ca=1, cb=0):
    return lax.dot_general(a, b, (((ca,), (cb,)), ((), ())), preferred_element_type=f32)


def iota(shape, dim):
    return lax.broadcasted_iota(jnp.int32, shape, dim)


def norm(v):
    centre = v - jnp.mean(v, axis=-1, keepdims=True)
    rstd = lax.rsqrt(jnp.mean(centre * centre, axis=-1, keepdims=True) + EPSILON)
    return centre * rstd, rstd


def norm_back(v, grad):
    hat, rstd = norm(v)
    along = jnp.mean(grad * hat, axis=-1, keepdims=True)
    return rstd * (grad - jnp.mean(grad, axis=-1, keepdims=True) - hat * along)


def rounded(v):
    return v.astype(bf16).astype(f32)


def head_masks(rows):
    low = (iota((rows, 128), 1) < 64).astype(f32)
    return low.astype(bf16), (1.0 - low).astype(bf16)


def two_heads(v):
    low, high = head_masks(v.shape[0])
    return jnp.concatenate([v * low, v * high], axis=0)


def merge_heads(v):
    rows = v.shape[0] // 2
    return jnp.where(iota((rows, 128), 1) < 64, v[:rows], v[rows:])


def block_forward(l, rows, S, win, middle=None):
    x = S["x"][l]
    hat, _ = norm(x)
    u1 = hat.astype(bf16)
    S["u1"][l] = u1
    for n in range(3):
        cols = slice(D * n, D * n + D)
        S["qkv"][l, :, cols] = mm(u1, win[l, :, cols]).astype(bf16)
    same = ((iota((256, 128), 0) & 127) >> 4) == (iota((256, 128), 1) >> 4)
    for g in range(rows // 128):
        part = slice(128 * g, 128 * g + 128)
        for p in range(3):
            q2 = S["qkv"][l, part, 128 * p : 128 * p + 128]
            k2 = S["qkv"][l, part, D + 128 * p : D + 128 * p + 128]
            v2 = S["qkv"][l, part, 2 * D + 128 * p : 2 * D + 128 * p + 128]
            scores = mm(two_heads(q2), k2, 1, 1) * SCALE
            scores = jnp.where(same, scores, -1e30)
            grown = jnp.exp(scores - jnp.max(scores, axis=-1, keepdims=True))
            prob = grown / jnp.sum(grown, axis=-1, keepdims=True)
            S["prob"][l, 3 * g + p] = prob
            S["att"][l, part, 128 * p : 128 * p + 128] = merge_heads(mm(prob.astype(bf16), v2)).astype(bf16)
    x1 = S["x"][l] + mm(S["att"][l], win[l, :, 3 * D : 4 * D])
    S["x1"][l] = x1
    hat, _ = norm(x1)
    u2 = hat.astype(bf16)
    S["u2"][l] = u2
    if middle is not None:
        middle()
    for n in range(4):
        pre = mm(u2, win[l, :, 4 * D + D * n : 5 * D + D * n])
        square = pre * pre
        bent = jnp.tanh(pre * (GELU_A + GELU_A * GELU_B * square))
        gate = 0.5 + 0.5 * bent
        value = pre * gate
        S["h"][l, :, D * n : D * n + D] = value.astype(bf16)
        bend = value * (1.0 - bent)
        S["slope"][l, :, D * n : D * n + D] = gate + bend * (GELU_A + 3.0 * GELU_A * GELU_B * square)


def block_end(l, S, wdn):
    return S["x1"][l] + mm(S["h"][l], wdn[l])


def block_backward(l, rows, S, win, wdn, dy_ref, early=None):
    dyb = dy_ref[...].astype(bf16)
    S["dyb"][l] = dyb
    for n in range(4):
        cols = slice(D * n, D * n + D)
        dh = rounded(mm(dyb, wdn[l, cols, :], 1, 1))
        S["dpre"][l, :, cols] = (dh * S["slope"][l, :, cols]).astype(bf16)
    if early is not None:
        early()
    du2 = rounded(mm(S["dpre"][l], win[l, :, 4 * D :], 1, 1))
    dx1 = dy_ref[...] + norm_back(S["x1"][l], du2)
    dy_ref[...] = dx1
    dx1b = dx1.astype(bf16)
    S["dx1b"][l] = dx1b
    S["datt"][...] = mm(dx1b, win[l, :, 3 * D : 4 * D], 1, 1).astype(bf16)
    for g in range(rows // 128):
        part = slice(128 * g, 128 * g + 128)
        for p in range(3):
            cq = slice(128 * p, 128 * p + 128)
            ck = slice(D + 128 * p, D + 128 * p + 128)
            cv = slice(2 * D + 128 * p, 2 * D + 128 * p + 128)
            qs = two_heads(S["qkv"][l, part, cq])
            dos = two_heads(S["datt"][part, cq])
            prob = S["prob"][l, 3 * g + p]
            dprob = mm(dos, S["qkv"][l, part, cv], 1, 1)
            dscore = prob * (dprob - jnp.sum(prob * dprob, axis=-1, keepdims=True)) * SCALE
            dsb = dscore.astype(bf16)
            S["dqkv"][l, part, cq] = merge_heads(mm(dsb, S["qkv"][l, part, ck])).astype(bf16)
            S["dqkv"][l, part, ck] = mm(dsb, qs, 0, 0).astype(bf16)
            S["dqkv"][l, part, cv] = mm(prob.astype(bf16), dos, 0, 0).astype(bf16)
    du1 = rounded(mm(S["dqkv"][l], win[l, :, : 3 * D], 1, 1))
    dy_ref[...] = dy_ref[...] + norm_back(S["x"][l], du1)


def weight_pairs(S, l):
    pairs = []
    for n in range(3):
        pairs.append((n, S["u1"].at[l], S["dqkv"].at[l, :, pl.ds(D * n, D)]))
    pairs.append((3, S["att"].at[l], S["dx1b"].at[l]))
    for n in range(4):
        pairs.append((4 + n, S["u2"].at[l], S["dpre"].at[l, :, pl.ds(D * n, D)]))
    return pairs


def block_shapes(layers, rows):
    return dict(
        x=((layers + 1, rows, D), f32),
        x1=((layers, rows, D), f32),
        u1=((layers, rows, D), bf16),
        u2=((layers, rows, D), bf16),
        qkv=((layers, rows, 3 * D), bf16),
        prob=((layers, 3 * rows // 128, 256, 128), f32),
        att=((layers, rows, D), bf16),
        slope=((layers, rows, FF), f32),
        h=((layers, rows, FF), bf16),
        dyb=((layers, rows, D), bf16),
        dpre=((layers, rows, FF), bf16),
        dx1b=((layers, rows, D), bf16),
        datt=((rows, D), bf16),
        dqkv=((layers, rows, 3 * D), bf16),
        dy=((rows, D), f32),
    )


class Place:
    def __init__(self):
        me = lax.axis_index("client")
        self.me = me
        self.c, self.y, self.z, self.x = me % 2, me // 2 % 4, me // 8 % 4, me // 32
        self.r, self.group = me % 8, me // 8 * 8
        self.partner = me + 1 - 2 * self.c
        self.yp, self.ym = self.at(0, 0, 1), self.at(0, 0, 3)
        self.xp, self.xm = self.at(1, 0, 0), self.at(3, 0, 0)
        self.zp, self.zm = self.at(0, 1, 0), self.at(0, 3, 0)

    def at(self, dx, dz, dy):
        x, z, y = (self.x + dx) % 4, (self.z + dz) % 4, (self.y + dy) % 4
        return ((x * 4 + z) * 4 + y) * 2 + self.c

    def greet(self, group, plane):
        peers = []
        if group:
            peers += [self.group + (self.r + i) % 8 for i in range(1, 8)]
        if plane:
            peers += [self.xp, self.xm, self.zp, self.zm]
        barrier = pltpu.get_barrier_semaphore()
        for peer in peers:
            pl.semaphore_signal(barrier, inc=1, device_id=(peer,), device_id_type=MESH)
        pl.semaphore_wait(barrier, len(peers))


class Wire:
    def __init__(self, send_sem, recv_sem):
        self.send_sem, self.recv_sem, self.sent = send_sem, recv_sem, []

    def make(self, src, dst, k, device):
        return pltpu.make_async_remote_copy(
            src_ref=src,
            dst_ref=dst,
            send_sem=self.send_sem.at[k],
            recv_sem=self.recv_sem.at[k],
            device_id=(device,),
            device_id_type=MESH,
        )

    def send(self, src, dst, k, device):
        copy = self.make(src, dst, k, device)
        copy.start()
        self.sent.append(copy)

    def wait(self, landed, k, device):
        self.make(landed, landed, k, device).wait_recv()

    def finish(self):
        for copy in self.sent:
            copy.wait_send()


class Line:
    def __init__(self, wire, me, up, down, k, view):
        self.wire, self.me, self.up, self.down, self.k, self.view = wire, me, up, down, k, view

    def both(self, ref, k, device):
        self.wire.send(ref, ref, self.k + k, device)

    def send(self):
        self.both(self.view(self.me, 0), 0, self.up)
        self.both(self.view(self.me, 1), 1, self.down)
        self.both(self.view(self.me, 1), 2, self.up)
        self.both(self.view(self.me, 0), 3, self.down)

    def relay(self):
        left, right = (self.me + 3) % 4, (self.me + 1) % 4
        self.wire.wait(self.view(left, 0), self.k, self.down)
        self.both(self.view(left, 0), 4, self.up)
        self.wire.wait(self.view(right, 1), self.k + 1, self.up)
        self.both(self.view(right, 1), 5, self.down)

    def rest(self):
        left, right, far = (self.me + 3) % 4, (self.me + 1) % 4, (self.me + 2) % 4
        self.wire.wait(self.view(left, 1), self.k + 2, self.down)
        self.wire.wait(self.view(right, 0), self.k + 3, self.up)
        self.wire.wait(self.view(far, 0), self.k + 4, self.down)
        self.wire.wait(self.view(far, 1), self.k + 5, self.up)


def plane_gather(wire, place, buf, k0):
    x, z = place.x, place.z
    lines = (
        Line(wire, x, place.xp, place.xm, k0, lambda at, h: buf.at[at, z, pl.ds(2 * h, 2)]),
        Line(wire, z, place.zp, place.zm, k0 + 6, lambda at, h: buf.at[x, at, pl.ds(4 + 2 * h, 2)]),
        Line(wire, z, place.zp, place.zm, k0 + 12, lambda at, h: buf.at[pl.ds(2 * h, 2), at, pl.ds(0, 4)]),
        Line(wire, x, place.xp, place.xm, k0 + 18, lambda at, h: buf.at[at, pl.ds(2 * h, 2), pl.ds(4, 4)]),
    )

    def first():
        lines[0].send()
        lines[1].send()

    def second():
        lines[0].relay()
        lines[1].relay()

    def third():
        lines[0].rest()
        lines[2].send()
        lines[1].rest()
        lines[3].send()

    def fourth():
        lines[2].relay()
        lines[3].relay()

    def fifth():
        lines[2].rest()
        lines[3].rest()

    return first, second, third, fourth, fifth


def add_rows(start, stop, step, body):
    def run(i, carry):
        body(pl.ds(pl.multiple_of(start + i * step, 16), step))
        return carry

    lax.fori_loop(0, (stop - start) // step, run, 0)


def route(arow, labels, shard, rank_in):
    eye = iota((128, 128), 0) == iota((128, 128), 1)
    acol = jnp.sum(jnp.where(eye, arow.astype(f32), 0.0), axis=1, keepdims=True).astype(jnp.int32)
    earlier = (acol == arow) & (iota((128, 128), 0) < iota((128, 128), 1))
    rank = jnp.sum(earlier.astype(f32), axis=0, keepdims=True).astype(jnp.int32)
    chosen = (jnp.broadcast_to(arow, (CAP, 128)) == shard) & (
        jnp.broadcast_to(rank, (CAP, 128)) == iota((CAP, 128), 0)
    )
    selector = chosen.astype(f32).astype(bf16)
    take = (iota((128, 16), 0) == iota((128, 16), 1) * IMG + rank_in).astype(f32).astype(bf16)
    by_row = mm(labels.astype(f32).astype(bf16), take).astype(bf16)
    lift = ((iota((128, 8), 0) >> 4) == iota((128, 8), 1)).astype(f32).astype(bf16)
    tall = mm(lift, by_row)
    mine = (iota((128, 16), 0) & 15) == iota((128, 16), 1)
    label = jnp.sum(jnp.where(mine, tall, 0.0), axis=1, keepdims=True)
    onehot = (label == iota((128, CLASSES), 1).astype(f32)).astype(f32).astype(bf16)
    return selector, mm(selector, onehot), arow * CAP + rank


def slot_rows(selector, arrived):
    spread = (iota((128, 2048), 0) == (iota((128, 2048), 1) >> 4)).astype(f32).astype(bf16)
    wide = mm(selector, spread).astype(bf16)
    repeat = ((iota((256, CAP), 0) >> 4) == iota((256, CAP), 1)).astype(f32).astype(bf16)
    tall = mm(repeat, wide)
    same = (iota((256, 2048), 0) & 15) == (iota((256, 2048), 1) & 15)
    return mm(jnp.where(same, tall, 0.0).astype(bf16), arrived)


def head_loss(last, classes, hot):
    filled = jnp.sum(hot, axis=1, keepdims=True)
    mean = jnp.mean(last.reshape(CAP, TOK, D), axis=1)
    hat, _ = norm(mean)
    pooled = hat.astype(bf16)
    logits = mm(pooled, classes, 1, 1)
    top = jnp.max(logits, axis=1, keepdims=True)
    grown = jnp.exp(logits - top)
    total = jnp.sum(grown, axis=1, keepdims=True)
    per = (jnp.log(total) + top - jnp.sum(hot * logits, axis=1, keepdims=True)) * filled
    eye = iota((CAP, CAP), 0) == iota((CAP, CAP), 1)
    losses = jnp.sum(jnp.where(eye, per, 0.0), axis=0, keepdims=True)
    dlogits = ((grown / total) * filled - hot).astype(bf16)
    gcls = mm(pooled, dlogits, 0, 0).astype(bf16)
    dpooled = rounded(mm(dlogits, classes))
    dmean = norm_back(mean, dpooled) * (1.0 / TOK)
    dlast = jnp.broadcast_to(dmean[:, None, :], (CAP, TOK, D)).reshape(CAP * TOK, D)
    return losses, gcls, dlast


CLIENT = block_shapes(1, 128)
SERVER = block_shapes(LAYERS, 256)
BUFFERS = dict(
    arrived=((4, 4, IMG, TOK, D), bf16),
    win=((LAYERS, D, 4 * D + FF), bf16),
    wdn=((LAYERS, FF, D), bf16),
    win_c=((1, D, 4 * D + FF), bf16),
    wdn_c=((1, FF, D), bf16),
    win_s=((LAYERS, 48, 4 * D + FF), bf16),
    wdn_s=((LAYERS, 192, D), bf16),
    table=((1, 128), jnp.int32),
    pout=((IMG, TOK, 256), bf16),
    pin=((IMG, TOK, 256), bf16),
    packed=((8, PACK, D), bf16),
    swapped=((4, PACK, D), bf16),
    from_m=((CUT_A, D), bf16),
    from_p=((PACK - CUT_A, D), bf16),
    fin_p=((PACK, D), bf16),
    fin_m=((PACK, D), bf16),
    line_x=((4, 8, TOK, D), bf16),
    line_z=((4, 8, TOK, D), bf16),
    pick_x=((4, 8, TOK, D), bf16),
    pick_z=((4, 8, TOK, D), bf16),
    ret_x=((2, 4, TOK, D), bf16),
    ret_z=((2, 4, TOK, D), bf16),
    got_x=((2, 8, TOK, D), bf16),
    got_z=((2, 8, TOK, D), bf16),
    order=((4, D, 512), bf16),
    dperm=((2, 128, 512), bf16),
    pp=((128, D), bf16),
    cpack=((16, 2, BLOCK, D), bf16),
    cswap=((16, BLOCK, D), bf16),
    cmine=((4, 4, BLOCK, D), bf16),
    hop_x=((2, 2, PART, D), bf16),
    hop_z=((2, 2, PART, D), bf16),
    end_x=((2, 4, PART, D), bf16),
    end_z=((2, 4, PART, D), bf16),
    half_x=((4, PART, D), bf16),
    half_z=((4, PART, D), bf16),
    two_x=((3, PART, D), bf16),
    two_z=((3, PART, D), bf16),
    low_x=((4, 24, D), bf16),
    low_z=((4, 16, D), bf16),
    three_x=((3, 24, D), bf16),
    three_z=((3, 16, D), bf16),
    gin=((LAYERS, 48, 4 * D + FF), f32),
    gdn=((LAYERS, 192, D), f32),
)
N_SEM = 160


def step_kernel(patches_t, embed, positions, arow, labels, classes, *refs):
    sources, refs = refs[:4], refs[4:]
    losses, gin, gdn, gcls_out, out_in, out_dn, out_pe, out_pos = refs[:8]
    refs = list(refs[8:])
    C = dict(zip(CLIENT, refs[: len(CLIENT)]))
    refs = refs[len(CLIENT) :]
    S = dict(zip(SERVER, refs[: len(SERVER)]))
    refs = refs[len(SERVER) :]
    B = dict(zip(BUFFERS, refs[: len(BUFFERS)]))
    send_sem, recv_sem, local_sem, source = refs[len(BUFFERS) :]
    win_c, wdn_c, win_s, wdn_s = B["win_c"], B["wdn_c"], B["win_s"], B["wdn_s"]
    loads = []
    for n, (src, dst) in enumerate(zip(sources, (win_c, wdn_c, win_s, wdn_s))):
        loads.append(pltpu.make_async_copy(src, dst, local_sem.at[n]))
    for n in (2, 3, 0, 1):
        loads[n].start()
    place = Place()
    x, z, y, c, r = place.x, place.z, place.y, place.c, place.r
    shard = place.me // 8
    win, wdn, arrived, packed = B["win"], B["wdn"], B["arrived"], B["packed"]
    B["pout"][...] = jnp.zeros_like(B["pout"])
    B["pout"][:, :, 0:192] = patches_t[...].T.reshape(IMG, TOK, 192)
    place.greet(True, True)
    wire = Wire(send_sem, recv_sem)

    for i in range(1, 8):
        j = (r + i) % 8
        wire.send(B["pout"].at[j], B["pin"].at[r], i, place.group + j)
    B["pin"][r] = B["pout"][r]

    def owner(dy, other=False):
        return (y + dy) % 4 * 2 + (1 - c if other else c)

    def window(l, down, rank, part):
        if down:
            low, size = {None: (0, 192), 0: (0, 96), 1: (96, 96)}[part]
            return wdn.at[l, pl.ds(pl.multiple_of(rank * 192 + low, 16), size), :]
        cols = {None: pl.ds(0, 3072), 0: pl.ds(0, 1536), 1: pl.ds(1536, 1536)}[part]
        return win.at[l, pl.ds(pl.multiple_of(rank * 48, 16), 48), cols]

    pieces = [(l, down) for l in range(LAYERS) for down in (False, True)]
    base = {piece: 8 + 11 * n for n, piece in enumerate(pieces)}

    def own_part(piece, part):
        l, down = piece
        if down:
            return wdn_s.at[l, pl.ds(96 * part, 96), :]
        return win_s.at[l, :, pl.ds(1536 * part, 1536)]

    def spread_first(piece):
        for part, device in ((0, place.yp), (1, place.ym)):
            wire.send(own_part(piece, part), window(*piece, r, part), base[piece] + part, device)

    def spread_last(piece):
        for part, device in ((1, place.yp), (0, place.ym)):
            wire.send(own_part(piece, part), window(*piece, r, part), base[piece] + 3 - part, device)
        l, down = piece
        mine = (wdn_s if down else win_s).at[l]
        here = window(l, down, r, None)
        wire.send(mine, here, base[piece] + 6, place.partner)
        here[...] = mine[...]

    loads[2].wait()
    spread_first(pieces[0])
    spread_last(pieces[0])
    loads[3].wait()
    spread_first(pieces[1])
    spread_last(pieces[1])
    for n in (0, 1):
        loads[n].wait()

    def forward(piece):
        l, down = piece
        b = base[piece]
        left, right = owner(3), owner(1)
        half = window(l, down, left, 0)
        wire.wait(half, b + 0, place.ym)
        wire.send(half, half, b + 4, place.yp)
        half = window(l, down, right, 1)
        wire.wait(half, b + 1, place.yp)
        wire.send(half, half, b + 5, place.ym)

    def across(piece):
        l, down = piece
        b = base[piece]
        left, right, far = owner(3), owner(1), owner(2)
        wire.wait(window(l, down, left, 1), b + 2, place.ym)
        whole = window(l, down, left, None)
        wire.send(whole, whole, b + 7, place.partner)
        wire.wait(window(l, down, right, 0), b + 3, place.yp)
        whole = window(l, down, right, None)
        wire.send(whole, whole, b + 8, place.partner)
        for part, device in ((0, place.ym), (1, place.yp)):
            half = window(l, down, far, part)
            wire.wait(half, b + 4 + part, device)
            wire.send(half, half, b + 9 + part, place.partner)

    def settle(piece):
        l, down = piece
        b = base[piece]
        wire.wait(window(l, down, owner(0, True), None), b + 6, place.partner)
        wire.wait(window(l, down, owner(3, True), None), b + 7, place.partner)
        wire.wait(window(l, down, owner(1, True), None), b + 8, place.partner)
        for part in range(2):
            wire.wait(window(l, down, owner(2, True), part), b + 9 + part, place.partner)

    for i in range(1, 8):
        j = (r - i + 8) % 8
        wire.wait(B["pin"].at[j], i, place.group + j)
    patch_rows = B["pin"][:, :, 0:192].reshape(128, 192)
    tiled = jnp.concatenate([positions[...].astype(f32)] * IMG, axis=0)
    C["x"][0] = mm(patch_rows, embed[...]) + tiled
    block_forward(0, 128, C, win_c)
    cut = block_end(0, C, wdn_c).astype(bf16)
    arrived[x, z] = cut.reshape(IMG, TOK, D)
    first, second, third, fourth, fifth = plane_gather(wire, place, arrived, 52)
    first()
    forward(pieces[0])
    selector, hot, table = route(arow[...], labels[...], shard, r)
    B["table"][...] = table
    to_scalar = pltpu.make_async_copy(B["table"], source, local_sem.at[4])
    to_scalar.start()
    second()
    forward(pieces[1])
    for piece in pieces[2:]:
        spread_first(piece)
        spread_last(piece)
    col = iota((1, 512), 1)
    at = col & 15
    lane = ((col >> 4) & 15) * 24 + (col >> 8) * 3
    wanted = lane + (at // 3) * 6 + at % 3
    B["order"][0] = ((iota((D, 512), 0) == wanted) & (at < 12)).astype(f32).astype(bf16)
    for q in range(3):
        entry = jnp.maximum(at - 12, 0) + 4 * q
        wanted = lane + (entry // 3) * 6 + entry % 3
        B["order"][1 + q] = ((iota((D, 512), 0) == wanted) & (at >= 12)).astype(f32).astype(bf16)
    B["pp"][...] = (iota((128, D), 1) - 256 == (iota((128, D), 0) & 15)).astype(f32).astype(bf16)
    B["pp"][:, 0:192] = B["pin"][:, :, 0:192].reshape(128, 192)
    packed[:, PACK - 48 :, :] = jnp.zeros((8, 48, D), bf16)
    third()
    across(pieces[0])
    across(pieces[1])
    forward(pieces[2])
    fourth()
    settle(pieces[0])
    forward(pieces[3])
    fifth()

    S["x"][0] = slot_rows(selector, arrived[...].reshape(2048, D))
    block_forward(0, 256, S, win)
    settle(pieces[1])
    S["x"][1] = block_end(0, S, wdn)
    across(pieces[2])
    settle(pieces[2])
    block_forward(1, 256, S, win, lambda: across(pieces[3]))
    settle(pieces[3])
    S["x"][2] = block_end(1, S, wdn)
    to_scalar.wait()
    ours = iota((CLASSES, SHARDS, D), 1) == shard
    table = jnp.sum(jnp.where(ours, classes[...].astype(f32), 0.0), axis=1).astype(bf16)
    loss, gcls, dlast = head_loss(S["x"][LAYERS], table, hot)
    losses[...] = loss
    for k in range(8):
        packed[k, PACK - 48 :, 0:CLASSES] = gcls[48 * k : 48 * k + 48]
    S["dy"][...] = dlast

    def backward(i, carry):
        block_backward(LAYERS - 1 - i, 256, S, win, wdn, S["dy"])
        return carry

    lax.fori_loop(0, LAYERS, backward, 0)

    line_x, line_z = B["line_x"], B["line_z"]
    gcut = S["dy"][...].astype(bf16).reshape(CAP, TOK, D)
    line_x[x] = gcut[:8]
    line_z[z] = gcut[8:]
    lines = (
        Line(wire, x, place.xp, place.xm, 76, lambda at, h: line_x.at[at, pl.ds(4 * h, 4)]),
        Line(wire, z, place.zp, place.zm, 82, lambda at, h: line_z.at[at, pl.ds(4 * h, 4)]),
    )
    for line in lines:
        line.send()

    def server_weights(l):
        for b, u, dout in weight_pairs(S, l):
            val = mm(u[...], dout[...], 0, 0).astype(bf16)
            for k in range(8):
                packed[k, 576 * l + 48 * b : 576 * l + 48 * b + 48, :] = val[48 * k : 48 * k + 48]
        for n in range(4):
            val = mm(S["h"][l, :, D * n : D * n + D], S["dyb"][l], 0, 0).astype(bf16)
            for j in range(2):
                packed[2 * n + j, 576 * l + D : 576 * l + 576, :] = val[192 * j : 192 * j + 192]

    rows_a, rows_b = pl.ds(0, CUT_A), pl.ds(CUT_A, PACK - CUT_A)

    def row(k, core):
        return (y + k) % 4 * 2 + core

    def swap(part, k0):
        for k in (2, 1, 3, 0):
            wire.send(packed.at[row(k, 1 - c), part], B["swapped"].at[k, part], k0 + k, place.partner)

    def combine(k, part, k0, start, stop):
        wire.wait(B["swapped"].at[k, part], k0 + k, place.partner)

        def body(rows):
            total = packed[row(k, c), rows, :].astype(f32) + B["swapped"][k, rows, :].astype(f32)
            packed[row(k, c), rows, :] = total.astype(bf16)

        add_rows(start, stop, 48, body)

    def combine_a(k):
        combine(k, rows_a, 94, 0, CUT_A)

    def combine_b(k):
        combine(k, rows_b, 98, CUT_A, PACK)

    server_weights(1)
    swap(rows_b, 98)
    for line in lines:
        line.relay()
    combine_b(2)
    wire.send(packed.at[row(2, c), rows_b], B["from_p"], 102, place.ym)
    combine_b(1)
    wire.send(packed.at[row(1, c), rows_b], B["fin_p"].at[rows_b], 103, place.yp)
    for line in lines:
        line.rest()
    pick_x, pick_z = B["pick_x"], B["pick_z"]

    def ring_one(src, hop, end, h, up, down, k0, k):
        if k == 2:
            wire.send(src(2, 0), hop.at[0], k0, up)
            wire.send(src(2, 1), hop.at[1], k0 + 1, down)
        if k == 1:
            wire.send(src(1, 1), end.at[0, pl.ds(h, h)], k0 + 2, up)
        if k == 3:
            wire.send(src(3, 0), end.at[1, pl.ds(0, h)], k0 + 3, down)

    def ring_two(src, load, hop, end, h, up, down, k0):
        wire.wait(hop.at[0], k0, down)
        load(1, 0, hop)
        wire.send(src(1, 0), end.at[0, pl.ds(0, h)], k0 + 4, up)
        wire.wait(hop.at[1], k0 + 1, up)
        load(3, 1, hop)
        wire.send(src(3, 1), end.at[1, pl.ds(h, h)], k0 + 5, down)

    def ring_three(end, h, up, down, k0):
        wire.wait(end.at[0, pl.ds(h, h)], k0 + 2, down)
        wire.wait(end.at[1, pl.ds(0, h)], k0 + 3, up)
        wire.wait(end.at[0, pl.ds(0, h)], k0 + 4, down)
        wire.wait(end.at[1, pl.ds(h, h)], k0 + 5, up)

    def part_of(pick):
        return lambda k, part: pick.at[k, pl.ds(4 * part, 4)]

    def load_of(pick):
        def load(k, part, hop):
            for i in range(4):
                at = 4 * part + i
                pick[k, at] = (pick[k, at].astype(f32) + hop[part, i].astype(f32)).astype(bf16)

        return load

    for k in (2, 1, 3, 0):
        zd, xd = (z + k) % 4, (x + k) % 4
        for m in range(8):
            at = source[0, (x * 4 + zd) * 8 + m]
            here = ((at >> 4) & 3 == z) & ((at & 15) < 8)
            pick_x[k, m] = jnp.where(here, line_x[(at >> 6) & 3, at & 7].astype(f32), 0.0).astype(bf16)
        ring_one(part_of(pick_x), B["ret_x"], B["got_x"], 4, place.zp, place.zm, 88, k)
        for m in range(8):
            at = source[0, (xd * 4 + z) * 8 + m]
            here = ((at >> 6) & 3 == x) & ((at & 15) >= 8)
            pick_z[k, m] = jnp.where(here, line_z[(at >> 4) & 3, at & 7].astype(f32), 0.0).astype(bf16)
        ring_one(part_of(pick_z), B["ret_z"], B["got_z"], 4, place.xp, place.xm, 109, k)
    server_weights(0)
    swap(rows_a, 94)
    ring_two(part_of(pick_x), load_of(pick_x), B["ret_x"], B["got_x"], 4, place.zp, place.zm, 88)
    ring_two(part_of(pick_z), load_of(pick_z), B["ret_z"], B["got_z"], 4, place.xp, place.xm, 109)
    combine_a(2)
    wire.send(packed.at[row(2, c), rows_a], B["from_m"], 104, place.yp)
    combine_a(3)
    wire.send(packed.at[row(3, c), rows_a], B["fin_m"].at[rows_a], 105, place.ym)
    combine_a(1)
    combine_b(3)
    ring_three(B["got_x"], 4, place.zp, place.zm, 88)
    ring_three(B["got_z"], 4, place.xp, place.xm, 109)
    for m in range(8):
        piece = pick_x[0, m].astype(f32) + pick_z[0, m].astype(f32)
        for k in range(2):
            piece = piece + B["got_x"][k, m].astype(f32) + B["got_z"][k, m].astype(f32)
        C["dy"][16 * m : 16 * m + 16] = piece
    cpack, cswap, cmine = B["cpack"], B["cswap"], B["cmine"]
    pairs = weight_pairs(C, 0)

    def emit(b, u, dout):
        val = mm(dout[...], u[...], 0, 0).astype(bf16)
        for i in range(2):
            for k in range(4):
                for core in range(2):
                    low = 192 * i + 48 * k + 24 * core
                    cpack[2 * b + i, core, 24 * k : 24 * k + 24] = val[low : low + 24]
        pair = pl.ds(2 * b, 2)
        wire.send(cpack.at[pair, 1 - c, pl.ds(0, MAIN)], cswap.at[pair, pl.ds(0, MAIN)], 116 + b, place.partner)

    def early():
        for pair in pairs[4:]:
            emit(*pair)
        B["dperm"][0] = mm(C["dyb"][0], B["order"][0]).astype(bf16)

    block_backward(0, 128, C, win_c, wdn_c, C["dy"], early)
    for pair in pairs[:4]:
        emit(*pair)
    last = C["dy"][...].astype(bf16)
    for q in range(4):
        val = mm(B["dperm"][0], C["h"][0, :, D * q : D * q + D], 0, 0)
        if q < 3:
            B["dperm"][1] = mm(last, B["order"][1 + q]).astype(bf16)
            val = val + mm(B["dperm"][1], B["pp"][...], 0, 0)
        val = val.astype(bf16)
        for core in range(2):
            for i in range(16):
                low = 256 * core + 16 * i
                cpack[i, core, MAIN + 16 * q : MAIN + 16 * q + 16] = val[low : low + 16]
    wire.send(cpack.at[:, 1 - c, pl.ds(MAIN, TAIL)], cswap.at[:, pl.ds(MAIN, TAIL)], 124, place.partner)

    X, Z = pl.ds(0, PART), pl.ds(PART, PART)

    def fold_x(k):
        for i in range(4):
            to = (x + k) % 4
            total = cpack[4 * to + i, c, :PART].astype(f32) + cswap[4 * to + i, :PART].astype(f32)
            cmine[to, i, :PART] = total.astype(bf16)

    def fold_z(k):
        for i in range(4):
            to = (z + k) % 4
            total = cpack[4 * i + to, c, PART:].astype(f32) + cswap[4 * i + to, PART:].astype(f32)
            cmine[i, to, PART:] = total.astype(bf16)

    def src_x(k, part):
        return cmine.at[(x + k) % 4, pl.ds(2 * part, 2), X]

    def src_z(k, part):
        return cmine.at[pl.ds(2 * part, 2), (z + k) % 4, Z]

    def load_x(k, part, hop):
        to = (x + k) % 4
        for i in range(2):
            at = 2 * part + i
            cmine[to, at, :PART] = (cmine[to, at, :PART].astype(f32) + hop[part, i].astype(f32)).astype(bf16)

    def load_z(k, part, hop):
        to = (z + k) % 4
        for i in range(2):
            at = 2 * part + i
            cmine[at, to, PART:] = (cmine[at, to, PART:].astype(f32) + hop[part, i].astype(f32)).astype(bf16)

    for b in (4, 5, 6, 7, 0, 1, 2, 3):
        wire.wait(cswap.at[pl.ds(2 * b, 2), pl.ds(0, MAIN)], 116 + b, place.partner)
    for k in (2, 1, 3):
        fold_x(k)
        ring_one(src_x, B["hop_x"], B["end_x"], 2, place.xp, place.xm, 125, k)
    wire.wait(cswap.at[:, pl.ds(MAIN, TAIL)], 124, place.partner)
    for k in (2, 1, 3):
        fold_z(k)
        ring_one(src_z, B["hop_z"], B["end_z"], 2, place.zp, place.zm, 131, k)

    fold_x(0)
    fold_z(0)

    wire.wait(B["from_m"], 104, place.ym)

    def add_a(rows):
        packed[row(1, c), rows, :] = (packed[row(1, c), rows, :].astype(f32) + B["from_m"][rows, :].astype(f32)).astype(bf16)

    add_rows(0, CUT_A, 48, add_a)
    wire.send(packed.at[row(1, c), rows_a], B["fin_p"].at[rows_a], 106, place.yp)
    wire.wait(B["from_p"], 102, place.yp)

    def add_b(i, carry):
        here = pl.ds(pl.multiple_of(i * 48, 16), 48)
        rows = pl.ds(pl.multiple_of(CUT_A + i * 48, 16), 48)
        packed[row(3, c), rows, :] = (packed[row(3, c), rows, :].astype(f32) + B["from_p"][here, :].astype(f32)).astype(bf16)
        return carry

    lax.fori_loop(0, (PACK - CUT_A) // 48, add_b, 0)
    wire.send(packed.at[row(3, c), rows_b], B["fin_m"].at[rows_b], 107, place.ym)

    ring_two(src_x, load_x, B["hop_x"], B["end_x"], 2, place.xp, place.xm, 125)
    ring_two(src_z, load_z, B["hop_z"], B["end_z"], 2, place.zp, place.zm, 131)
    half_x, half_z = B["half_x"], B["half_z"]
    ring_three(B["end_x"], 2, place.xp, place.xm, 125)
    for i in range(4):
        total = cmine[x, i, :PART].astype(f32) + B["end_x"][0, i].astype(f32) + B["end_x"][1, i].astype(f32)
        half_x[i] = total.astype(bf16)
    for k in (2, 1, 3):
        wire.send(half_x.at[(z + k) % 4], B["two_x"].at[k - 1], 136 + k, place.at(0, k, 0))
    ring_three(B["end_z"], 2, place.zp, place.zm, 131)
    for i in range(4):
        total = cmine[i, z, PART:].astype(f32) + B["end_z"][0, i].astype(f32) + B["end_z"][1, i].astype(f32)
        half_z[i] = total.astype(bf16)
    for k in (2, 1, 3):
        wire.send(half_z.at[(x + k) % 4], B["two_z"].at[k - 1], 139 + k, place.at(k, 0, 0))
    combine_a(0)
    combine_b(0)
    for k in range(1, 4):
        wire.wait(B["two_x"].at[k - 1], 136 + k, place.at(0, 4 - k, 0))
    upper = half_x[z].astype(f32)
    for k in range(3):
        upper = upper + B["two_x"][k].astype(f32)
    for k in range(1, 4):
        wire.wait(B["two_z"].at[k - 1], 139 + k, place.at(4 - k, 0, 0))
    lower = half_z[x].astype(f32)
    for k in range(3):
        lower = lower + B["two_z"][k].astype(f32)
    line, column = iota((64, TAIL), 0), iota((64, TAIL), 1)
    inside, owner_y = line & 15, line >> 4
    entry = owner_y * 3 + inside % 3
    spot = jnp.where(inside < 12, (inside // 3) * 16 + entry, (entry // 4) * 16 + 12 + entry % 4)
    pick = (column == spot) & (inside < 15)
    ordered = mm(pick.astype(f32).astype(bf16), lower[16:].astype(bf16)).astype(bf16)
    main = jnp.concatenate([upper, lower[:16]], axis=0).astype(bf16)
    for k in range(4):
        B["low_x"][k] = main[24 * k : 24 * k + 24]
        B["low_z"][k] = ordered[16 * k : 16 * k + 16]
    for k in (2, 1, 3):
        to = (y + k) % 4
        wire.send(B["low_x"].at[to], B["three_x"].at[k - 1], 142 + k, place.at(0, 0, k))
        wire.send(B["low_z"].at[to], B["three_z"].at[k - 1], 145 + k, place.at(0, 0, k))

    wire.wait(B["fin_p"].at[rows_b], 103, place.ym)
    wire.wait(B["fin_m"].at[rows_a], 105, place.yp)
    wire.wait(B["fin_p"].at[rows_a], 106, place.ym)
    wire.wait(B["fin_m"].at[rows_b], 107, place.yp)

    def total_of(first_row, rows):
        at = pl.ds(first_row, rows)
        return packed[row(0, c), at, :].astype(f32) + B["fin_p"][at, :].astype(f32) + B["fin_m"][at, :].astype(f32)

    for l in range(LAYERS):
        for b in range(8):
            B["gin"][l, :, D * b : D * b + D] = total_of(576 * l + 48 * b, 48)
        for b in range(4):
            B["gdn"][l, 48 * b : 48 * b + 48, :] = total_of(576 * l + D + 48 * b, 48)
    leaving = [
        pltpu.make_async_copy(B["gin"], gin, local_sem.at[5]),
        pltpu.make_async_copy(B["gdn"], gdn, local_sem.at[6]),
    ]
    for copy in leaving:
        copy.start()
    gcls_out[...] = total_of(PACK - 48, 48)[:, 0:128].T[0:CLASSES]

    for k in range(1, 4):
        wire.wait(B["three_x"].at[k - 1], 142 + k, place.at(0, 0, 4 - k))
        wire.wait(B["three_z"].at[k - 1], 145 + k, place.at(0, 0, 4 - k))
    main = B["low_x"][y].astype(f32)
    tail = B["low_z"][y].astype(f32)
    for k in range(3):
        main = main + B["three_x"][k].astype(f32)
        tail = tail + B["three_z"][k].astype(f32)
    out_in[...] = main
    for q in range(4):
        out_dn[:, D * q : D * q + D] = tail[3 * q : 3 * q + 3]
    out_pe[...] = tail[12:15, 0:192]
    out_pos[...] = tail[12:15, 256:272]
    for copy in leaving:
        copy.wait()
    wire.finish()


def finish_kernel(*refs):
    count = len(refs) // 3
    given, results, held = refs[:count], refs[count : 2 * count], refs[2 * count : 3 * count]
    sem = refs[-1]
    inward = [pltpu.make_async_copy(given[n], held[n], sem.at[0, n]) for n in range(count)]
    outward = [pltpu.make_async_copy(held[n], results[n], sem.at[1, n]) for n in range(count)]
    for copy in inward:
        copy.start()
    for copy, onward in zip(inward, outward):
        copy.wait()
        onward.start()
    for copy in outward:
        copy.wait()


def per_device(patches, labels, assign, patch_embed, positions, client_in, client_down, server_in, server_down, classifier):
    shapes = [
        ((1, CAP), f32),
        ((LAYERS, 48, 4 * D + FF), f32),
        ((LAYERS, 192, D), f32),
        ((CLASSES, 48), f32),
        ((24, D), f32),
        ((3, FF), f32),
        ((3, 192), f32),
        ((3, TOK), f32),
    ]
    scratch = list(CLIENT.values()) + list(SERVER.values()) + list(BUFFERS.values())
    results = pl.pallas_call(
        step_kernel,
        out_shape=[jax.ShapeDtypeStruct(*s) for s in shapes],
        in_specs=[VMEM] * 6 + [ANY] * 4,
        out_specs=[VMEM, HBM, HBM] + [VMEM] * 5,
        scratch_shapes=[pltpu.VMEM(*s) for s in scratch]
        + [
            pltpu.SemaphoreType.DMA((N_SEM,)),
            pltpu.SemaphoreType.DMA((N_SEM,)),
            pltpu.SemaphoreType.DMA((7,)),
            pltpu.SMEM((1, 128), jnp.int32),
        ],
        compiler_params=pltpu.CompilerParams(collective_id=0, has_side_effects=True, vmem_limit_bytes=67043328),
        name="step",
    )(
        patches.T,
        patch_embed,
        positions,
        assign.reshape(1, 128),
        labels.reshape(8, 128),
        classifier.transpose(2, 0, 1),
        client_in[None],
        client_down[None],
        server_in,
        server_down,
    )
    losses, gin, gdn, gcls, out_in, out_dn, out_pe, out_pos = pl.pallas_call(
        finish_kernel,
        out_shape=[jax.ShapeDtypeStruct(*s) for s in shapes],
        in_specs=[HBM] * len(shapes),
        out_specs=[HBM] * len(shapes),
        scratch_shapes=[pltpu.VMEM(*s) for s in shapes] + [pltpu.SemaphoreType.DMA((2, len(shapes)))],
        compiler_params=pltpu.CompilerParams(vmem_limit_bytes=67043328),
        name="finish",
    )(*results)
    return losses, out_pe.T, out_pos.T, out_in.T, out_dn.T, gin, gdn, gcls.T


def solution(mesh):
    in_specs = (
        P("client", None),
        P(),
        P(),
        P(),
        P(),
        P(),
        P(),
        P(None, "client", None),
        P(None, "client", None),
        P(),
    )
    out_specs = (
        P("client", None),
        P(None, "client"),
        P(None, "client"),
        P(None, "client"),
        P(None, "client"),
        P(None, "client", None),
        P(None, "client", None),
        P("client", None),
    )
    return jax.shard_map(per_device, mesh=mesh, in_specs=in_specs, out_specs=out_specs, check_vma=False)
```

```python
import math

import jax
import jax.numpy as jnp
from jax import lax
from jax.experimental import pallas as pl
from jax.experimental.pallas import tpu as pltpu
from jax.sharding import PartitionSpec as P

D = 384
FF = 1536
TOK = 16
IMG = 8
CLASSES = 10
SHARDS = 16
LAYERS = 2
CAP = 16
EPSILON = 1e-06
SCALE = 0.125
GELU_A = math.sqrt(2.0 / math.pi)
GELU_B = 0.044715
PACK = LAYERS * (D + FF // 8) + D // 8
CUT_A = 576
MAIN = 96
TAIL = 64
PART = 80
BLOCK = MAIN + TAIL

bf16 = jnp.bfloat16
f32 = jnp.float32
MESH = pl.DeviceIdType.MESH
VMEM = pl.BlockSpec(memory_space=pltpu.VMEM)
SMEM = pl.BlockSpec(memory_space=pltpu.SMEM)
ANY = pl.BlockSpec(memory_space=pl.ANY)
HBM = pl.BlockSpec(memory_space=pltpu.HBM)


def mm(a, b, ca=1, cb=0):
    return lax.dot_general(a, b, (((ca,), (cb,)), ((), ())), preferred_element_type=f32)


def iota(shape, dim):
    return lax.broadcasted_iota(jnp.int32, shape, dim)


def norm(v):
    centre = v - jnp.mean(v, axis=-1, keepdims=True)
    rstd = lax.rsqrt(jnp.mean(centre * centre, axis=-1, keepdims=True) + EPSILON)
    return centre * rstd, rstd


def norm_back(v, grad):
    hat, rstd = norm(v)
    along = jnp.mean(grad * hat, axis=-1, keepdims=True)
    return rstd * (grad - jnp.mean(grad, axis=-1, keepdims=True) - hat * along)


def rounded(v):
    return v.astype(bf16).astype(f32)


def head_masks(rows):
    low = (iota((rows, 128), 1) < 64).astype(f32)
    return low.astype(bf16), (1.0 - low).astype(bf16)


def two_heads(v):
    low, high = head_masks(v.shape[0])
    return jnp.concatenate([v * low, v * high], axis=0)


def merge_heads(v):
    rows = v.shape[0] // 2
    return jnp.where(iota((rows, 128), 1) < 64, v[:rows], v[rows:])


def block_forward(l, rows, S, win, middle=None):
    x = S["x"][l]
    hat, _ = norm(x)
    u1 = hat.astype(bf16)
    S["u1"][l] = u1
    for n in range(3):
        cols = slice(D * n, D * n + D)
        S["qkv"][l, :, cols] = mm(u1, win[l, :, cols]).astype(bf16)
    same = ((iota((256, 128), 0) & 127) >> 4) == (iota((256, 128), 1) >> 4)
    for g in range(rows // 128):
        part = slice(128 * g, 128 * g + 128)
        for p in range(3):
            q2 = S["qkv"][l, part, 128 * p : 128 * p + 128]
            k2 = S["qkv"][l, part, D + 128 * p : D + 128 * p + 128]
            v2 = S["qkv"][l, part, 2 * D + 128 * p : 2 * D + 128 * p + 128]
            scores = mm(two_heads(q2), k2, 1, 1) * SCALE
            scores = jnp.where(same, scores, -1e30)
            grown = jnp.exp(scores - jnp.max(scores, axis=-1, keepdims=True))
            prob = grown / jnp.sum(grown, axis=-1, keepdims=True)
            S["prob"][l, 3 * g + p] = prob
            S["att"][l, part, 128 * p : 128 * p + 128] = merge_heads(mm(prob.astype(bf16), v2)).astype(bf16)
    x1 = S["x"][l] + mm(S["att"][l], win[l, :, 3 * D : 4 * D])
    S["x1"][l] = x1
    hat, _ = norm(x1)
    u2 = hat.astype(bf16)
    S["u2"][l] = u2
    if middle is not None:
        middle()
    for n in range(4):
        pre = mm(u2, win[l, :, 4 * D + D * n : 5 * D + D * n])
        square = pre * pre
        bent = jnp.tanh(pre * (GELU_A + GELU_A * GELU_B * square))
        gate = 0.5 + 0.5 * bent
        value = pre * gate
        S["h"][l, :, D * n : D * n + D] = value.astype(bf16)
        bend = value * (1.0 - bent)
        S["slope"][l, :, D * n : D * n + D] = gate + bend * (GELU_A + 3.0 * GELU_A * GELU_B * square)


def block_end(l, S, wdn):
    return S["x1"][l] + mm(S["h"][l], wdn[l])


def block_backward(l, rows, S, win, wdn, dy_ref, early=None):
    dyb = dy_ref[...].astype(bf16)
    S["dyb"][l] = dyb
    for n in range(4):
        cols = slice(D * n, D * n + D)
        dh = rounded(mm(dyb, wdn[l, cols, :], 1, 1))
        S["dpre"][l, :, cols] = (dh * S["slope"][l, :, cols]).astype(bf16)
    if early is not None:
        early()
    du2 = rounded(mm(S["dpre"][l], win[l, :, 4 * D :], 1, 1))
    dx1 = dy_ref[...] + norm_back(S["x1"][l], du2)
    dy_ref[...] = dx1
    dx1b = dx1.astype(bf16)
    S["dx1b"][l] = dx1b
    S["datt"][...] = mm(dx1b, win[l, :, 3 * D : 4 * D], 1, 1).astype(bf16)
    for g in range(rows // 128):
        part = slice(128 * g, 128 * g + 128)
        for p in range(3):
            cq = slice(128 * p, 128 * p + 128)
            ck = slice(D + 128 * p, D + 128 * p + 128)
            cv = slice(2 * D + 128 * p, 2 * D + 128 * p + 128)
            qs = two_heads(S["qkv"][l, part, cq])
            dos = two_heads(S["datt"][part, cq])
            prob = S["prob"][l, 3 * g + p]
            dprob = mm(dos, S["qkv"][l, part, cv], 1, 1)
            dscore = prob * (dprob - jnp.sum(prob * dprob, axis=-1, keepdims=True)) * SCALE
            dsb = dscore.astype(bf16)
            S["dqkv"][l, part, cq] = merge_heads(mm(dsb, S["qkv"][l, part, ck])).astype(bf16)
            S["dqkv"][l, part, ck] = mm(dsb, qs, 0, 0).astype(bf16)
            S["dqkv"][l, part, cv] = mm(prob.astype(bf16), dos, 0, 0).astype(bf16)
    du1 = rounded(mm(S["dqkv"][l], win[l, :, : 3 * D], 1, 1))
    dy_ref[...] = dy_ref[...] + norm_back(S["x"][l], du1)


def weight_pairs(S, l):
    pairs = []
    for n in range(3):
        pairs.append((n, S["u1"].at[l], S["dqkv"].at[l, :, pl.ds(D * n, D)]))
    pairs.append((3, S["att"].at[l], S["dx1b"].at[l]))
    for n in range(4):
        pairs.append((4 + n, S["u2"].at[l], S["dpre"].at[l, :, pl.ds(D * n, D)]))
    return pairs


def block_shapes(layers, rows):
    return dict(
        x=((layers + 1, rows, D), f32),
        x1=((layers, rows, D), f32),
        u1=((layers, rows, D), bf16),
        u2=((layers, rows, D), bf16),
        qkv=((layers, rows, 3 * D), bf16),
        prob=((layers, 3 * rows // 128, 256, 128), f32),
        att=((layers, rows, D), bf16),
        slope=((layers, rows, FF), f32),
        h=((layers, rows, FF), bf16),
        dyb=((layers, rows, D), bf16),
        dpre=((layers, rows, FF), bf16),
        dx1b=((layers, rows, D), bf16),
        datt=((rows, D), bf16),
        dqkv=((layers, rows, 3 * D), bf16),
        dy=((rows, D), f32),
    )


class Place:
    def __init__(self):
        me = lax.axis_index("client")
        self.me = me
        self.c, self.y, self.z, self.x = me % 2, me // 2 % 4, me // 8 % 4, me // 32
        self.r, self.group = me % 8, me // 8 * 8
        self.partner = me + 1 - 2 * self.c
        self.yp, self.ym = self.at(0, 0, 1), self.at(0, 0, 3)
        self.xp, self.xm = self.at(1, 0, 0), self.at(3, 0, 0)
        self.zp, self.zm = self.at(0, 1, 0), self.at(0, 3, 0)

    def at(self, dx, dz, dy):
        x, z, y = (self.x + dx) % 4, (self.z + dz) % 4, (self.y + dy) % 4
        return ((x * 4 + z) * 4 + y) * 2 + self.c

    def greet(self):
        peers = [self.group + (self.r + i) % 8 for i in range(1, 8)]
        peers += [self.xp, self.xm, self.zp, self.zm]
        barrier = pltpu.get_barrier_semaphore()
        for peer in peers:
            pl.semaphore_signal(barrier, inc=1, device_id=(peer,), device_id_type=MESH)
        return len(peers)


class Wire:
    def __init__(self, send_sem, recv_sem):
        self.send_sem, self.recv_sem, self.sent = send_sem, recv_sem, []

    def make(self, src, dst, k, device):
        return pltpu.make_async_remote_copy(
            src_ref=src,
            dst_ref=dst,
            send_sem=self.send_sem.at[k],
            recv_sem=self.recv_sem.at[k],
            device_id=(device,),
            device_id_type=MESH,
        )

    def send(self, src, dst, k, device):
        copy = self.make(src, dst, k, device)
        copy.start()
        self.sent.append(copy)

    def wait(self, landed, k, device):
        self.make(landed, landed, k, device).wait_recv()

    def finish(self):
        for copy in self.sent:
            copy.wait_send()


class Line:
    def __init__(self, wire, me, up, down, k, view):
        self.wire, self.me, self.up, self.down, self.k, self.view = wire, me, up, down, k, view

    def both(self, ref, k, device):
        self.wire.send(ref, ref, self.k + k, device)

    def send(self):
        self.both(self.view(self.me, 0), 0, self.up)
        self.both(self.view(self.me, 1), 1, self.down)
        self.both(self.view(self.me, 1), 2, self.up)
        self.both(self.view(self.me, 0), 3, self.down)

    def relay(self):
        left, right = (self.me + 3) % 4, (self.me + 1) % 4
        self.wire.wait(self.view(left, 0), self.k, self.down)
        self.both(self.view(left, 0), 4, self.up)
        self.wire.wait(self.view(right, 1), self.k + 1, self.up)
        self.both(self.view(right, 1), 5, self.down)

    def rest(self):
        left, right, far = (self.me + 3) % 4, (self.me + 1) % 4, (self.me + 2) % 4
        self.wire.wait(self.view(left, 1), self.k + 2, self.down)
        self.wire.wait(self.view(right, 0), self.k + 3, self.up)
        self.wire.wait(self.view(far, 0), self.k + 4, self.down)
        self.wire.wait(self.view(far, 1), self.k + 5, self.up)


def plane_gather(wire, place, buf, k0):
    x, z = place.x, place.z
    lines = (
        Line(wire, x, place.xp, place.xm, k0, lambda at, h: buf.at[at, z, pl.ds(2 * h, 2)]),
        Line(wire, z, place.zp, place.zm, k0 + 6, lambda at, h: buf.at[x, at, pl.ds(4 + 2 * h, 2)]),
        Line(wire, z, place.zp, place.zm, k0 + 12, lambda at, h: buf.at[pl.ds(2 * h, 2), at, pl.ds(0, 4)]),
        Line(wire, x, place.xp, place.xm, k0 + 18, lambda at, h: buf.at[at, pl.ds(2 * h, 2), pl.ds(4, 4)]),
    )

    def first():
        lines[0].send()
        lines[1].send()

    def second():
        lines[0].relay()
        lines[1].relay()

    def third():
        lines[0].rest()
        lines[2].send()
        lines[1].rest()
        lines[3].send()

    def fourth():
        lines[2].relay()
        lines[3].relay()

    def fifth():
        lines[2].rest()
        lines[3].rest()

    return first, second, third, fourth, fifth


def add_rows(start, stop, step, body):
    def run(i, carry):
        body(pl.ds(pl.multiple_of(start + i * step, 16), step))
        return carry

    lax.fori_loop(0, (stop - start) // step, run, 0)


def route(arow, labels, shard, rank_in):
    eye = iota((128, 128), 0) == iota((128, 128), 1)
    acol = jnp.sum(jnp.where(eye, arow.astype(f32), 0.0), axis=1, keepdims=True).astype(jnp.int32)
    earlier = (acol == arow) & (iota((128, 128), 0) < iota((128, 128), 1))
    rank = jnp.sum(earlier.astype(f32), axis=0, keepdims=True).astype(jnp.int32)
    chosen = (jnp.broadcast_to(arow, (CAP, 128)) == shard) & (
        jnp.broadcast_to(rank, (CAP, 128)) == iota((CAP, 128), 0)
    )
    selector = chosen.astype(f32).astype(bf16)
    take = (iota((128, 16), 0) == iota((128, 16), 1) * IMG + rank_in).astype(f32).astype(bf16)
    by_row = mm(labels.astype(f32).astype(bf16), take).astype(bf16)
    lift = ((iota((128, 8), 0) >> 4) == iota((128, 8), 1)).astype(f32).astype(bf16)
    tall = mm(lift, by_row)
    mine = (iota((128, 16), 0) & 15) == iota((128, 16), 1)
    label = jnp.sum(jnp.where(mine, tall, 0.0), axis=1, keepdims=True)
    onehot = (label == iota((128, CLASSES), 1).astype(f32)).astype(f32).astype(bf16)
    return selector, mm(selector, onehot), arow * CAP + rank


def slot_rows(selector, arrived):
    spread = (iota((128, 2048), 0) == (iota((128, 2048), 1) >> 4)).astype(f32).astype(bf16)
    wide = mm(selector, spread).astype(bf16)
    repeat = ((iota((256, CAP), 0) >> 4) == iota((256, CAP), 1)).astype(f32).astype(bf16)
    tall = mm(repeat, wide)
    same = (iota((256, 2048), 0) & 15) == (iota((256, 2048), 1) & 15)
    return mm(jnp.where(same, tall, 0.0).astype(bf16), arrived)


def head_loss(last, classes, hot):
    filled = jnp.sum(hot, axis=1, keepdims=True)
    mean = jnp.mean(last.reshape(CAP, TOK, D), axis=1)
    hat, _ = norm(mean)
    pooled = hat.astype(bf16)
    logits = mm(pooled, classes, 1, 1)
    top = jnp.max(logits, axis=1, keepdims=True)
    grown = jnp.exp(logits - top)
    total = jnp.sum(grown, axis=1, keepdims=True)
    per = (jnp.log(total) + top - jnp.sum(hot * logits, axis=1, keepdims=True)) * filled
    eye = iota((CAP, CAP), 0) == iota((CAP, CAP), 1)
    losses = jnp.sum(jnp.where(eye, per, 0.0), axis=0, keepdims=True)
    dlogits = ((grown / total) * filled - hot).astype(bf16)
    gcls = mm(pooled, dlogits, 0, 0).astype(bf16)
    dpooled = rounded(mm(dlogits, classes))
    dmean = norm_back(mean, dpooled) * (1.0 / TOK)
    dlast = jnp.broadcast_to(dmean[:, None, :], (CAP, TOK, D)).reshape(CAP * TOK, D)
    return losses, gcls, dlast


CLIENT = block_shapes(1, 128)
SERVER = block_shapes(LAYERS, 256)
BUFFERS = dict(
    arrived=((4, 4, IMG, TOK, D), bf16),
    win=((LAYERS, D, 4 * D + FF), bf16),
    wdn=((LAYERS, FF, D), bf16),
    patches_t=((192, 128), bf16),
    embed=((192, D), bf16),
    positions=((TOK, D), bf16),
    arow=((1, 128), jnp.int32),
    labels=((8, 128), jnp.int32),
    classes=((CLASSES, SHARDS, D), bf16),
    win_c=((1, D, 4 * D + FF), bf16),
    wdn_c=((1, FF, D), bf16),
    win_s=((LAYERS, 48, 4 * D + FF), bf16),
    wdn_s=((LAYERS, 192, D), bf16),
    table=((1, 128), jnp.int32),
    pout=((IMG, TOK, 256), bf16),
    pin=((IMG, TOK, 256), bf16),
    packed=((8, PACK, D), bf16),
    swapped=((4, PACK, D), bf16),
    from_m=((CUT_A, D), bf16),
    from_p=((PACK - CUT_A, D), bf16),
    fin_p=((PACK, D), bf16),
    fin_m=((PACK, D), bf16),
    line_x=((4, 8, TOK, D), bf16),
    line_z=((4, 8, TOK, D), bf16),
    pick_x=((4, 8, TOK, D), bf16),
    pick_z=((4, 8, TOK, D), bf16),
    ret_x=((2, 4, TOK, D), bf16),
    ret_z=((2, 4, TOK, D), bf16),
    got_x=((2, 8, TOK, D), bf16),
    got_z=((2, 8, TOK, D), bf16),
    order=((4, D, 512), bf16),
    dperm=((2, 128, 512), bf16),
    pp=((128, D), bf16),
    cpack=((16, 2, BLOCK, D), bf16),
    cswap=((16, BLOCK, D), bf16),
    cmine=((4, 4, BLOCK, D), bf16),
    hop_x=((2, 2, PART, D), bf16),
    hop_z=((2, 2, PART, D), bf16),
    end_x=((2, 4, PART, D), bf16),
    end_z=((2, 4, PART, D), bf16),
    half_x=((4, PART, D), bf16),
    half_z=((4, PART, D), bf16),
    two_x=((3, PART, D), bf16),
    two_z=((3, PART, D), bf16),
    low_x=((4, 24, D), bf16),
    low_z=((4, 16, D), bf16),
    three_x=((3, 24, D), bf16),
    three_z=((3, 16, D), bf16),
    gin=((LAYERS, 48, 4 * D + FF), f32),
    gdn=((LAYERS, 192, D), f32),
)
LOADED = ("patches_t", "embed", "positions", "arow", "labels", "classes", "win_c", "wdn_c", "win_s", "wdn_s")
N_SEM = 160


def step_kernel(*refs):
    sources, refs = refs[:10], refs[10:]
    losses, gin, gdn, gcls_out, out_in, out_dn, out_pe, out_pos = refs[:8]
    refs = list(refs[8:])
    C = dict(zip(CLIENT, refs[: len(CLIENT)]))
    refs = refs[len(CLIENT) :]
    S = dict(zip(SERVER, refs[: len(SERVER)]))
    refs = refs[len(SERVER) :]
    B = dict(zip(BUFFERS, refs[: len(BUFFERS)]))
    send_sem, recv_sem, local_sem, source = refs[len(BUFFERS) :]
    held = [B[name] for name in LOADED]
    patches_t, embed, positions, arow, labels, classes, win_c, wdn_c, win_s, wdn_s = held
    loads = [pltpu.make_async_copy(src, dst, local_sem.at[n]) for n, (src, dst) in enumerate(zip(sources, held))]
    place = Place()
    x, z, y, c, r = place.x, place.z, place.y, place.c, place.r
    shard = place.me // 8
    win, wdn, arrived, packed = B["win"], B["wdn"], B["arrived"], B["packed"]
    met = place.greet()
    for n in (8, 0, 9, 1, 2, 6, 7, 3, 4, 5):
        loads[n].start()
    B["pout"][...] = jnp.zeros_like(B["pout"])
    loads[0].wait()
    B["pout"][:, :, 0:192] = patches_t[...].T.reshape(IMG, TOK, 192)
    pl.semaphore_wait(pltpu.get_barrier_semaphore(), met)
    wire = Wire(send_sem, recv_sem)

    for i in range(1, 8):
        j = (r + i) % 8
        wire.send(B["pout"].at[j], B["pin"].at[r], i, place.group + j)
    B["pin"][r] = B["pout"][r]

    def owner(dy, other=False):
        return (y + dy) % 4 * 2 + (1 - c if other else c)

    def window(l, down, rank, part):
        if down:
            low, size = {None: (0, 192), 0: (0, 96), 1: (96, 96)}[part]
            return wdn.at[l, pl.ds(pl.multiple_of(rank * 192 + low, 16), size), :]
        cols = {None: pl.ds(0, 3072), 0: pl.ds(0, 1536), 1: pl.ds(1536, 1536)}[part]
        return win.at[l, pl.ds(pl.multiple_of(rank * 48, 16), 48), cols]

    pieces = [(l, down) for l in range(LAYERS) for down in (False, True)]
    base = {piece: 8 + 11 * n for n, piece in enumerate(pieces)}

    def own_part(piece, part):
        l, down = piece
        if down:
            return wdn_s.at[l, pl.ds(96 * part, 96), :]
        return win_s.at[l, :, pl.ds(1536 * part, 1536)]

    def spread_first(piece):
        for part, device in ((0, place.yp), (1, place.ym)):
            wire.send(own_part(piece, part), window(*piece, r, part), base[piece] + part, device)

    def spread_last(piece):
        for part, device in ((1, place.yp), (0, place.ym)):
            wire.send(own_part(piece, part), window(*piece, r, part), base[piece] + 3 - part, device)
        l, down = piece
        mine = (wdn_s if down else win_s).at[l]
        here = window(l, down, r, None)
        wire.send(mine, here, base[piece] + 6, place.partner)
        here[...] = mine[...]

    loads[8].wait()
    spread_first(pieces[0])
    spread_last(pieces[0])
    loads[9].wait()
    spread_first(pieces[1])
    spread_last(pieces[1])
    for n in range(1, 8):
        loads[n].wait()

    def forward(piece):
        l, down = piece
        b = base[piece]
        left, right = owner(3), owner(1)
        half = window(l, down, left, 0)
        wire.wait(half, b + 0, place.ym)
        wire.send(half, half, b + 4, place.yp)
        half = window(l, down, right, 1)
        wire.wait(half, b + 1, place.yp)
        wire.send(half, half, b + 5, place.ym)

    def across(piece):
        l, down = piece
        b = base[piece]
        left, right, far = owner(3), owner(1), owner(2)
        wire.wait(window(l, down, left, 1), b + 2, place.ym)
        whole = window(l, down, left, None)
        wire.send(whole, whole, b + 7, place.partner)
        wire.wait(window(l, down, right, 0), b + 3, place.yp)
        whole = window(l, down, right, None)
        wire.send(whole, whole, b + 8, place.partner)
        for part, device in ((0, place.ym), (1, place.yp)):
            half = window(l, down, far, part)
            wire.wait(half, b + 4 + part, device)
            wire.send(half, half, b + 9 + part, place.partner)

    def settle(piece):
        l, down = piece
        b = base[piece]
        wire.wait(window(l, down, owner(0, True), None), b + 6, place.partner)
        wire.wait(window(l, down, owner(3, True), None), b + 7, place.partner)
        wire.wait(window(l, down, owner(1, True), None), b + 8, place.partner)
        for part in range(2):
            wire.wait(window(l, down, owner(2, True), part), b + 9 + part, place.partner)

    for i in range(1, 8):
        j = (r - i + 8) % 8
        wire.wait(B["pin"].at[j], i, place.group + j)
    patch_rows = B["pin"][:, :, 0:192].reshape(128, 192)
    tiled = jnp.concatenate([positions[...].astype(f32)] * IMG, axis=0)
    C["x"][0] = mm(patch_rows, embed[...]) + tiled
    block_forward(0, 128, C, win_c)
    cut = block_end(0, C, wdn_c).astype(bf16)
    arrived[x, z] = cut.reshape(IMG, TOK, D)
    first, second, third, fourth, fifth = plane_gather(wire, place, arrived, 52)
    first()
    forward(pieces[0])
    selector, hot, table = route(arow[...], labels[...], shard, r)
    B["table"][...] = table
    to_scalar = pltpu.make_async_copy(B["table"], source, local_sem.at[10])
    to_scalar.start()
    second()
    forward(pieces[1])
    for piece in pieces[2:]:
        spread_first(piece)
        spread_last(piece)
    col = iota((1, 512), 1)
    at = col & 15
    lane = ((col >> 4) & 15) * 24 + (col >> 8) * 3
    wanted = lane + (at // 3) * 6 + at % 3
    B["order"][0] = ((iota((D, 512), 0) == wanted) & (at < 12)).astype(f32).astype(bf16)
    for q in range(3):
        entry = jnp.maximum(at - 12, 0) + 4 * q
        wanted = lane + (entry // 3) * 6 + entry % 3
        B["order"][1 + q] = ((iota((D, 512), 0) == wanted) & (at >= 12)).astype(f32).astype(bf16)
    B["pp"][...] = (iota((128, D), 1) - 256 == (iota((128, D), 0) & 15)).astype(f32).astype(bf16)
    B["pp"][:, 0:192] = B["pin"][:, :, 0:192].reshape(128, 192)
    packed[:, PACK - 48 :, :] = jnp.zeros((8, 48, D), bf16)
    third()
    across(pieces[0])
    across(pieces[1])
    forward(pieces[2])
    fourth()
    settle(pieces[0])
    forward(pieces[3])
    fifth()

    S["x"][0] = slot_rows(selector, arrived[...].reshape(2048, D))
    block_forward(0, 256, S, win)
    settle(pieces[1])
    S["x"][1] = block_end(0, S, wdn)
    across(pieces[2])
    settle(pieces[2])
    block_forward(1, 256, S, win, lambda: across(pieces[3]))
    settle(pieces[3])
    S["x"][2] = block_end(1, S, wdn)
    to_scalar.wait()
    ours = iota((CLASSES, SHARDS, D), 1) == shard
    table = jnp.sum(jnp.where(ours, classes[...].astype(f32), 0.0), axis=1).astype(bf16)
    loss, gcls, dlast = head_loss(S["x"][LAYERS], table, hot)
    losses[...] = loss
    for k in range(8):
        packed[k, PACK - 48 :, 0:CLASSES] = gcls[48 * k : 48 * k + 48]
    S["dy"][...] = dlast

    def backward(i, carry):
        block_backward(LAYERS - 1 - i, 256, S, win, wdn, S["dy"])
        return carry

    lax.fori_loop(0, LAYERS, backward, 0)

    line_x, line_z = B["line_x"], B["line_z"]
    gcut = S["dy"][...].astype(bf16).reshape(CAP, TOK, D)
    line_x[x] = gcut[:8]
    line_z[z] = gcut[8:]
    lines = (
        Line(wire, x, place.xp, place.xm, 76, lambda at, h: line_x.at[at, pl.ds(4 * h, 4)]),
        Line(wire, z, place.zp, place.zm, 82, lambda at, h: line_z.at[at, pl.ds(4 * h, 4)]),
    )
    for line in lines:
        line.send()

    def server_weights(l):
        for b, u, dout in weight_pairs(S, l):
            val = mm(u[...], dout[...], 0, 0).astype(bf16)
            for k in range(8):
                packed[k, 576 * l + 48 * b : 576 * l + 48 * b + 48, :] = val[48 * k : 48 * k + 48]
        for n in range(4):
            val = mm(S["h"][l, :, D * n : D * n + D], S["dyb"][l], 0, 0).astype(bf16)
            for j in range(2):
                packed[2 * n + j, 576 * l + D : 576 * l + 576, :] = val[192 * j : 192 * j + 192]

    rows_a, rows_b = pl.ds(0, CUT_A), pl.ds(CUT_A, PACK - CUT_A)

    def row(k, core):
        return (y + k) % 4 * 2 + core

    def swap(part, k0):
        for k in (2, 1, 3, 0):
            wire.send(packed.at[row(k, 1 - c), part], B["swapped"].at[k, part], k0 + k, place.partner)

    def combine(k, part, k0, start, stop):
        wire.wait(B["swapped"].at[k, part], k0 + k, place.partner)

        def body(rows):
            total = packed[row(k, c), rows, :].astype(f32) + B["swapped"][k, rows, :].astype(f32)
            packed[row(k, c), rows, :] = total.astype(bf16)

        add_rows(start, stop, 48, body)

    def combine_a(k):
        combine(k, rows_a, 94, 0, CUT_A)

    def combine_b(k):
        combine(k, rows_b, 98, CUT_A, PACK)

    server_weights(1)
    swap(rows_b, 98)
    for line in lines:
        line.relay()
    combine_b(2)
    wire.send(packed.at[row(2, c), rows_b], B["from_p"], 102, place.ym)
    combine_b(1)
    wire.send(packed.at[row(1, c), rows_b], B["fin_p"].at[rows_b], 103, place.yp)
    for line in lines:
        line.rest()
    pick_x, pick_z = B["pick_x"], B["pick_z"]

    def ring_one(src, hop, end, h, up, down, k0, k):
        if k == 2:
            wire.send(src(2, 0), hop.at[0], k0, up)
            wire.send(src(2, 1), hop.at[1], k0 + 1, down)
        if k == 1:
            wire.send(src(1, 1), end.at[0, pl.ds(h, h)], k0 + 2, up)
        if k == 3:
            wire.send(src(3, 0), end.at[1, pl.ds(0, h)], k0 + 3, down)

    def ring_two(src, load, hop, end, h, up, down, k0):
        wire.wait(hop.at[0], k0, down)
        load(1, 0, hop)
        wire.send(src(1, 0), end.at[0, pl.ds(0, h)], k0 + 4, up)
        wire.wait(hop.at[1], k0 + 1, up)
        load(3, 1, hop)
        wire.send(src(3, 1), end.at[1, pl.ds(h, h)], k0 + 5, down)

    def ring_three(end, h, up, down, k0):
        wire.wait(end.at[0, pl.ds(h, h)], k0 + 2, down)
        wire.wait(end.at[1, pl.ds(0, h)], k0 + 3, up)
        wire.wait(end.at[0, pl.ds(0, h)], k0 + 4, down)
        wire.wait(end.at[1, pl.ds(h, h)], k0 + 5, up)

    def part_of(pick):
        return lambda k, part: pick.at[k, pl.ds(4 * part, 4)]

    def load_of(pick):
        def load(k, part, hop):
            for i in range(4):
                at = 4 * part + i
                pick[k, at] = (pick[k, at].astype(f32) + hop[part, i].astype(f32)).astype(bf16)

        return load

    for k in (2, 1, 3, 0):
        zd, xd = (z + k) % 4, (x + k) % 4
        for m in range(8):
            at = source[0, (x * 4 + zd) * 8 + m]
            here = ((at >> 4) & 3 == z) & ((at & 15) < 8)
            pick_x[k, m] = jnp.where(here, line_x[(at >> 6) & 3, at & 7].astype(f32), 0.0).astype(bf16)
        ring_one(part_of(pick_x), B["ret_x"], B["got_x"], 4, place.zp, place.zm, 88, k)
        for m in range(8):
            at = source[0, (xd * 4 + z) * 8 + m]
            here = ((at >> 6) & 3 == x) & ((at & 15) >= 8)
            pick_z[k, m] = jnp.where(here, line_z[(at >> 4) & 3, at & 7].astype(f32), 0.0).astype(bf16)
        ring_one(part_of(pick_z), B["ret_z"], B["got_z"], 4, place.xp, place.xm, 109, k)
    server_weights(0)
    swap(rows_a, 94)
    ring_two(part_of(pick_x), load_of(pick_x), B["ret_x"], B["got_x"], 4, place.zp, place.zm, 88)
    ring_two(part_of(pick_z), load_of(pick_z), B["ret_z"], B["got_z"], 4, place.xp, place.xm, 109)
    combine_a(2)
    wire.send(packed.at[row(2, c), rows_a], B["from_m"], 104, place.yp)
    combine_a(3)
    wire.send(packed.at[row(3, c), rows_a], B["fin_m"].at[rows_a], 105, place.ym)
    combine_a(1)
    combine_b(3)
    ring_three(B["got_x"], 4, place.zp, place.zm, 88)
    ring_three(B["got_z"], 4, place.xp, place.xm, 109)
    for m in range(8):
        piece = pick_x[0, m].astype(f32) + pick_z[0, m].astype(f32)
        for k in range(2):
            piece = piece + B["got_x"][k, m].astype(f32) + B["got_z"][k, m].astype(f32)
        C["dy"][16 * m : 16 * m + 16] = piece
    cpack, cswap, cmine = B["cpack"], B["cswap"], B["cmine"]
    pairs = weight_pairs(C, 0)

    def emit(b, u, dout):
        val = mm(dout[...], u[...], 0, 0).astype(bf16)
        for i in range(2):
            for k in range(4):
                for core in range(2):
                    low = 192 * i + 48 * k + 24 * core
                    cpack[2 * b + i, core, 24 * k : 24 * k + 24] = val[low : low + 24]
        pair = pl.ds(2 * b, 2)
        wire.send(cpack.at[pair, 1 - c, pl.ds(0, MAIN)], cswap.at[pair, pl.ds(0, MAIN)], 116 + b, place.partner)

    def early():
        for pair in pairs[4:]:
            emit(*pair)
        B["dperm"][0] = mm(C["dyb"][0], B["order"][0]).astype(bf16)

    block_backward(0, 128, C, win_c, wdn_c, C["dy"], early)
    for pair in pairs[:4]:
        emit(*pair)
    last = C["dy"][...].astype(bf16)
    for q in range(4):
        val = mm(B["dperm"][0], C["h"][0, :, D * q : D * q + D], 0, 0)
        if q < 3:
            B["dperm"][1] = mm(last, B["order"][1 + q]).astype(bf16)
            val = val + mm(B["dperm"][1], B["pp"][...], 0, 0)
        val = val.astype(bf16)
        for core in range(2):
            for i in range(16):
                low = 256 * core + 16 * i
                cpack[i, core, MAIN + 16 * q : MAIN + 16 * q + 16] = val[low : low + 16]
    wire.send(cpack.at[:, 1 - c, pl.ds(MAIN, TAIL)], cswap.at[:, pl.ds(MAIN, TAIL)], 124, place.partner)

    X, Z = pl.ds(0, PART), pl.ds(PART, PART)

    def fold_x(k):
        for i in range(4):
            to = (x + k) % 4
            total = cpack[4 * to + i, c, :PART].astype(f32) + cswap[4 * to + i, :PART].astype(f32)
            cmine[to, i, :PART] = total.astype(bf16)

    def fold_z(k):
        for i in range(4):
            to = (z + k) % 4
            total = cpack[4 * i + to, c, PART:].astype(f32) + cswap[4 * i + to, PART:].astype(f32)
            cmine[i, to, PART:] = total.astype(bf16)

    def src_x(k, part):
        return cmine.at[(x + k) % 4, pl.ds(2 * part, 2), X]

    def src_z(k, part):
        return cmine.at[pl.ds(2 * part, 2), (z + k) % 4, Z]

    def load_x(k, part, hop):
        to = (x + k) % 4
        for i in range(2):
            at = 2 * part + i
            cmine[to, at, :PART] = (cmine[to, at, :PART].astype(f32) + hop[part, i].astype(f32)).astype(bf16)

    def load_z(k, part, hop):
        to = (z + k) % 4
        for i in range(2):
            at = 2 * part + i
            cmine[at, to, PART:] = (cmine[at, to, PART:].astype(f32) + hop[part, i].astype(f32)).astype(bf16)

    for b in (4, 5, 6, 7, 0, 1, 2, 3):
        wire.wait(cswap.at[pl.ds(2 * b, 2), pl.ds(0, MAIN)], 116 + b, place.partner)
    for k in (2, 1, 3):
        fold_x(k)
        ring_one(src_x, B["hop_x"], B["end_x"], 2, place.xp, place.xm, 125, k)
    wire.wait(cswap.at[:, pl.ds(MAIN, TAIL)], 124, place.partner)
    for k in (2, 1, 3):
        fold_z(k)
        ring_one(src_z, B["hop_z"], B["end_z"], 2, place.zp, place.zm, 131, k)

    fold_x(0)
    fold_z(0)

    wire.wait(B["from_m"], 104, place.ym)

    def add_a(rows):
        packed[row(1, c), rows, :] = (packed[row(1, c), rows, :].astype(f32) + B["from_m"][rows, :].astype(f32)).astype(bf16)

    add_rows(0, CUT_A, 48, add_a)
    wire.send(packed.at[row(1, c), rows_a], B["fin_p"].at[rows_a], 106, place.yp)
    wire.wait(B["from_p"], 102, place.yp)

    def add_b(i, carry):
        here = pl.ds(pl.multiple_of(i * 48, 16), 48)
        rows = pl.ds(pl.multiple_of(CUT_A + i * 48, 16), 48)
        packed[row(3, c), rows, :] = (packed[row(3, c), rows, :].astype(f32) + B["from_p"][here, :].astype(f32)).astype(bf16)
        return carry

    lax.fori_loop(0, (PACK - CUT_A) // 48, add_b, 0)
    wire.send(packed.at[row(3, c), rows_b], B["fin_m"].at[rows_b], 107, place.ym)

    ring_two(src_x, load_x, B["hop_x"], B["end_x"], 2, place.xp, place.xm, 125)
    ring_two(src_z, load_z, B["hop_z"], B["end_z"], 2, place.zp, place.zm, 131)
    half_x, half_z = B["half_x"], B["half_z"]
    ring_three(B["end_x"], 2, place.xp, place.xm, 125)
    for i in range(4):
        total = cmine[x, i, :PART].astype(f32) + B["end_x"][0, i].astype(f32) + B["end_x"][1, i].astype(f32)
        half_x[i] = total.astype(bf16)
    for k in (2, 1, 3):
        wire.send(half_x.at[(z + k) % 4], B["two_x"].at[k - 1], 136 + k, place.at(0, k, 0))
    ring_three(B["end_z"], 2, place.zp, place.zm, 131)
    for i in range(4):
        total = cmine[i, z, PART:].astype(f32) + B["end_z"][0, i].astype(f32) + B["end_z"][1, i].astype(f32)
        half_z[i] = total.astype(bf16)
    for k in (2, 1, 3):
        wire.send(half_z.at[(x + k) % 4], B["two_z"].at[k - 1], 139 + k, place.at(k, 0, 0))
    combine_a(0)
    combine_b(0)
    for k in range(1, 4):
        wire.wait(B["two_x"].at[k - 1], 136 + k, place.at(0, 4 - k, 0))
    upper = half_x[z].astype(f32)
    for k in range(3):
        upper = upper + B["two_x"][k].astype(f32)
    for k in range(1, 4):
        wire.wait(B["two_z"].at[k - 1], 139 + k, place.at(4 - k, 0, 0))
    lower = half_z[x].astype(f32)
    for k in range(3):
        lower = lower + B["two_z"][k].astype(f32)
    line, column = iota((64, TAIL), 0), iota((64, TAIL), 1)
    inside, owner_y = line & 15, line >> 4
    entry = owner_y * 3 + inside % 3
    spot = jnp.where(inside < 12, (inside // 3) * 16 + entry, (entry // 4) * 16 + 12 + entry % 4)
    pick = (column == spot) & (inside < 15)
    ordered = mm(pick.astype(f32).astype(bf16), lower[16:].astype(bf16)).astype(bf16)
    main = jnp.concatenate([upper, lower[:16]], axis=0).astype(bf16)
    for k in range(4):
        B["low_x"][k] = main[24 * k : 24 * k + 24]
        B["low_z"][k] = ordered[16 * k : 16 * k + 16]
    for k in (2, 1, 3):
        to = (y + k) % 4
        wire.send(B["low_x"].at[to], B["three_x"].at[k - 1], 142 + k, place.at(0, 0, k))
        wire.send(B["low_z"].at[to], B["three_z"].at[k - 1], 145 + k, place.at(0, 0, k))

    wire.wait(B["fin_p"].at[rows_b], 103, place.ym)
    wire.wait(B["fin_m"].at[rows_a], 105, place.yp)
    wire.wait(B["fin_p"].at[rows_a], 106, place.ym)
    wire.wait(B["fin_m"].at[rows_b], 107, place.yp)

    def total_of(first_row, rows):
        at = pl.ds(first_row, rows)
        return packed[row(0, c), at, :].astype(f32) + B["fin_p"][at, :].astype(f32) + B["fin_m"][at, :].astype(f32)

    for l in range(LAYERS):
        for b in range(8):
            B["gin"][l, :, D * b : D * b + D] = total_of(576 * l + 48 * b, 48)
        for b in range(4):
            B["gdn"][l, 48 * b : 48 * b + 48, :] = total_of(576 * l + D + 48 * b, 48)
    leaving = [
        pltpu.make_async_copy(B["gin"], gin, local_sem.at[11]),
        pltpu.make_async_copy(B["gdn"], gdn, local_sem.at[12]),
    ]
    for copy in leaving:
        copy.start()
    gcls_out[...] = total_of(PACK - 48, 48)[:, 0:128].T[0:CLASSES]

    for k in range(1, 4):
        wire.wait(B["three_x"].at[k - 1], 142 + k, place.at(0, 0, 4 - k))
        wire.wait(B["three_z"].at[k - 1], 145 + k, place.at(0, 0, 4 - k))
    main = B["low_x"][y].astype(f32)
    tail = B["low_z"][y].astype(f32)
    for k in range(3):
        main = main + B["three_x"][k].astype(f32)
        tail = tail + B["three_z"][k].astype(f32)
    out_in[...] = main
    for q in range(4):
        out_dn[:, D * q : D * q + D] = tail[3 * q : 3 * q + 3]
    out_pe[...] = tail[12:15, 0:192]
    out_pos[...] = tail[12:15, 256:272]
    for copy in leaving:
        copy.wait()
    wire.finish()


def finish_kernel(*refs):
    count = len(refs) // 3
    given, results, held = refs[:count], refs[count : 2 * count], refs[2 * count : 3 * count]
    sem = refs[-1]
    inward = [pltpu.make_async_copy(given[n], held[n], sem.at[0, n]) for n in range(count)]
    outward = [pltpu.make_async_copy(held[n], results[n], sem.at[1, n]) for n in range(count)]
    for copy in inward:
        copy.start()
    for copy, onward in zip(inward, outward):
        copy.wait()
        onward.start()
    for copy in outward:
        copy.wait()


def per_device(patches, labels, assign, patch_embed, positions, client_in, client_down, server_in, server_down, classifier):
    shapes = [
        ((1, CAP), f32),
        ((LAYERS, 48, 4 * D + FF), f32),
        ((LAYERS, 192, D), f32),
        ((CLASSES, 48), f32),
        ((24, D), f32),
        ((3, FF), f32),
        ((3, 192), f32),
        ((3, TOK), f32),
    ]
    scratch = list(CLIENT.values()) + list(SERVER.values()) + list(BUFFERS.values())
    results = pl.pallas_call(
        step_kernel,
        out_shape=[jax.ShapeDtypeStruct(*s) for s in shapes],
        in_specs=[ANY] * 10,
        out_specs=[VMEM, HBM, HBM] + [VMEM] * 5,
        scratch_shapes=[pltpu.VMEM(*s) for s in scratch]
        + [
            pltpu.SemaphoreType.DMA((N_SEM,)),
            pltpu.SemaphoreType.DMA((N_SEM,)),
            pltpu.SemaphoreType.DMA((13,)),
            pltpu.SMEM((1, 128), jnp.int32),
        ],
        compiler_params=pltpu.CompilerParams(collective_id=0, has_side_effects=True, vmem_limit_bytes=67043328),
        name="step",
    )(
        patches.T,
        patch_embed,
        positions,
        assign.reshape(1, 128),
        labels.reshape(8, 128),
        classifier.transpose(2, 0, 1),
        client_in[None],
        client_down[None],
        server_in,
        server_down,
    )
    losses, gin, gdn, gcls, out_in, out_dn, out_pe, out_pos = pl.pallas_call(
        finish_kernel,
        out_shape=[jax.ShapeDtypeStruct(*s) for s in shapes],
        in_specs=[HBM] * len(shapes),
        out_specs=[HBM] * len(shapes),
        scratch_shapes=[pltpu.VMEM(*s) for s in shapes] + [pltpu.SemaphoreType.DMA((2, len(shapes)))],
        compiler_params=pltpu.CompilerParams(vmem_limit_bytes=67043328),
        name="finish",
    )(*results)
    return losses, out_pe.T, out_pos.T, out_in.T, out_dn.T, gin, gdn, gcls.T


def solution(mesh):
    in_specs = (
        P("client", None),
        P(),
        P(),
        P(),
        P(),
        P(),
        P(),
        P(None, "client", None),
        P(None, "client", None),
        P(),
    )
    out_specs = (
        P("client", None),
        P(None, "client"),
        P(None, "client"),
        P(None, "client"),
        P(None, "client"),
        P(None, "client", None),
        P(None, "client", None),
        P("client", None),
    )
    return jax.shard_map(per_device, mesh=mesh, in_specs=in_specs, out_specs=out_specs, check_vma=False)
```
